32 devices in a mesh: row: 4 (over y, core), col: 8 (over z, x).
Axes of the slice: x: 2, y: 2, z: 4, core: 2. Of those that a mesh axis runs over, the one named last changes fastest.
Arguments:
- l_saved: bfloat16 [16, 4, 256, 8, 256], P(None, 'row', None, 'col'), as said below
- l_grad: bfloat16 [16, 4, 256, 8, 256], P(None, 'row', None, 'col'), as said below
Outputs:
- grad_out: float32 [16, 4, 256, 8, 256], P(None, 'row', None, 'col')
Inputs may be any that keep to these rules, and one draw needn't show every extreme that they name: Read as one matrix of 16384 rows, l_saved is lower triangular with its diagonal between 1 and 2. Read as one matrix, l_grad is zero above the diagonal.
All inputs are finite; a program needn't handle non-finite values.
Results may differ from the reference program's by a relative error of at most 0.0003.
Values may be sent and summed in bfloat16 or wider, within the bound.
A program may use at most 64 MiB of HBM per device.

```python
import jax
import jax.numpy as jnp
from jax import lax

TILE = 256
N = 16384
TR = 16
N_ROW = 4
N_COL = 8


def global_index(shape):
    tile_row = lax.broadcasted_iota(jnp.int32, shape, 0) * N_ROW + lax.broadcasted_iota(jnp.int32, shape, 1)
    rows = tile_row * TILE + lax.broadcasted_iota(jnp.int32, shape, 2)
    cols = lax.broadcasted_iota(jnp.int32, shape, 3) * TILE + lax.broadcasted_iota(jnp.int32, shape, 4)
    return (rows, cols)


def draw_l_saved(key, part):
    shape = (TR, N_ROW, TILE, N_COL, TILE)
    rows, cols = global_index(shape)
    first, second = jax.random.split(jax.random.fold_in(key, 11))
    base = jax.random.normal(first, shape, jnp.float32)
    same_tile = rows // TILE == cols // TILE
    spread = jnp.where(same_tile, 0.35 / TILE ** 0.5, (N * TILE) ** (-0.25))
    diagonal = jax.random.uniform(second, shape, jnp.float32, 1.0, 2.0)
    value = jnp.where(rows > cols, base * spread, jnp.where(rows == cols, diagonal, 0.0))
    return value.astype(jnp.bfloat16)


def draw_l_grad(key, part):
    shape = (TR, N_ROW, TILE, N_COL, TILE)
    rows, cols = global_index(shape)
    first = jax.random.fold_in(jax.random.fold_in(key, 23), 0)
    base = jax.random.normal(first, shape, jnp.float32)
    return jnp.where(rows >= cols, base, 0.0).astype(jnp.bfloat16)


def setup_inputs(seed: int = 0) -> dict:
    seeds = jax.random.split(jax.random.key(seed), 3)
    l_saved = draw_l_saved(jax.random.fold_in(seeds[2], 71), 0)
    l_grad = draw_l_grad(jax.random.fold_in(seeds[2], 71), 0)
    return dict(l_saved=l_saved, l_grad=l_grad)


HIGH = lax.Precision.HIGHEST

def right_solve(factor, rhs):
    return lax.linalg.triangular_solve(factor, rhs, left_side=False, lower=True)

def diag_gradient(factor, lower_part):
    eye = jnp.eye(factor.shape[0], dtype=jnp.float32)
    middle = jnp.dot(factor.T.astype(jnp.float32), lower_part.astype(jnp.float32), precision=HIGH, preferred_element_type=jnp.float32)
    middle = jnp.tril(middle) - 0.5 * middle * eye
    half = lax.linalg.triangular_solve(factor, middle, left_side=True, lower=True, transpose_a=True)
    full = right_solve(factor, half)
    return full + full.T

def stacked_inner(left, right):
    flat_left = left.reshape(-1, left.shape[-1])
    flat_right = right.reshape(-1, right.shape[-1]).astype(jnp.float32)
    return lax.dot_general(flat_left.astype(jnp.float32), flat_right.astype(jnp.float32), (((0,), (0,)), ((), ())), precision=HIGH, preferred_element_type=jnp.float32)

def reference(l_saved, l_grad):
    n_tiles = N // TILE
    n_cols = N_COL
    factor = l_saved.reshape(n_tiles, TILE, n_cols, TILE).transpose(0, 2, 1, 3)
    grad = l_grad.reshape(n_tiles, TILE, n_cols, TILE).transpose(0, 2, 1, 3).astype(jnp.float32)
    tile_ids = jnp.arange(n_tiles, dtype=jnp.int32)
    col_ids = jnp.arange(n_cols, dtype=jnp.int32)
    eye = jnp.eye(TILE, dtype=jnp.float32)
    for panel in (n_cols - 1, n_cols - 2):
        diag_factor = factor[panel, panel].astype(jnp.float32)
        inverse = right_solve(diag_factor, eye)
        below = (tile_ids > panel)[:, None, None]
        column = grad[:, panel]
        solved = jnp.dot(column.reshape(-1, TILE).astype(jnp.float32), inverse.astype(jnp.float32), precision=HIGH, preferred_element_type=jnp.float32).reshape(n_tiles, TILE, TILE)
        cbar = jnp.where(below, solved, jnp.float32(0.0))
        total = column[panel] - stacked_inner(cbar, factor[:, panel])
        sym = diag_gradient(diag_factor, jnp.tril(total))

        def one_column(kcol):
            row_factor = factor[panel, kcol].astype(jnp.float32)
            update = jnp.dot(cbar.reshape(-1, TILE).astype(jnp.float32), row_factor.astype(jnp.float32), precision=HIGH, preferred_element_type=jnp.float32)
            fresh = grad[:, kcol] - update.reshape(n_tiles, TILE, TILE)
            summed = stacked_inner(cbar, factor[:, kcol])
            own = grad[panel, kcol] - (summed + jnp.dot(sym.astype(jnp.float32), row_factor.astype(jnp.float32), precision=HIGH, preferred_element_type=jnp.float32))
            return fresh.at[panel].set(own)
        updated = lax.map(one_column, col_ids).transpose(1, 0, 2, 3)
        abar = jnp.tril(sym) - 0.5 * sym * eye
        panel_col = jnp.where(below, cbar, jnp.where((tile_ids == panel)[:, None, None], abar[None], jnp.float32(0.0)))
        grad = jnp.where((col_ids < panel)[None, :, None, None], updated, grad)
        grad = grad.at[:, panel].set(panel_col)
    return grad.transpose(0, 2, 1, 3).reshape(TR, N_ROW, TILE, N_COL, TILE)
```

```python
import functools

import jax
import jax.numpy as jnp
from jax import lax
from jax.experimental import pallas as pl
from jax.experimental.pallas import tpu as pltpu
from jax.sharding import PartitionSpec as P

F32 = jnp.float32
BF16 = jnp.bfloat16
HIGH3 = lax.Precision.HIGH
MESH = pl.DeviceIdType.MESH
CHUNKS = 8


def dot3(a, b, ca=1, cb=0):
    return lax.dot_general(
        a, b, (((ca,), (cb,)), ((), ())), precision=HIGH3, preferred_element_type=F32
    )


def outer(a, b):
    return lax.dot_general(a, b, (((0,), (0,)), ((), ())), preferred_element_type=F32)


def panel_kernel(
    n_row,
    n_col,
    l_ref,
    g_ref,
    gbuf,
    xh,
    xl,
    own,
    lk,
    lbuf,
    w,
    h,
    tout,
    tin,
    tslot,
    hin,
    hsum,
    hslot,
    htwin,
    hfull,
    gd,
    sbuf,
    gs,
    gr,
    ls,
    lr,
    ks,
    kr,
    ts,
    tr,
    hs,
    hr,
    ds,
    dr,
    ss,
    sr,
):
    tile = l_ref.shape[1]
    half = tile // 2
    n = gbuf.shape[1]
    first = l_ref.shape[0] - n
    loc = first - 1
    ring = n_col // 2
    cut = n // 2
    head = min(2, n)
    pairs = n_row // 2

    row = lax.axis_index("row")
    col = lax.axis_index("col")
    q, p = col // 2, col % 2
    y, c = row // 2, row % 2
    panel = q == ring - 1
    top = y == pairs - 1
    lower = jnp.maximum(col - 2, 0)
    twin = 2 * q + 1 - p
    mate = 2 * y + 1 - c
    root = n_row - 2 + c

    rows = lax.broadcasted_iota(jnp.int32, (tile, tile), 0)
    cols = lax.broadcasted_iota(jnp.int32, (tile, tile), 1)

    def rdma(src, dst, s_sem, r_sem, dev):
        return pltpu.make_async_remote_copy(
            src_ref=src, dst_ref=dst, send_sem=s_sem, recv_sem=r_sem, device_id=dev, device_id_type=MESH
        )

    barrier = pltpu.get_barrier_semaphore()

    def greet(dev):
        pl.semaphore_signal(barrier, inc=1, device_id=dev, device_id_type=MESH)

    greet({"col": twin})
    greet({"row": mate})

    @pl.when(q > 0)
    def _():
        greet({"col": col - 2})

    @pl.when(jnp.logical_not(panel))
    def _():
        greet({"col": col + 2})

    @pl.when(jnp.logical_not(top))
    def _():
        greet({"row": root})

    @pl.when(top)
    def _():
        for k in range(pairs - 1):
            greet({"row": 2 * k + c})

    @pl.when(top & panel)
    def _():
        greet({"row": mate, "col": twin})

    heard = (
        2
        + (q > 0).astype(jnp.int32)
        + jnp.logical_not(panel).astype(jnp.int32)
        + jnp.where(top, pairs - 1, 1)
        + (top & panel).astype(jnp.int32)
    )
    pl.semaphore_wait(barrier, heard)

    def g_down(t, src):
        return rdma(src, gbuf.at[p, t], gs.at[t, 0], gr.at[p, t], {"col": lower})

    def g_cross(t, src):
        return rdma(src, gbuf.at[p, t], gs.at[t, 1], gr.at[p, t], {"col": twin})

    def g_wait(s, t):
        rdma(gbuf.at[s, t], gbuf.at[s, t], gs.at[t, 0], gr.at[s, t], {"col": twin}).wait_recv()

    def f_cross(t):
        return rdma(l_ref.at[first + t], gbuf.at[0, t], gs.at[t, 1], gr.at[0, t], {"col": twin})

    def l_down(i, src):
        return rdma(src, lbuf.at[p, i], ls.at[i, 0], lr.at[p, i], {"col": lower})

    def l_cross(i, src):
        return rdma(src, lbuf.at[p, i], ls.at[i, 1], lr.at[p, i], {"col": twin})

    def l_wait(s, i):
        rdma(lbuf.at[s, i], lbuf.at[s, i], ls.at[i, 0], lr.at[s, i], {"col": twin}).wait_recv()

    def k_star(k):
        return rdma(l_ref.at[loc], lk.at[c], ks.at[k], kr.at[c], {"row": 2 * k + c})

    def k_mate(src):
        return rdma(src, lk.at[c], ks.at[pairs], kr.at[c], {"row": mate})

    def k_wait(i):
        rdma(lk.at[i], lk.at[i], ks.at[pairs], kr.at[i], {"row": mate}).wait_recv()

    def t_mate():
        return rdma(tout.at[1 - c], tin, ts.at[0], tr.at[pairs], {"row": mate})

    def t_root():
        return rdma(tout.at[c], tslot.at[y], ts.at[1], tr.at[y], {"row": root})

    def h_mate(k):
        return rdma(h.at[k, 1 - c], hin.at[k], hs.at[k, 0], hr.at[k, 0], {"row": mate})

    def h_root(k):
        return rdma(hsum.at[k], hslot.at[k, y], hs.at[k, 1], hr.at[k, 3 + y], {"row": root})

    def h_twin(k):
        return rdma(hsum.at[k], htwin.at[k], hs.at[k, 2], hr.at[k, 1], {"col": twin})

    def h_full(k):
        return rdma(hfull.at[k, c], hfull.at[k, c], hs.at[k, 3], hr.at[k, 2], {"row": mate})

    def d_mate(k):
        return rdma(g_ref.at[loc], gd.at[k], ds.at[0], dr.at[k], {"row": mate})

    def d_twin(k):
        return rdma(g_ref.at[loc], gd.at[k], ds.at[1], dr.at[k], {"col": twin})

    def d_diag(k):
        return rdma(g_ref.at[loc], gd.at[k], ds.at[2], dr.at[k], {"row": mate, "col": twin})

    def s_down(k):
        return rdma(sbuf.at[p, k], sbuf.at[p, k], ss.at[k, 0], sr.at[p, k], {"col": lower})

    def s_cross(k):
        return rdma(sbuf.at[p, k], sbuf.at[p, k], ss.at[k, 1], sr.at[p, k], {"col": twin})

    def loop(a, b, body):
        def step(i, carry):
            body(i)
            return carry

        lax.fori_loop(a, b, step, 0)

    def when_p0(cond, body):
        pl.when(cond)(body)

    @pl.when(top)
    def _():
        for k in range(pairs - 1):
            k_star(k).start()
        k_mate(l_ref.at[loc]).start()
        lk[c] = l_ref[loc]

    def gather_rows():
        @pl.when(jnp.logical_not(top))
        def _():
            k_wait(c)
            k_mate(lk.at[c]).start()

        k_wait(1 - c)

    def start_inverse():
        for k in range(2):
            d = lbuf[k, k].astype(F32)
            e = (rows == cols).astype(F32)
            on = d * e
            rc = 1.0 / jnp.sum(on, axis=1, keepdims=True)
            rr = 1.0 / jnp.sum(on, axis=0, keepdims=True)
            off = ((rows & 1) == 1) & (cols == rows - 1)
            w[k] = e * rr - rc * jnp.where(off, d, 0.0) * rr

    levels = []
    size = 2
    while size < tile:
        levels.append(size)
        size *= 2

    def inverse_level(size):
        sh = size.bit_length() - 1
        off = (((rows >> sh) & 1) == 1) & ((cols >> sh) == (rows >> sh) - 1)
        for k in range(2):
            part = jnp.where(off, lbuf[k, k].astype(F32), 0.0)
            cur = w[k]
            w[k] = cur - dot3(cur, dot3(part, cur))

    def finish_inverse():
        w[2] = -dot3(w[1], dot3(lbuf[0, 1].astype(F32), w[0]))

    def put_x(i, x):
        hi = x.astype(BF16)
        xh[i] = hi
        xl[i] = (x - hi.astype(F32)).astype(BF16)

    h[...] = jnp.zeros_like(h)

    def add_h(k, left, right):
        h[k] += outer(left, right).reshape(2, half, tile)

    @pl.when(jnp.logical_not(panel))
    def _():
        def relay(t):
            g_wait(p, t)

            @pl.when(q > 0)
            def _():
                g_down(t, gbuf.at[p, t]).start()

            g_cross(t, gbuf.at[p, t]).start()

        def relay_l(i):
            l_wait(p, i)

            @pl.when(q > 0)
            def _():
                l_down(i, lbuf.at[p, i]).start()

            l_cross(i, lbuf.at[p, i]).start()

        def use(t):
            g_wait(1 - p, t)
            right = l_ref[first + t]
            add_h(0, gbuf[0, t], right)
            add_h(1, gbuf[1, t], right)

        for t in range(head):
            relay(t)
        gather_rows()

        @pl.when(p == 0)
        def _():
            relay_l(0)

        relay_l(1)

        @pl.when(p == 0)
        def _():
            l_wait(1, 1)

        @pl.when(p == 1)
        def _():
            l_wait(0, 0)
            l_wait(0, 1)

        def solve_x():
            finish_inverse()
            k0, k1 = lk[0].astype(F32), lk[1].astype(F32)
            put_x(0, dot3(w[0], k0))
            put_x(1, dot3(w[2], k0) + dot3(w[1], k1))

        work = [start_inverse] + [functools.partial(inverse_level, s) for s in levels] + [solve_x]
        t = head
        for job in work:
            if t < n:
                relay(t)
                use(t - 2)
                t += 1
            job()
        done = t

        def both(i):
            relay(i)
            use(i - 2)

        if done < n:
            loop(done, n, both)
        loop(max(n - 2, 0), n, use)

        h0, h1 = h[0].reshape(tile, tile), h[1].reshape(tile, tile)
        tout[1] = dot3(w[1], h1, 0, 0)
        tout[0] = dot3(w[0], h0, 0, 0) + dot3(w[2], h1, 0, 0)
        t_mate().start()

        @pl.when(jnp.logical_not(top))
        def _():
            t_mate().wait_recv()
            tout[c] += tin[...]
            t_root().start()
            own[...] = g_ref[loc].astype(F32)

        @pl.when(top)
        def _():
            def s_wait(s, k):
                rdma(sbuf.at[s, k], sbuf.at[s, k], ss.at[k, 0], sr.at[s, k], {"col": twin}).wait_recv()

            def s_relay(k):
                s_wait(p, k)

                @pl.when(q > 0)
                def _():
                    s_down(k).start()

                s_cross(k).start()

            loop(0, CHUNKS, s_relay)
            t_mate().wait_recv()
            total = g_ref[loc].astype(F32) - (tout[c] + tin[...])
            for k in range(pairs - 1):
                rdma(tslot.at[k], tslot.at[k], ts.at[1], tr.at[k], {"row": mate}).wait_recv()
                total = total - tslot[k]
            own[...] = total
            loop(0, CHUNKS, lambda k: s_wait(1 - p, k))
            k0, k1 = lk[0].astype(F32), lk[1].astype(F32)
            s0, s1 = sbuf[0].reshape(tile, tile), sbuf[1].reshape(tile, tile)
            own[...] -= dot3(s0, k0) + dot3(s1, k1)

        def drain_g(t):
            @pl.when(q > 0)
            def _():
                g_down(t, gbuf.at[p, t]).wait_send()

            g_cross(t, gbuf.at[p, t]).wait_send()

        loop(0, n, drain_g)

        def drain_l(i):
            @pl.when(q > 0)
            def _():
                l_down(i, lbuf.at[p, i]).wait_send()

            l_cross(i, lbuf.at[p, i]).wait_send()

        @pl.when(p == 0)
        def _():
            drain_l(0)

        drain_l(1)
        t_mate().wait_send()

        @pl.when(jnp.logical_not(top))
        def _():
            t_root().wait_send()

        @pl.when(top)
        def _():
            def drain_s(k):
                @pl.when(q > 0)
                def _():
                    s_down(k).wait_send()

                s_cross(k).wait_send()

            loop(0, CHUNKS, drain_s)

    @pl.when(panel)
    def _():
        def send(t):
            if ring > 1:
                g_down(t, g_ref.at[first + t]).start()

        def cross_lo(t):
            f_cross(t).start()

        def cross_hi(t):
            g_cross(t, g_ref.at[first + t]).start()

        lead = min(2, cut)
        for t in range(head):
            send(t)

        @pl.when(p == 0)
        def _():
            for t in range(cut, min(cut + 2, n)):
                cross_lo(t)

        @pl.when(p == 1)
        def _():
            for t in range(lead):
                cross_hi(t)

        gather_rows()

        @pl.when(p == 0)
        def _():
            for i in range(2):
                if ring > 1:
                    l_down(i, lk.at[i]).start()
                l_cross(i, lk.at[i]).start()
                lbuf[0, i] = lk[i]
            loop(min(cut + 2, n), n, cross_lo)

            @pl.when(top & (c == 1))
            def _():
                d_mate(1).start()
                d_diag(1).start()
                gd[1] = g_ref[loc]

        @pl.when(p == 1)
        def _():
            if ring > 1:
                l_down(1, lk.at[1]).start()
            l_cross(1, lk.at[1]).start()
            lbuf[1, 1] = lk[1]
            loop(lead, cut, cross_hi)

            @pl.when(top & (c == 1))
            def _():
                d_mate(2).start()
                d_twin(2).start()
                d_diag(2).start()
                gd[2] = g_ref[loc]

        loop(head, n, send)

        loop(0, n, lambda t: add_h(0, g_ref[first + t], l_ref[first + t]))
        h_mate(0).start()

        @pl.when(p == 0)
        def _():
            l_wait(1, 1)

        @pl.when(p == 1)
        def _():
            l_wait(0, 0)
            l_wait(0, 1)

        def reduce_mate(k):
            h_mate(k).wait_recv()
            hsum[k] = h[k, c] + hin[k]

            @pl.when(jnp.logical_not(top))
            def _():
                h_root(k).start()

        def reduce_root(k):
            total = hsum[k]
            for i in range(pairs - 1):
                rdma(
                    hslot.at[k, i], hslot.at[k, i], hs.at[k, 1], hr.at[k, 3 + i], {"row": mate}
                ).wait_recv()
                total = total + hslot[k, i]
            hsum[k] = total
            h_twin(k).start()

        start_inverse()
        reduce_mate(0)
        for i, s in enumerate(levels):
            inverse_level(s)
            if i == len(levels) // 2:

                @pl.when(top)
                def _():
                    reduce_root(0)

        finish_inverse()

        def keep(t):
            gbuf[p, t] = g_ref[first + t]

        loop(0, n, keep)

        @pl.when(p == 0)
        def _():
            def use(t):
                g_wait(1, t)
                add_h(1, gbuf[1, t], l_ref[first + t])

            loop(0, cut, use)

        @pl.when(p == 1)
        def _():
            def fill(t):
                gbuf[0, t] = g_ref[first + t]

            loop(0, cut, fill)

            def use(t):
                g_wait(0, t)
                add_h(1, g_ref[first + t], gbuf[0, t])

            loop(cut, n, use)

        h_mate(1).start()
        reduce_mate(1)

        @pl.when(top)
        def _():
            reduce_root(1)

        @pl.when(p == 1)
        def _():
            loop(cut, n, cross_hi)

        @pl.when(p == 0)
        def _():
            put_x(0, -w[0])
            put_x(1, -w[2])

        @pl.when(p == 1)
        def _():
            xh[0] = jnp.zeros((tile, tile), BF16)
            xl[0] = jnp.zeros((tile, tile), BF16)
            put_x(1, -w[1])

        @pl.when(jnp.logical_not(top))
        def _():
            own[...] = jnp.zeros((tile, tile), F32)

        @pl.when(top)
        def _():
            rdma(htwin.at[0], htwin.at[0], hs.at[0, 2], hr.at[0, 1], {"col": twin}).wait_recv()
            rdma(htwin.at[1], htwin.at[1], hs.at[1, 2], hr.at[1, 1], {"col": twin}).wait_recv()
            mine, theirs = hsum[0], htwin[0]
            hfull[0, c] = jnp.where(p == 0, mine, theirs)
            hfull[2, c] = jnp.where(p == 0, theirs, mine)
            hfull[1, c] = hsum[1] + htwin[1]
            for k in range(3):
                h_full(k).start()
            for k in range(3):
                rdma(
                    hfull.at[k, 1 - c], hfull.at[k, 1 - c], hs.at[k, 3], hr.at[k, 2], {"row": mate}
                ).wait_recv()

            def d_wait(k):
                rdma(gd.at[k], gd.at[k], ds.at[0], dr.at[k], {"row": mate}).wait_recv()

            @pl.when(jnp.logical_not((c == 1) & (p == 1)))
            def _():
                d_wait(2)

            @pl.when(c == 0)
            def _():
                d_wait(1)

            eye = (rows == cols).astype(F32)

            def low(x):
                return jnp.where(rows >= cols, x, 0.0)

            w66, w77, w76 = w[0], w[1], w[2]
            l77 = lbuf[1, 1].astype(F32)

            def full(k):
                return hfull[k].reshape(tile, tile)

            q77 = low(gd[2].astype(F32) - dot3(w77, full(2), 0, 0))
            m77 = dot3(l77, q77, 0, 0)
            phi77 = low(m77) - 0.5 * m77 * eye

            def put_s(s, o):
                sbuf[p] = s.reshape(CHUNKS, tile // CHUNKS, tile)
                own[...] = o

            def tri(s):
                return low(s) - 0.5 * s * eye

            @pl.when((c == 1) & (p == 1))
            def _():
                half77 = dot3(dot3(w77, phi77, 0, 0), w77)
                s = half77 + half77.T
                put_s(s, tri(s))

            @pl.when(jnp.logical_not((c == 1) & (p == 1)))
            def _():
                g76 = jnp.where(c == 1, g_ref[loc].astype(F32), gd[1].astype(F32))
                q76 = g76 - dot3(w77, full(1), 0, 0)
                phi76 = dot3(l77, q76, 0, 0)

                @pl.when((c == 0) & (p == 0))
                def _():
                    t66 = dot3(w66, full(0), 0, 0) + dot3(w76, full(1), 0, 0)
                    q66 = low(g_ref[loc].astype(F32) - t66)
                    m66 = dot3(lbuf[0, 0].astype(F32), q66, 0, 0) + dot3(lbuf[0, 1].astype(F32), q76, 0, 0)
                    phi66 = low(m66) - 0.5 * m66 * eye
                    inner = dot3(phi76, w66) + dot3(phi77, w76)
                    half66 = dot3(w66, dot3(phi66, w66), 0, 0) + dot3(w76, inner, 0, 0)
                    s = half66 + half66.T
                    put_s(s, tri(s))

                @pl.when(jnp.logical_not((c == 0) & (p == 0)))
                def _():
                    inner = dot3(phi76, w66) + dot3(phi77 + phi77.T, w76)

                    @pl.when(c == 1)
                    def _():
                        s = dot3(w77, inner, 0, 0)
                        put_s(s, s)

                    @pl.when(c == 0)
                    def _():
                        put_s(dot3(inner, w77, 0, 0), jnp.zeros((tile, tile), F32))

            if ring > 1:
                loop(0, CHUNKS, lambda k: s_down(k).start())

        @pl.when(p == 0)
        def _():
            loop(cut, n, lambda t: g_wait(1, t))
            loop(cut, n, lambda t: f_cross(t).wait_send())
            for i in range(2):
                if ring > 1:
                    l_down(i, lk.at[i]).wait_send()
                l_cross(i, lk.at[i]).wait_send()

            @pl.when(top & (c == 1))
            def _():
                d_mate(1).wait_send()
                d_diag(1).wait_send()

        @pl.when(p == 1)
        def _():
            loop(0, n, lambda t: g_cross(t, g_ref.at[first + t]).wait_send())
            if ring > 1:
                l_down(1, lk.at[1]).wait_send()
            l_cross(1, lk.at[1]).wait_send()

            @pl.when(top & (c == 1))
            def _():
                d_mate(2).wait_send()
                d_twin(2).wait_send()
                d_diag(2).wait_send()

        if ring > 1:
            loop(0, n, lambda t: g_down(t, g_ref.at[first + t]).wait_send())
        for k in range(2):
            h_mate(k).wait_send()

            @pl.when(jnp.logical_not(top))
            def _():
                h_root(k).wait_send()

            @pl.when(top)
            def _():
                h_twin(k).wait_send()

        @pl.when(top)
        def _():
            for k in range(3):
                h_full(k).wait_send()
            if ring > 1:
                loop(0, CHUNKS, lambda k: s_down(k).wait_send())

    @pl.when(top)
    def _():
        for k in range(pairs - 1):
            k_star(k).wait_send()
        k_mate(l_ref.at[loc]).wait_send()

    @pl.when(jnp.logical_not(top))
    def _():
        k_mate(lk.at[c]).wait_send()


def panel(factor, grad, n_row, n_col, first):
    rows_here, tile = factor.shape[0], factor.shape[1]
    n = rows_here - first
    half = tile // 2
    pairs = n_row // 2
    vmem = pl.BlockSpec(memory_space=pltpu.VMEM)
    dma = pltpu.SemaphoreType.DMA
    return pl.pallas_call(
        functools.partial(panel_kernel, n_row, n_col),
        out_shape=(
            jax.ShapeDtypeStruct((2, n, tile, tile), BF16),
            jax.ShapeDtypeStruct((2, tile, tile), BF16),
            jax.ShapeDtypeStruct((2, tile, tile), BF16),
            jax.ShapeDtypeStruct((tile, tile), F32),
        ),
        in_specs=[vmem, vmem],
        out_specs=(vmem, vmem, vmem, vmem),
        scratch_shapes=[
            pltpu.VMEM((2, tile, tile), BF16),
            pltpu.VMEM((2, 2, tile, tile), BF16),
            pltpu.VMEM((3, tile, tile), F32),
            pltpu.VMEM((2, 2, half, tile), F32),
            pltpu.VMEM((2, tile, tile), F32),
            pltpu.VMEM((tile, tile), F32),
            pltpu.VMEM((pairs, tile, tile), F32),
            pltpu.VMEM((2, half, tile), F32),
            pltpu.VMEM((2, half, tile), F32),
            pltpu.VMEM((2, pairs, half, tile), F32),
            pltpu.VMEM((2, half, tile), F32),
            pltpu.VMEM((3, 2, half, tile), F32),
            pltpu.VMEM((3, tile, tile), BF16),
            pltpu.VMEM((2, CHUNKS, tile // CHUNKS, tile), F32),
            dma((n, 2)),
            dma((2, n)),
            dma((2, 2)),
            dma((2, 2)),
            dma((pairs + 1,)),
            dma((2,)),
            dma((2,)),
            dma((pairs + 1,)),
            dma((3, 4)),
            dma((3, 3 + pairs)),
            dma((3,)),
            dma((3,)),
            dma((CHUNKS, 2)),
            dma((2, CHUNKS)),
        ],
        compiler_params=pltpu.CompilerParams(
            collective_id=0, has_side_effects=True, vmem_limit_bytes=40 * 1024 * 1024
        ),
        name="panel",
    )(factor, grad)


def update_kernel(n_col, first, base_ref, gbuf, xh, xl, own, out_ref):
    tile = base_ref.shape[1]
    lane = out_ref.shape[1]
    parts = tile // lane
    step = pl.program_id(0)
    right = lax.axis_index("col") >= n_col - 2

    def store(i, value):
        for b in range(parts):
            out_ref[pl.ds(i * tile * parts + b, tile, stride=parts), :] = value[:, b * lane : (b + 1) * lane]

    def base(i):
        return jnp.where(right, 0.0, base_ref[i].astype(F32))

    @pl.when(step == 0)
    def _():
        for i in range(first - 1):
            store(i, base(i))
        store(first - 1, own[...])

    @pl.when(step > 0)
    def _():
        for i in range(first):
            total = base(i)
            for part in (xl, xh):
                for s in range(2):
                    total = total - jnp.dot(gbuf[s, i], part[s], preferred_element_type=F32)
            store(i, total)


def update(grad, gbuf, xh, xl, own, n_col, first):
    rows_here, tile = grad.shape[0], grad.shape[1]
    lane = 128
    whole = lambda k: pl.BlockSpec((2, tile, tile), lambda a: (0, 0, 0))
    return pl.pallas_call(
        functools.partial(update_kernel, n_col, first),
        grid=(rows_here // first,),
        out_shape=jax.ShapeDtypeStruct((rows_here * tile * tile // lane, lane), F32),
        in_specs=[
            pl.BlockSpec((first, tile, tile), lambda a: (a, 0, 0)),
            pl.BlockSpec((2, first, tile, tile), lambda a: (0, jnp.maximum(a - 1, 0), 0, 0)),
            whole(0),
            whole(1),
            pl.BlockSpec((tile, tile), lambda a: (0, 0)),
        ],
        out_specs=pl.BlockSpec((first * tile * tile // lane, lane), lambda a: (a, 0)),
        name="update",
    )(grad, gbuf, xh, xl, own)


def per_device(l_saved, l_grad):
    rows_here, tile = l_saved.shape[0], l_saved.shape[2]
    n_row = lax.axis_size("row")
    n_col = lax.axis_size("col")
    assert n_col % n_row == 0 and n_row % 2 == 0
    first = n_col // n_row
    assert rows_here % first == 0
    factor = l_saved.reshape(rows_here, tile, tile)
    grad = l_grad.reshape(rows_here, tile, tile)
    gbuf, xh, xl, own = panel(factor, grad, n_row, n_col, first)
    out = update(grad, gbuf, xh, xl, own, n_col, first)
    return out.reshape(l_grad.shape)


def solution(mesh):
    spec = P(None, "row", None, "col", None)
    return jax.shard_map(
        per_device, mesh=mesh, in_specs=(spec, spec), out_specs=spec, check_vma=False
    )
```

```python
import functools

import jax
import jax.numpy as jnp
from jax import lax
from jax.experimental import pallas as pl
from jax.experimental.pallas import tpu as pltpu
from jax.sharding import PartitionSpec as P

F32 = jnp.float32
BF16 = jnp.bfloat16
HIGH3 = lax.Precision.HIGH
MESH = pl.DeviceIdType.MESH
CHUNKS = 8
SUB = 4
LANE = 128
VMEM = 40 * 1024 * 1024


def dot3(a, b, ca=1, cb=0):
    return lax.dot_general(
        a, b, (((ca,), (cb,)), ((), ())), precision=HIGH3, preferred_element_type=F32
    )


def outer(a, b):
    return lax.dot_general(a, b, (((0,), (0,)), ((), ())), preferred_element_type=F32)


def panel_kernel(
    n_row,
    n_col,
    l_hbm,
    g_hbm,
    lin,
    lv,
    gv,
    gbuf,
    xh,
    xl,
    lk,
    lbuf,
    w,
    h,
    tout,
    tin,
    tslot,
    hin,
    hsum,
    hslot,
    htwin,
    hfull,
    gd,
    sbuf,
    vs,
    gs,
    gr,
    ls,
    lr,
    ks,
    kr,
    ts,
    tr,
    hs,
    hr,
    ds,
    dr,
    ss,
    sr,
):
    held, tile = lv.shape[0], lv.shape[3]
    half = tile // 2
    n = gbuf.shape[1]
    first = held - n
    loc = first - 1
    ring = n_col // 2
    cut = n // 2
    head = min(2, n)
    pairs = n_row // 2
    parts = tile // LANE

    row = lax.axis_index("row")
    col = lax.axis_index("col")
    q, p = col // 2, col % 2
    y, c = row // 2, row % 2
    panel = q == ring - 1
    top = y == pairs - 1
    below = q > 0
    lower = jnp.maximum(col - 2, 0)
    twin = 2 * q + 1 - p
    mate = 2 * y + 1 - c
    root = n_row - 2 + c

    rows = lax.broadcasted_iota(jnp.int32, (tile, tile), 0)
    cols = lax.broadcasted_iota(jnp.int32, (tile, tile), 1)

    def rdma(src, dst, s_sem, r_sem, dev):
        return pltpu.make_async_remote_copy(
            src_ref=src, dst_ref=dst, send_sem=s_sem, recv_sem=r_sem, device_id=dev, device_id_type=MESH
        )

    def loop(a, b, body):
        def step(i, carry):
            body(i)
            return carry

        if a < b:
            lax.fori_loop(a, b, step, 0)

    def load(src, dst, k, a, b):
        return pltpu.make_async_copy(src.at[pl.ds(a, b - a)], dst.at[pl.ds(a, b - a)], vs.at[k])

    spans = [
        (l_hbm, lv, 0, loc, first),
        (g_hbm, gv, 1, first, first + head),
        (l_hbm, lv, 2, first, held),
        (g_hbm, gv, 3, first + head, held),
        (g_hbm, gv, 4, 0, first),
    ]
    loads = [load(*span) for span in spans if span[3] < span[4]]
    for cp in loads:
        cp.start()

    barrier = pltpu.get_barrier_semaphore()

    def greet(dev):
        pl.semaphore_signal(barrier, inc=1, device_id=dev, device_id_type=MESH)

    greet({"col": twin})
    greet({"row": mate})

    @pl.when(below)
    def _():
        greet({"col": col - 2})

    @pl.when(jnp.logical_not(panel))
    def _():
        greet({"col": col + 2})

    @pl.when(jnp.logical_not(top))
    def _():
        greet({"row": root})

    @pl.when(top)
    def _():
        for k in range(pairs - 1):
            greet({"row": 2 * k + c})

    @pl.when(top & panel)
    def _():
        greet({"row": mate, "col": twin})

    heard = (
        2
        + below.astype(jnp.int32)
        + jnp.logical_not(panel).astype(jnp.int32)
        + jnp.where(top, pairs - 1, 1)
        + (top & panel).astype(jnp.int32)
    )
    with jax.named_scope("barrier"):
        pl.semaphore_wait(barrier, heard)

    with jax.named_scope("loads"):
        for cp in loads:
            cp.wait()

    def mat(ref, *at):
        return ref[at].reshape(tile, tile)

    def g_down(t, k, src):
        return rdma(src.at[k], gbuf.at[p, t, k], gs.at[t, k, 0], gr.at[p, t, k], {"col": lower})

    def g_cross(t, k, src):
        return rdma(src.at[k], gbuf.at[p, t, k], gs.at[t, k, 1], gr.at[p, t, k], {"col": twin})

    def g_wait(s, t, k):
        ref = gbuf.at[s, t, k]
        rdma(ref, ref, gs.at[t, k, 0], gr.at[s, t, k], {"col": twin}).wait_recv()

    def f_cross(t, k):
        return rdma(lv.at[first + t, k], gbuf.at[0, t, k], gs.at[t, k, 1], gr.at[0, t, k], {"col": twin})

    def l_down(k, src):
        return rdma(src.at[k], lbuf.at[p, c, k], ls.at[p, k, 0], lr.at[p, c, k], {"col": lower})

    def l_cross(k, src):
        return rdma(src.at[k], lbuf.at[p, c, k], ls.at[p, k, 1], lr.at[p, c, k], {"col": twin})

    def l_mate(s, k):
        ref = lbuf.at[s, c, k]
        return rdma(ref, ref, ls.at[s, k, 2], lr.at[s, c, k], {"row": mate})

    def l_wait(s, i, k):
        ref = lbuf.at[s, i, k]
        rdma(ref, ref, ls.at[s, k, 2], lr.at[s, i, k], {"row": mate}).wait_recv()

    def k_star(k):
        return rdma(lv.at[loc], lk.at[c], ks.at[k], kr.at[c], {"row": 2 * k + c})

    def k_mate(src):
        return rdma(src, lk.at[c], ks.at[pairs], kr.at[c], {"row": mate})

    def k_wait(i):
        rdma(lk.at[i], lk.at[i], ks.at[pairs], kr.at[i], {"row": mate}).wait_recv()

    def t_mate():
        return rdma(tout.at[1 - c], tin, ts.at[0], tr.at[pairs], {"row": mate})

    def t_root():
        return rdma(tout.at[c], tslot.at[y], ts.at[1], tr.at[y], {"row": root})

    def h_mate(k):
        return rdma(h.at[k, 1 - c], hin.at[k], hs.at[k, 0], hr.at[k, 0], {"row": mate})

    def h_root(k):
        return rdma(hsum.at[k], hslot.at[k, y], hs.at[k, 1], hr.at[k, 3 + y], {"row": root})

    def h_twin(k):
        return rdma(hsum.at[k], htwin.at[k], hs.at[k, 2], hr.at[k, 1], {"col": twin})

    def h_full(k):
        return rdma(hfull.at[k, c], hfull.at[k, c], hs.at[k, 3], hr.at[k, 2], {"row": mate})

    def d_copy(k, src, i, dev):
        return rdma(src, gd.at[k], ds.at[i], dr.at[k], dev)

    def d_wait(k):
        d_copy(k, gd.at[k], 0, {"row": mate}).wait_recv()

    def s_down(k):
        return rdma(sbuf.at[p, k], sbuf.at[p, k], ss.at[k, 0], sr.at[p, k], {"col": lower})

    def s_cross(k):
        return rdma(sbuf.at[p, k], sbuf.at[p, k], ss.at[k, 1], sr.at[p, k], {"col": twin})

    def s_wait(s, k):
        rdma(sbuf.at[s, k], sbuf.at[s, k], ss.at[k, 0], sr.at[s, k], {"col": twin}).wait_recv()

    @pl.when(top)
    def _():
        for k in range(pairs - 1):
            k_star(k).start()
        k_mate(lv.at[loc]).start()
        lk[c] = lv[loc]

    def gather_rows():
        @pl.when(jnp.logical_not(top))
        def _():
            k_wait(c)
            k_mate(lk.at[c]).start()

        k_wait(1 - c)

    def start_inverse(k):
        d = mat(lbuf, k, k).astype(F32)
        e = (rows == cols).astype(F32)
        on = d * e
        rc = 1.0 / jnp.sum(on, axis=1, keepdims=True)
        rr = 1.0 / jnp.sum(on, axis=0, keepdims=True)
        off = ((rows & 1) == 1) & (cols == rows - 1)
        w[k] = e * rr - rc * jnp.where(off, d, 0.0) * rr

    n_lev = tile.bit_length() - 2

    def inverse_level(sh, k):
        off = ((jnp.right_shift(rows, sh) & 1) == 1) & (
            jnp.right_shift(cols, sh) == jnp.right_shift(rows, sh) - 1
        )
        part = jnp.where(off, mat(lbuf, k, k).astype(F32), 0.0)
        cur = w[k]
        w[k] = cur - dot3(cur, dot3(part, cur))

    def finish_inverse():
        w[2] = -dot3(w[1], dot3(mat(lbuf, 0, 1).astype(F32), w[0]))

    def put_x(i, x):
        hi = x.astype(BF16)
        xh[i] = hi
        xl[i] = (x - hi.astype(F32)).astype(BF16)

    def store(a, value):
        for b in range(parts):
            lin[a, pl.ds(b, tile, stride=parts), :] = value[:, b * LANE : (b + 1) * LANE]

    h[...] = jnp.zeros_like(h)

    def add_h(k, left, right):
        h[k] += outer(left, right).reshape(2, half, tile)

    def times_x(total, i, g):
        for part in (xl, xh):
            total = total - jnp.dot(g, part[i], preferred_element_type=F32)
        return total

    @pl.when(jnp.logical_not(panel))
    def _():
        def relay(t, work=()):
            for k in range(SUB):
                with jax.named_scope("w_main"):
                    g_wait(p, t, k)

                @pl.when(below)
                def _():
                    g_down(t, k, gbuf.at[p, t]).start()

                g_cross(t, k, gbuf.at[p, t]).start()
                if k < len(work):
                    work[k]()

        def use(t):
            with jax.named_scope("w_cross"):
                for k in range(SUB):
                    g_wait(1 - p, t, k)
            right = mat(lv, first + t)
            add_h(0, mat(gbuf, 0, t), right)
            add_h(1, mat(gbuf, 1, t), right)

        def low(t):
            total = mat(gv, first + t).astype(F32)
            for s in range(2):
                total = times_x(total, s, mat(gbuf, s, t))
            store(first + t, total)

        main_l = (p == 0) | (c == 1)
        other_l = (p == 1) | (c == 1)

        for t in range(head):
            relay(t)
        with jax.named_scope("gather"):
            gather_rows()

        with jax.named_scope("l_relay"):

            @pl.when(main_l)
            def _():
                def step(k):
                    l_wait(p, c, k)

                    @pl.when(below)
                    def _():
                        l_down(k, lbuf.at[p, c]).start()

                    l_cross(k, lbuf.at[p, c]).start()
                    l_mate(p, k).start()

                loop(0, SUB, step)

        if n > head:
            relay(head)
        with jax.named_scope("l_wait"):

            @pl.when(other_l)
            def _():
                def step(k):
                    l_wait(1 - p, c, k)
                    l_mate(1 - p, k).start()

                loop(0, SUB, step)

            loop(0, SUB, lambda k: l_wait(0, 1 - c, k))

            @pl.when(c == 0)
            def _():
                loop(0, SUB, lambda k: l_wait(1, 1, k))

        start_inverse(0)
        start_inverse(1)
        if n > head + 1:
            use(0)

        base = min(head + 1, n)
        inside = min(n_lev, n - base)

        def level_step(i):
            lev = i - base + 1
            relay(
                i,
                (
                    lambda: inverse_level(lev, 0),
                    lambda: inverse_level(lev, 1),
                    lambda: use(i - 2),
                ),
            )

        loop(base, base + inside, level_step)

        def level_rest(lev):
            inverse_level(lev, 0)
            inverse_level(lev, 1)

        loop(inside + 1, n_lev + 1, level_rest)

        def x_first():
            put_x(0, dot3(w[0], mat(lk, 0).astype(F32)))

        def x_second():
            put_x(1, dot3(w[2], mat(lk, 0).astype(F32)) + dot3(w[1], mat(lk, 1).astype(F32)))

        at = base + inside
        if at < n:
            relay(at, (finish_inverse, x_first, x_second, lambda: use(at - 2)))
            at += 1
        else:
            finish_inverse()
            x_first()
            x_second()
        begun = at

        per = 3 if n <= begun + 4 else 1

        def low_step(i):
            j = (i - begun) * per
            relay(i, [functools.partial(lambda d: low(j + d), d) for d in range(per)] + [lambda: use(i - 2)])

        loop(begun, n, low_step)
        lows = per * max(n - begun, 0)
        used = max(n - 2, 0) if n > base else 0

        def send_t():
            loop(used, n, use)
            h0, h1 = mat(h, 0), mat(h, 1)
            tout[1] = dot3(w[1], h1, 0, 0)
            tout[0] = dot3(w[0], h0, 0, 0) + dot3(w[2], h1, 0, 0)
            t_mate().start()

        def upper(a):
            store(a, mat(gv, a).astype(F32))

        @pl.when(jnp.logical_not(top))
        def _():
            send_t()
            with jax.named_scope("w_tmate"):
                t_mate().wait_recv()
            tout[c] += tin[...]
            t_root().start()
            loop(lows, n, low)
            loop(0, loc + 1, upper)

        @pl.when(top)
        def _():
            def s_relay(k):
                with jax.named_scope("w_s"):
                    s_wait(p, k)

                @pl.when(below)
                def _():
                    s_down(k).start()

                s_cross(k).start()

            loop(0, CHUNKS, s_relay)
            send_t()
            loop(lows, n, low)
            loop(0, loc, upper)
            with jax.named_scope("w_s2"):
                loop(0, CHUNKS, lambda k: s_wait(1 - p, k))
            k0, k1 = mat(lk, 0).astype(F32), mat(lk, 1).astype(F32)
            total = mat(gv, loc).astype(F32) - dot3(mat(sbuf, 0), k0) - dot3(mat(sbuf, 1), k1)
            with jax.named_scope("w_tmate2"):
                t_mate().wait_recv()
            total = total - (tout[c] + tin[...])
            with jax.named_scope("w_tslot"):
                for k in range(pairs - 1):
                    rdma(tslot.at[k], tslot.at[k], ts.at[1], tr.at[k], {"row": mate}).wait_recv()
            for k in range(pairs - 1):
                total = total - tslot[k]
            store(loc, total)

        drain = jax.named_scope("drain")
        drain.__enter__()

        def drain_g(t):
            for k in range(SUB):

                @pl.when(below)
                def _():
                    g_down(t, k, gbuf.at[p, t]).wait_send()

                g_cross(t, k, gbuf.at[p, t]).wait_send()

        loop(0, n, drain_g)

        @pl.when(main_l)
        def _():
            def step(k):
                @pl.when(below)
                def _():
                    l_down(k, lbuf.at[p, c]).wait_send()

                l_cross(k, lbuf.at[p, c]).wait_send()
                l_mate(p, k).wait_send()

            loop(0, SUB, step)

        @pl.when(other_l)
        def _():
            loop(0, SUB, lambda k: l_mate(1 - p, k).wait_send())

        t_mate().wait_send()

        @pl.when(jnp.logical_not(top))
        def _():
            t_root().wait_send()

        @pl.when(top)
        def _():
            def drain_s(k):
                @pl.when(below)
                def _():
                    s_down(k).wait_send()

                s_cross(k).wait_send()

            loop(0, CHUNKS, drain_s)

        drain.__exit__(None, None, None)

    @pl.when(panel)
    def _():
        def each(body):
            def run(t):
                for k in range(SUB):
                    body(t, k)

            return run

        send = each(lambda t, k: g_down(t, k, gv.at[first + t]).start() if ring > 1 else None)
        cross_lo = each(lambda t, k: f_cross(t, k).start())
        cross_hi = each(lambda t, k: g_cross(t, k, gv.at[first + t]).start())
        lead = min(2, cut)
        mid = min(cut + 2, n)
        loop(0, head, send)

        @pl.when(p == 0)
        def _():
            loop(cut, mid, cross_lo)

        @pl.when(p == 1)
        def _():
            loop(0, lead, cross_hi)

        with jax.named_scope("gather"):
            gather_rows()

        def send_l():
            def step(k):
                if ring > 1:
                    l_down(k, lk.at[c]).start()
                l_cross(k, lk.at[c]).start()

            loop(0, SUB, step)

        @pl.when(p == 0)
        def _():
            send_l()
            lbuf[0] = lk[...]
            loop(mid, n, cross_lo)

            @pl.when(top & (c == 1))
            def _():
                d_copy(1, gv.at[loc], 0, {"row": mate}).start()
                d_copy(1, gv.at[loc], 1, {"row": mate, "col": twin}).start()
                gd[1] = gv[loc]

        @pl.when(p == 1)
        def _():
            @pl.when(c == 1)
            def _():
                send_l()

            lbuf[1, 1] = lk[1]
            loop(lead, cut, cross_hi)

            @pl.when(top & (c == 1))
            def _():
                d_copy(2, gv.at[loc], 0, {"row": mate}).start()
                d_copy(2, gv.at[loc], 1, {"col": twin}).start()
                gd[2] = gv[loc]

        loop(head, n, send)

        with jax.named_scope("hd"):
            loop(0, n, lambda t: add_h(0, mat(gv, first + t), mat(lv, first + t)))
        h_mate(0).start()

        with jax.named_scope("l_wait"):
            @pl.when((p == 1) | (c == 1))
            def _():
                def step(k):
                    l_wait(1 - p, c, k)
                    l_mate(1 - p, k).start()

                loop(0, SUB, step)

            @pl.when(p == 1)
            def _():
                loop(0, SUB, lambda k: l_wait(0, 1 - c, k))

            @pl.when((p == 0) & (c == 0))
            def _():
                loop(0, SUB, lambda k: l_wait(1, 1, k))

        def reduce_mate(k):
            with jax.named_scope("w_hmate"):
                h_mate(k).wait_recv()
            hsum[k] = h[k, c] + hin[k]

            @pl.when(jnp.logical_not(top))
            def _():
                h_root(k).start()

        def reduce_root(k):
            total = hsum[k]
            for i in range(pairs - 1):
                with jax.named_scope("w_hroot"):
                    rdma(
                        hslot.at[k, i], hslot.at[k, i], hs.at[k, 1], hr.at[k, 3 + i], {"row": mate}
                    ).wait_recv()
                total = total + hslot[k, i]
            hsum[k] = total
            h_twin(k).start()

        start_inverse(0)
        start_inverse(1)
        reduce_mate(0)

        def level(lev):
            inverse_level(lev, 0)
            inverse_level(lev, 1)

        early = (n_lev + 1) // 2
        loop(1, early + 1, level)

        @pl.when(top)
        def _():
            reduce_root(0)

        loop(early + 1, n_lev + 1, level)
        finish_inverse()

        def g_whole(s, t):
            with jax.named_scope("w_x"):
                for k in range(SUB):
                    g_wait(s, t, k)

        @pl.when(p == 0)
        def _():
            def use(t):
                g_whole(1, t)
                add_h(1, mat(gbuf, 1, t), mat(lv, first + t))

            loop(0, cut, use)

        @pl.when(p == 1)
        def _():
            def use(t):
                g_whole(0, t)
                add_h(1, mat(gv, first + t), mat(gbuf, 0, t))

            loop(cut, n, use)

        h_mate(1).start()

        @pl.when(top & (c == 1) & (p == 0))
        def _():
            d_wait(2)
            d_copy(2, gd.at[2], 2, {"row": mate}).start()

        reduce_mate(1)

        @pl.when(top)
        def _():
            reduce_root(1)

        @pl.when(p == 1)
        def _():
            loop(cut, n, cross_hi)

        @pl.when(top)
        def _():
            with jax.named_scope("w_htwin"):
                for k in range(2):
                    rdma(htwin.at[k], htwin.at[k], hs.at[k, 2], hr.at[k, 1], {"col": twin}).wait_recv()
            mine, theirs = hsum[0], htwin[0]
            hfull[0, c] = jnp.where(p == 0, mine, theirs)
            hfull[2, c] = jnp.where(p == 0, theirs, mine)
            hfull[1, c] = hsum[1] + htwin[1]
            for k in range(3):
                h_full(k).start()
            with jax.named_scope("w_hfull"):
                for k in range(3):
                    ref = hfull.at[k, 1 - c]
                    rdma(ref, ref, hs.at[k, 3], hr.at[k, 2], {"row": mate}).wait_recv()

                @pl.when(c == 0)
                def _():
                    d_wait(1)
                    d_wait(2)

            eye = (rows == cols).astype(F32)

            def keep(x):
                return jnp.where(rows >= cols, x, 0.0)

            w66, w77, w76 = w[0], w[1], w[2]
            l77 = mat(lbuf, 1, 1).astype(F32)
            g_here = mat(gv, loc).astype(F32)

            q77 = keep(mat(gd, 2).astype(F32) - dot3(w77, mat(hfull, 2), 0, 0))
            m77 = dot3(l77, q77, 0, 0)
            phi77 = keep(m77) - 0.5 * m77 * eye

            def put_s(s, o):
                sbuf[p] = s.reshape(CHUNKS, tile // CHUNKS, tile)
                if ring > 1:
                    loop(0, CHUNKS, lambda k: s_down(k).start())
                store(loc, o)

            def tri(s):
                return keep(s) - 0.5 * s * eye

            @pl.when((c == 1) & (p == 1))
            def _():
                half77 = dot3(dot3(w77, phi77, 0, 0), w77)
                s = half77 + half77.T
                put_s(s, tri(s))

            @pl.when(jnp.logical_not((c == 1) & (p == 1)))
            def _():
                g76 = jnp.where(c == 1, g_here, mat(gd, 1).astype(F32))
                q76 = g76 - dot3(w77, mat(hfull, 1), 0, 0)
                phi76 = dot3(l77, q76, 0, 0)

                @pl.when((c == 0) & (p == 0))
                def _():
                    t66 = dot3(w66, mat(hfull, 0), 0, 0) + dot3(w76, mat(hfull, 1), 0, 0)
                    q66 = keep(g_here - t66)
                    l66, l76 = mat(lbuf, 0, 0).astype(F32), mat(lbuf, 0, 1).astype(F32)
                    m66 = dot3(l66, q66, 0, 0) + dot3(l76, q76, 0, 0)
                    phi66 = keep(m66) - 0.5 * m66 * eye
                    inner = dot3(phi76, w66) + dot3(phi77, w76)
                    half66 = dot3(w66, dot3(phi66, w66), 0, 0) + dot3(w76, inner, 0, 0)
                    s = half66 + half66.T
                    put_s(s, tri(s))

                @pl.when(jnp.logical_not((c == 0) & (p == 0)))
                def _():
                    inner = dot3(phi76, w66) + dot3(phi77 + phi77.T, w76)

                    @pl.when(c == 1)
                    def _():
                        s = dot3(w77, inner, 0, 0)
                        put_s(s, s)

                    @pl.when(c == 0)
                    def _():
                        put_s(dot3(inner, w77, 0, 0), jnp.zeros((tile, tile), F32))

        zero = jnp.zeros((tile, tile), F32)
        loop(0, loc, lambda a: store(a, zero))

        @pl.when(jnp.logical_not(top))
        def _():
            store(loc, zero)

        put_x(1, jnp.where(p == 0, -w[2], -w[1]))

        with jax.named_scope("low"):

            @pl.when(p == 0)
            def _():
                put_x(0, -w[0])

                def low(t):
                    total = times_x(zero, 0, mat(gv, first + t))
                    store(first + t, times_x(total, 1, mat(gbuf, 1, t)))

                def late(t):
                    g_whole(1, t)
                    low(t)

                loop(0, cut, low)
                loop(cut, n, late)

            @pl.when(p == 1)
            def _():
                loop(0, n, lambda t: store(first + t, times_x(zero, 1, mat(gv, first + t))))

        drain = jax.named_scope("drain")
        drain.__enter__()

        def drain_l():
            def step(k):
                if ring > 1:
                    l_down(k, lk.at[c]).wait_send()
                l_cross(k, lk.at[c]).wait_send()

            loop(0, SUB, step)

        @pl.when(p == 0)
        def _():
            loop(cut, n, each(lambda t, k: f_cross(t, k).wait_send()))
            drain_l()

            @pl.when(top & (c == 1))
            def _():
                d_copy(1, gv.at[loc], 0, {"row": mate}).wait_send()
                d_copy(1, gv.at[loc], 1, {"row": mate, "col": twin}).wait_send()
                d_copy(2, gd.at[2], 2, {"row": mate}).wait_send()

        @pl.when(p == 1)
        def _():
            loop(0, n, each(lambda t, k: g_cross(t, k, gv.at[first + t]).wait_send()))

            @pl.when(c == 1)
            def _():
                drain_l()

            @pl.when(top & (c == 1))
            def _():
                d_copy(2, gv.at[loc], 0, {"row": mate}).wait_send()
                d_copy(2, gv.at[loc], 1, {"col": twin}).wait_send()

        @pl.when((p == 1) | (c == 1))
        def _():
            loop(0, SUB, lambda k: l_mate(1 - p, k).wait_send())

        if ring > 1:
            loop(0, n, each(lambda t, k: g_down(t, k, gv.at[first + t]).wait_send()))
        for k in range(2):
            h_mate(k).wait_send()

            @pl.when(jnp.logical_not(top))
            def _():
                h_root(k).wait_send()

            @pl.when(top)
            def _():
                h_twin(k).wait_send()

        @pl.when(top)
        def _():
            for k in range(3):
                h_full(k).wait_send()
            if ring > 1:
                loop(0, CHUNKS, lambda k: s_down(k).wait_send())

        drain.__exit__(None, None, None)

    @pl.when(top)
    def _():
        for k in range(pairs - 1):
            k_star(k).wait_send()
        k_mate(lv.at[loc]).wait_send()

    @pl.when(jnp.logical_not(top))
    def _():
        k_mate(lk.at[c]).wait_send()


def panel(factor, grad, n_row, n_col, first):
    rows_here, tile = factor.shape[0], factor.shape[1]
    n = rows_here - first
    half = tile // 2
    pairs = n_row // 2
    sub = (SUB, tile // SUB, tile)
    hbm = pl.BlockSpec(memory_space=pltpu.HBM)
    dma = pltpu.SemaphoreType.DMA
    return pl.pallas_call(
        functools.partial(panel_kernel, n_row, n_col),
        out_shape=jax.ShapeDtypeStruct((rows_here, tile * tile // LANE, LANE), F32),
        in_specs=[hbm, hbm],
        out_specs=pl.BlockSpec(memory_space=pltpu.VMEM),
        scratch_shapes=[
            pltpu.VMEM((rows_here, *sub), BF16),
            pltpu.VMEM((rows_here, *sub), BF16),
            pltpu.VMEM((2, n, *sub), BF16),
            pltpu.VMEM((2, tile, tile), BF16),
            pltpu.VMEM((2, tile, tile), BF16),
            pltpu.VMEM((2, *sub), BF16),
            pltpu.VMEM((2, 2, *sub), BF16),
            pltpu.VMEM((3, tile, tile), F32),
            pltpu.VMEM((2, 2, half, tile), F32),
            pltpu.VMEM((2, tile, tile), F32),
            pltpu.VMEM((tile, tile), F32),
            pltpu.VMEM((pairs, tile, tile), F32),
            pltpu.VMEM((2, half, tile), F32),
            pltpu.VMEM((2, half, tile), F32),
            pltpu.VMEM((2, pairs, half, tile), F32),
            pltpu.VMEM((2, half, tile), F32),
            pltpu.VMEM((3, 2, half, tile), F32),
            pltpu.VMEM((3, *sub), BF16),
            pltpu.VMEM((2, CHUNKS, tile // CHUNKS, tile), F32),
            dma((5,)),
            dma((n, SUB, 2)),
            dma((2, n, SUB)),
            dma((2, SUB, 3)),
            dma((2, 2, SUB)),
            dma((pairs + 1,)),
            dma((2,)),
            dma((2,)),
            dma((pairs + 1,)),
            dma((3, 4)),
            dma((3, 3 + pairs)),
            dma((3,)),
            dma((3,)),
            dma((CHUNKS, 2)),
            dma((2, CHUNKS)),
        ],
        compiler_params=pltpu.CompilerParams(
            collective_id=0, has_side_effects=True, vmem_limit_bytes=VMEM
        ),
        name="panel",
    )(
        pltpu.with_memory_space_constraint(factor.reshape(rows_here, *sub), pltpu.HBM),
        pltpu.with_memory_space_constraint(grad.reshape(rows_here, *sub), pltpu.HBM),
    )


def per_device(l_saved, l_grad):
    rows_here, tile = l_saved.shape[0], l_saved.shape[2]
    n_row = lax.axis_size("row")
    n_col = lax.axis_size("col")
    assert n_col % n_row == 0 and n_row % 2 == 0 and tile % (SUB * 16) == 0
    first = n_col // n_row
    factor = l_saved.reshape(rows_here, tile, tile)
    grad = l_grad.reshape(rows_here, tile, tile)
    lin = panel(factor, grad, n_row, n_col, first)
    return lin.reshape(l_grad.shape)


def solution(mesh):
    spec = P(None, "row", None, "col", None)
    return jax.shard_map(
        per_device, mesh=mesh, in_specs=(spec, spec), out_specs=spec, check_vma=False
    )
```

```python
import functools

import jax
import jax.numpy as jnp
from jax import lax
from jax.experimental import pallas as pl
from jax.experimental.pallas import tpu as pltpu
from jax.sharding import PartitionSpec as P

F32 = jnp.float32
BF16 = jnp.bfloat16
HIGH3 = lax.Precision.HIGH
MESH = pl.DeviceIdType.MESH
CHUNKS = 8
SUB = 4
LANE = 128
VMEM = 40 * 1024 * 1024


def dot3(a, b, ca=1, cb=0):
    return lax.dot_general(
        a, b, (((ca,), (cb,)), ((), ())), precision=HIGH3, preferred_element_type=F32
    )


def outer(a, b):
    return lax.dot_general(a, b, (((0,), (0,)), ((), ())), preferred_element_type=F32)


def panel_kernel(
    n_row,
    n_col,
    l_hbm,
    g_hbm,
    lin,
    lv,
    gv,
    gbuf,
    xh,
    xl,
    lk,
    lbuf,
    w,
    h,
    tout,
    tin,
    tslot,
    hin,
    hsum,
    hslot,
    htwin,
    hfull,
    gd,
    sbuf,
    vs,
    gs,
    gm,
    gx,
    ls,
    lm,
    lx,
    lf,
    ks,
    kr,
    ts,
    tr,
    hs,
    hr,
    hq,
    ds,
    dr,
    ss,
    sm,
    sx,
):
    held, tile = lv.shape[0], lv.shape[3]
    half = tile // 2
    n = gbuf.shape[1]
    first = held - n
    loc = first - 1
    ring = n_col // 2
    cut = n // 2
    head = min(2, n)
    pairs = n_row // 2
    parts = tile // LANE

    row = lax.axis_index("row")
    col = lax.axis_index("col")
    q, p = col // 2, col % 2
    y, c = row // 2, row % 2
    panel = q == ring - 1
    top = y == pairs - 1
    below = q > 0
    lower = jnp.maximum(col - 2, 0)
    twin = 2 * q + 1 - p
    mate = 2 * y + 1 - c
    root = n_row - 2 + c

    rows = lax.broadcasted_iota(jnp.int32, (tile, tile), 0)
    cols = lax.broadcasted_iota(jnp.int32, (tile, tile), 1)

    def rdma(src, dst, s_sem, r_sem, dev):
        return pltpu.make_async_remote_copy(
            src_ref=src, dst_ref=dst, send_sem=s_sem, recv_sem=r_sem, device_id=dev, device_id_type=MESH
        )

    def loop(a, b, body):
        def step(i, carry):
            body(i)
            return carry

        if a < b:
            lax.fori_loop(a, b, step, 0)

    def load(src, dst, k, a, b):
        return pltpu.make_async_copy(src.at[pl.ds(a, b - a)], dst.at[pl.ds(a, b - a)], vs.at[k])

    spans = [
        (l_hbm, lv, 0, loc, first),
        (g_hbm, gv, 1, first, first + head),
        (l_hbm, lv, 2, first, held),
        (g_hbm, gv, 3, first + head, held),
        (g_hbm, gv, 4, 0, first),
    ]
    loads = {span[2]: load(*span) for span in spans if span[3] < span[4]}
    for cp in loads.values():
        cp.start()

    def loaded(*ks):
        for k in ks:
            if k in loads:
                loads[k].wait()

    barrier = pltpu.get_barrier_semaphore()

    def greet(dev):
        pl.semaphore_signal(barrier, inc=1, device_id=dev, device_id_type=MESH)

    greet({"col": twin})
    greet({"row": mate})

    @pl.when(below)
    def _():
        greet({"col": col - 2})

    @pl.when(jnp.logical_not(panel))
    def _():
        greet({"col": col + 2})

    @pl.when(jnp.logical_not(top))
    def _():
        greet({"row": root})

    @pl.when(top)
    def _():
        for k in range(pairs - 1):
            greet({"row": 2 * k + c})

    @pl.when(top & panel)
    def _():
        greet({"row": mate, "col": twin})

    heard = (
        2
        + below.astype(jnp.int32)
        + jnp.logical_not(panel).astype(jnp.int32)
        + jnp.where(top, pairs - 1, 1)
        + (top & panel).astype(jnp.int32)
    )
    with jax.named_scope("barrier"):
        pl.semaphore_wait(barrier, heard)

    loaded(0)

    def mat(ref, *at):
        return ref[at].reshape(tile, tile)

    def g_down(t, k, src):
        return rdma(src.at[k], gbuf.at[p, t, k], gs.at[0], gm.at[t, k], {"col": lower})

    def g_cross(t, k, src):
        return rdma(src.at[k], gbuf.at[p, t, k], gs.at[1], gx.at[t], {"col": twin})

    def f_cross(t, k):
        return rdma(lv.at[first + t, k], gbuf.at[0, t, k], gs.at[1], gx.at[t], {"col": twin})

    def g_main(t, k):
        ref = gbuf.at[p, t, k]
        rdma(ref, ref, gs.at[0], gm.at[t, k], {"col": twin}).wait_recv()

    def g_twin(t):
        ref = gbuf.at[1 - p, t]
        rdma(ref, ref, gs.at[1], gx.at[t], {"col": twin}).wait_recv()

    def g_sent(k, ref):
        rdma(ref, ref, gs.at[k], gx.at[0], {"col": twin}).wait_send()

    def l_down(k, src):
        return rdma(src.at[k], lbuf.at[p, c, k], ls.at[0], lm.at[k], {"col": lower})

    def l_cross(k, src):
        return rdma(src.at[k], lbuf.at[p, c, k], ls.at[1], lx.at[k], {"col": twin})

    def l_mate(s, k):
        ref = lbuf.at[s, c, k]
        return rdma(ref, ref, ls.at[2 + s], lf.at[s], {"row": mate})

    def l_main(k):
        ref = lbuf.at[p, c, k]
        rdma(ref, ref, ls.at[0], lm.at[k], {"col": twin}).wait_recv()

    def l_twin(k):
        ref = lbuf.at[1 - p, c, k]
        rdma(ref, ref, ls.at[1], lx.at[k], {"col": twin}).wait_recv()

    def l_full(s):
        ref = lbuf.at[s, 1 - c]
        rdma(ref, ref, ls.at[2], lf.at[s], {"row": mate}).wait_recv()

    def l_sent(k):
        ref = lbuf.at[0, 0]
        rdma(ref, ref, ls.at[k], lf.at[0], {"row": mate}).wait_send()

    def k_star(k):
        return rdma(lv.at[loc], lk.at[c], ks.at[k], kr.at[c], {"row": 2 * k + c})

    def k_mate(src):
        return rdma(src, lk.at[c], ks.at[pairs], kr.at[c], {"row": mate})

    def k_wait(i):
        rdma(lk.at[i], lk.at[i], ks.at[pairs], kr.at[i], {"row": mate}).wait_recv()

    def t_mate():
        return rdma(tout.at[1 - c], tin, ts.at[0], tr.at[pairs], {"row": mate})

    def t_root():
        return rdma(tout.at[c], tslot.at[y], ts.at[1], tr.at[y], {"row": root})

    def h_mate(k):
        return rdma(h.at[k, 1 - c], hin.at[k], hs.at[k], hr.at[k], {"row": mate})

    def h_root(k):
        return rdma(hsum.at[k], hslot.at[k, y], hs.at[2 + k], hq.at[k, y], {"row": root})

    def h_twin(k):
        return rdma(hsum.at[k], htwin.at[k], hs.at[2 + k], hr.at[2 + k], {"col": twin})

    def h_full():
        return rdma(hfull.at[c], hfull.at[c], hs.at[4], hr.at[4], {"row": mate})

    def d_copy(k, src, i, dev):
        return rdma(src, gd.at[k], ds.at[i], dr.at[k], dev)

    def d_wait(k):
        d_copy(k, gd.at[k], 0, {"row": mate}).wait_recv()

    def s_down(k):
        return rdma(sbuf.at[p, k], sbuf.at[p, k], ss.at[0], sm.at[k], {"col": lower})

    def s_cross(k):
        return rdma(sbuf.at[p, k], sbuf.at[p, k], ss.at[1], sx.at[0], {"col": twin})

    def s_main(k):
        s_down(k).wait_recv()

    def s_twin():
        ref = sbuf.at[1 - p]
        rdma(ref, ref, ss.at[1], sx.at[0], {"col": twin}).wait_recv()

    def s_sent(k):
        ref = sbuf.at[p]
        rdma(ref, ref, ss.at[k], sx.at[0], {"col": twin}).wait_send()

    @pl.when(top)
    def _():
        for k in range(pairs - 1):
            k_star(k).start()
        k_mate(lv.at[loc]).start()
        lk[c] = lv[loc]

    def gather_rows():
        @pl.when(jnp.logical_not(top))
        def _():
            k_wait(c)
            k_mate(lk.at[c]).start()

        k_wait(1 - c)

    def start_inverse(k):
        d = mat(lbuf, k, k).astype(F32)
        e = (rows == cols).astype(F32)
        on = d * e
        rc = 1.0 / jnp.sum(on, axis=1, keepdims=True)
        rr = 1.0 / jnp.sum(on, axis=0, keepdims=True)
        off = ((rows & 1) == 1) & (cols == rows - 1)
        w[k] = e * rr - rc * jnp.where(off, d, 0.0) * rr

    n_lev = tile.bit_length() - 2

    def inverse_level(sh, k):
        off = ((jnp.right_shift(rows, sh) & 1) == 1) & (
            jnp.right_shift(cols, sh) == jnp.right_shift(rows, sh) - 1
        )
        part = jnp.where(off, mat(lbuf, k, k).astype(F32), 0.0)
        cur = w[k]
        w[k] = cur - dot3(cur, dot3(part, cur))

    def finish_inverse():
        w[2] = -dot3(w[1], dot3(mat(lbuf, 0, 1).astype(F32), w[0]))

    def put_x(i, x):
        hi = x.astype(BF16)
        xh[i] = hi
        xl[i] = (x - hi.astype(F32)).astype(BF16)

    def store(a, value):
        for b in range(parts):
            lin[a, pl.ds(b, tile, stride=parts), :] = value[:, b * LANE : (b + 1) * LANE]

    h[...] = jnp.zeros_like(h)

    def add_h(k, left, right):
        h[k] += outer(left, right).reshape(2, half, tile)

    def times_x(total, i, g):
        for part in (xl, xh):
            total = total - jnp.dot(g, part[i], preferred_element_type=F32)
        return total

    @pl.when(jnp.logical_not(panel))
    def _():
        loaded(1, 2, 3, 4)

        def relay(t, work=()):
            for k in range(SUB):
                with jax.named_scope("w_main"):
                    g_main(t, k)

                @pl.when(below)
                def _():
                    g_down(t, k, gbuf.at[p, t]).start()

                g_cross(t, k, gbuf.at[p, t]).start()
                if k < len(work):
                    work[k]()

        def use(t):
            with jax.named_scope("w_cross"):
                g_twin(t)
            right = mat(lv, first + t)
            add_h(0, mat(gbuf, 0, t), right)
            add_h(1, mat(gbuf, 1, t), right)

        def low(t):
            total = mat(gv, first + t).astype(F32)
            for s in range(2):
                total = times_x(total, s, mat(gbuf, s, t))
            store(first + t, total)

        main_l = (p == 0) | (c == 1)
        other_l = (p == 1) | (c == 1)

        for t in range(head):
            relay(t)
        with jax.named_scope("gather"):
            gather_rows()

        with jax.named_scope("l_relay"):

            @pl.when(main_l)
            def _():
                def step(k):
                    l_main(k)

                    @pl.when(below)
                    def _():
                        l_down(k, lbuf.at[p, c]).start()

                    l_cross(k, lbuf.at[p, c]).start()
                    l_mate(p, k).start()

                loop(0, SUB, step)

        if n > head:
            relay(head)
        with jax.named_scope("l_wait"):

            @pl.when(other_l)
            def _():
                def step(k):
                    l_twin(k)
                    l_mate(1 - p, k).start()

                loop(0, SUB, step)

            l_full(0)

            @pl.when(c == 0)
            def _():
                l_full(1)

        start_inverse(0)
        start_inverse(1)
        if n > head + 1:
            use(0)

        base = min(head + 1, n)
        inside = min(n_lev, n - base)

        def level_step(i):
            lev = i - base + 1
            relay(
                i,
                (
                    lambda: inverse_level(lev, 0),
                    lambda: inverse_level(lev, 1),
                    lambda: use(i - 2),
                ),
            )

        loop(base, base + inside, level_step)

        def level_rest(lev):
            inverse_level(lev, 0)
            inverse_level(lev, 1)

        loop(inside + 1, n_lev + 1, level_rest)

        def x_first():
            put_x(0, dot3(w[0], mat(lk, 0).astype(F32)))

        def x_second():
            put_x(1, dot3(w[2], mat(lk, 0).astype(F32)) + dot3(w[1], mat(lk, 1).astype(F32)))

        at = base + inside
        if at < n:
            relay(at, (finish_inverse, x_first, x_second, lambda: use(at - 2)))
            at += 1
        else:
            finish_inverse()
            x_first()
            x_second()
        begun = at

        per = 3 if n <= begun + 4 else 1

        def low_step(i):
            j = (i - begun) * per
            relay(i, [functools.partial(lambda d: low(j + d), d) for d in range(per)] + [lambda: use(i - 2)])

        loop(begun, n, low_step)
        lows = per * max(n - begun, 0)
        used = max(n - 2, 0) if n > base else 0

        def send_t():
            loop(used, n, use)
            h0, h1 = mat(h, 0), mat(h, 1)
            tout[1] = dot3(w[1], h1, 0, 0)
            tout[0] = dot3(w[0], h0, 0, 0) + dot3(w[2], h1, 0, 0)
            t_mate().start()

        def upper(a):
            store(a, mat(gv, a).astype(F32))

        @pl.when(jnp.logical_not(top))
        def _():
            send_t()
            with jax.named_scope("w_tmate"):
                t_mate().wait_recv()
            tout[c] += tin[...]
            t_root().start()
            loop(lows, n, low)
            loop(0, loc + 1, upper)

        @pl.when(top)
        def _():
            def s_relay(k):
                with jax.named_scope("w_s"):
                    s_main(k)

                @pl.when(below)
                def _():
                    s_down(k).start()

                s_cross(k).start()

            loop(0, CHUNKS, s_relay)
            send_t()
            loop(lows, n, low)
            loop(0, loc, upper)
            with jax.named_scope("w_s2"):
                s_twin()
            k0, k1 = mat(lk, 0).astype(F32), mat(lk, 1).astype(F32)
            total = mat(gv, loc).astype(F32) - dot3(mat(sbuf, 0), k0) - dot3(mat(sbuf, 1), k1)
            with jax.named_scope("w_tmate2"):
                t_mate().wait_recv()
            total = total - (tout[c] + tin[...])
            with jax.named_scope("w_tslot"):
                for k in range(pairs - 1):
                    rdma(tslot.at[k], tslot.at[k], ts.at[1], tr.at[k], {"row": mate}).wait_recv()
            for k in range(pairs - 1):
                total = total - tslot[k]
            store(loc, total)

        drain = jax.named_scope("drain")
        drain.__enter__()

        g_sent(1, gbuf.at[p])

        @pl.when(below)
        def _():
            g_sent(0, gbuf.at[p])

        @pl.when(main_l)
        def _():
            l_sent(1)
            l_sent(2 + p)

            @pl.when(below)
            def _():
                l_sent(0)

        @pl.when(other_l)
        def _():
            l_sent(3 - p)

        t_mate().wait_send()

        @pl.when(jnp.logical_not(top))
        def _():
            t_root().wait_send()

        @pl.when(top)
        def _():
            s_sent(1)

            @pl.when(below)
            def _():
                s_sent(0)

        drain.__exit__(None, None, None)

    @pl.when(panel)
    def _():
        def each(body):
            def run(t):
                for k in range(SUB):
                    body(t, k)

            return run

        send = each(lambda t, k: g_down(t, k, gv.at[first + t]).start() if ring > 1 else None)
        cross_lo = each(lambda t, k: f_cross(t, k).start())
        cross_hi = each(lambda t, k: g_cross(t, k, gv.at[first + t]).start())
        lead = min(2, cut)
        mid = min(cut + 2, n)
        loaded(1)
        loop(0, head, send)

        @pl.when(p == 0)
        def _():
            loaded(2)
            loop(cut, mid, cross_lo)

        @pl.when(p == 1)
        def _():
            loop(0, lead, cross_hi)
            loaded(2)

        loaded(3, 4)
        with jax.named_scope("gather"):
            gather_rows()

        def send_l():
            def step(k):
                if ring > 1:
                    l_down(k, lk.at[c]).start()
                l_cross(k, lk.at[c]).start()

            loop(0, SUB, step)

        @pl.when(p == 0)
        def _():
            send_l()
            lbuf[0] = lk[...]
            loop(mid, n, cross_lo)

            @pl.when(top & (c == 1))
            def _():
                d_copy(1, gv.at[loc], 0, {"row": mate}).start()
                d_copy(1, gv.at[loc], 1, {"row": mate, "col": twin}).start()
                gd[1] = gv[loc]

        @pl.when(p == 1)
        def _():
            @pl.when(c == 1)
            def _():
                send_l()

            lbuf[1, 1] = lk[1]
            loop(lead, cut, cross_hi)

            @pl.when(top & (c == 1))
            def _():
                d_copy(2, gv.at[loc], 0, {"row": mate}).start()
                d_copy(2, gv.at[loc], 1, {"col": twin}).start()
                gd[2] = gv[loc]

        loop(head, n, send)

        with jax.named_scope("hd"):
            loop(0, n, lambda t: add_h(0, mat(gv, first + t), mat(lv, first + t)))
        h_mate(0).start()

        with jax.named_scope("l_wait"):
            @pl.when((p == 1) | (c == 1))
            def _():
                def step(k):
                    l_twin(k)
                    l_mate(1 - p, k).start()

                loop(0, SUB, step)

            @pl.when(p == 1)
            def _():
                l_full(0)

            @pl.when((p == 0) & (c == 0))
            def _():
                l_full(1)

        def reduce_mate(k):
            with jax.named_scope("w_hmate"):
                h_mate(k).wait_recv()
            hsum[k] = h[k, c] + hin[k]

            @pl.when(jnp.logical_not(top))
            def _():
                h_root(k).start()

        def reduce_root(k):
            total = hsum[k]
            for i in range(pairs - 1):
                with jax.named_scope("w_hroot"):
                    ref = hslot.at[k, i]
                    rdma(ref, ref, hs.at[2 + k], hq.at[k, i], {"row": mate}).wait_recv()
                total = total + hslot[k, i]
            hsum[k] = total
            h_twin(k).start()

        start_inverse(0)
        start_inverse(1)
        reduce_mate(0)

        def level(lev):
            inverse_level(lev, 0)
            inverse_level(lev, 1)

        early = (n_lev + 1) // 2
        loop(1, early + 1, level)

        @pl.when(top)
        def _():
            reduce_root(0)

        loop(early + 1, n_lev + 1, level)
        finish_inverse()

        @pl.when(p == 0)
        def _():
            def use(t):
                with jax.named_scope("w_x"):
                    g_twin(t)
                add_h(1, mat(gbuf, 1, t), mat(lv, first + t))

            loop(0, cut, use)

        @pl.when(p == 1)
        def _():
            def use(t):
                with jax.named_scope("w_x"):
                    g_twin(t)
                add_h(1, mat(gv, first + t), mat(gbuf, 0, t))

            loop(cut, n, use)

        h_mate(1).start()

        @pl.when(top & (c == 1) & (p == 0))
        def _():
            d_wait(2)
            d_copy(2, gd.at[2], 2, {"row": mate}).start()

        reduce_mate(1)

        @pl.when(top)
        def _():
            reduce_root(1)

        @pl.when(p == 1)
        def _():
            loop(cut, n, cross_hi)

        @pl.when(top)
        def _():
            with jax.named_scope("w_htwin"):
                for k in range(2):
                    h_twin(k).wait_recv()
            mine, theirs = hsum[0], htwin[0]
            hfull[c, 0] = jnp.where(p == 0, mine, theirs)
            hfull[c, 2] = jnp.where(p == 0, theirs, mine)
            hfull[c, 1] = hsum[1] + htwin[1]
            h_full().start()
            with jax.named_scope("w_hfull"):
                ref = hfull.at[1 - c]
                rdma(ref, ref, hs.at[4], hr.at[4], {"row": mate}).wait_recv()

                @pl.when(c == 0)
                def _():
                    d_wait(1)
                    d_wait(2)

            eye = (rows == cols).astype(F32)

            def keep(x):
                return jnp.where(rows >= cols, x, 0.0)

            w66, w77, w76 = w[0], w[1], w[2]
            l77 = mat(lbuf, 1, 1).astype(F32)
            g_here = mat(gv, loc).astype(F32)

            def full(k):
                return jnp.concatenate([hfull[0, k], hfull[1, k]], 0)

            q77 = keep(mat(gd, 2).astype(F32) - dot3(w77, full(2), 0, 0))
            m77 = dot3(l77, q77, 0, 0)
            phi77 = keep(m77) - 0.5 * m77 * eye

            def put_s(s, o):
                sbuf[p] = s.reshape(CHUNKS, tile // CHUNKS, tile)
                if ring > 1:
                    loop(0, CHUNKS, lambda k: s_down(k).start())
                store(loc, o)

            def tri(s):
                return keep(s) - 0.5 * s * eye

            @pl.when((c == 1) & (p == 1))
            def _():
                half77 = dot3(dot3(w77, phi77, 0, 0), w77)
                s = half77 + half77.T
                put_s(s, tri(s))

            @pl.when(jnp.logical_not((c == 1) & (p == 1)))
            def _():
                g76 = jnp.where(c == 1, g_here, mat(gd, 1).astype(F32))
                q76 = g76 - dot3(w77, full(1), 0, 0)
                phi76 = dot3(l77, q76, 0, 0)

                @pl.when((c == 0) & (p == 0))
                def _():
                    t66 = dot3(w66, full(0), 0, 0) + dot3(w76, full(1), 0, 0)
                    q66 = keep(g_here - t66)
                    l66, l76 = mat(lbuf, 0, 0).astype(F32), mat(lbuf, 0, 1).astype(F32)
                    m66 = dot3(l66, q66, 0, 0) + dot3(l76, q76, 0, 0)
                    phi66 = keep(m66) - 0.5 * m66 * eye
                    inner = dot3(phi76, w66) + dot3(phi77, w76)
                    half66 = dot3(w66, dot3(phi66, w66), 0, 0) + dot3(w76, inner, 0, 0)
                    s = half66 + half66.T
                    put_s(s, tri(s))

                @pl.when(jnp.logical_not((c == 0) & (p == 0)))
                def _():
                    inner = dot3(phi76, w66) + dot3(phi77 + phi77.T, w76)

                    @pl.when(c == 1)
                    def _():
                        s = dot3(w77, inner, 0, 0)
                        put_s(s, s)

                    @pl.when(c == 0)
                    def _():
                        put_s(dot3(inner, w77, 0, 0), jnp.zeros((tile, tile), F32))

        zero = jnp.zeros((tile, tile), F32)
        loop(0, loc, lambda a: store(a, zero))

        @pl.when(jnp.logical_not(top))
        def _():
            store(loc, zero)

        put_x(1, jnp.where(p == 0, -w[2], -w[1]))

        with jax.named_scope("low"):

            @pl.when(p == 0)
            def _():
                put_x(0, -w[0])

                def low(t):
                    total = times_x(zero, 0, mat(gv, first + t))
                    store(first + t, times_x(total, 1, mat(gbuf, 1, t)))

                def late(t):
                    g_twin(t)
                    low(t)

                loop(0, cut, low)
                loop(cut, n, late)

            @pl.when(p == 1)
            def _():
                loop(0, n, lambda t: store(first + t, times_x(zero, 1, mat(gv, first + t))))

        drain = jax.named_scope("drain")
        drain.__enter__()

        @pl.when(p == 0)
        def _():
            g_sent(1, gbuf.at[0, pl.ds(cut, n - cut)])

            @pl.when(top & (c == 1))
            def _():
                d_copy(1, gv.at[loc], 0, {"row": mate}).wait_send()
                d_copy(1, gv.at[loc], 1, {"row": mate, "col": twin}).wait_send()
                d_copy(2, gd.at[2], 2, {"row": mate}).wait_send()

        @pl.when(p == 1)
        def _():
            g_sent(1, gbuf.at[1])

            @pl.when(top & (c == 1))
            def _():
                d_copy(2, gv.at[loc], 0, {"row": mate}).wait_send()
                d_copy(2, gv.at[loc], 1, {"col": twin}).wait_send()

        @pl.when((p == 0) | (c == 1))
        def _():
            l_sent(1)
            if ring > 1:
                l_sent(0)

        @pl.when((p == 1) | (c == 1))
        def _():
            l_sent(3 - p)

        if ring > 1:
            g_sent(0, gbuf.at[p])
        for k in range(2):
            h_mate(k).wait_send()

            @pl.when(jnp.logical_not(top))
            def _():
                h_root(k).wait_send()

            @pl.when(top)
            def _():
                h_twin(k).wait_send()

        @pl.when(top)
        def _():
            h_full().wait_send()
            if ring > 1:
                s_sent(0)

        drain.__exit__(None, None, None)

    @pl.when(top)
    def _():
        for k in range(pairs - 1):
            k_star(k).wait_send()
        k_mate(lv.at[loc]).wait_send()

    @pl.when(jnp.logical_not(top))
    def _():
        k_mate(lk.at[c]).wait_send()


def panel(factor, grad, n_row, n_col, first):
    rows_here, tile = factor.shape[0], factor.shape[1]
    n = rows_here - first
    half = tile // 2
    pairs = n_row // 2
    sub = (SUB, tile // SUB, tile)
    hbm = pl.BlockSpec(memory_space=pltpu.HBM)
    dma = pltpu.SemaphoreType.DMA
    return pl.pallas_call(
        functools.partial(panel_kernel, n_row, n_col),
        out_shape=jax.ShapeDtypeStruct((rows_here, tile * tile // LANE, LANE), F32),
        in_specs=[hbm, hbm],
        out_specs=pl.BlockSpec(memory_space=pltpu.VMEM),
        scratch_shapes=[
            pltpu.VMEM((rows_here, *sub), BF16),
            pltpu.VMEM((rows_here, *sub), BF16),
            pltpu.VMEM((2, n, *sub), BF16),
            pltpu.VMEM((2, tile, tile), BF16),
            pltpu.VMEM((2, tile, tile), BF16),
            pltpu.VMEM((2, *sub), BF16),
            pltpu.VMEM((2, 2, *sub), BF16),
            pltpu.VMEM((3, tile, tile), F32),
            pltpu.VMEM((2, 2, half, tile), F32),
            pltpu.VMEM((2, tile, tile), F32),
            pltpu.VMEM((tile, tile), F32),
            pltpu.VMEM((pairs, tile, tile), F32),
            pltpu.VMEM((2, half, tile), F32),
            pltpu.VMEM((2, half, tile), F32),
            pltpu.VMEM((2, pairs, half, tile), F32),
            pltpu.VMEM((2, half, tile), F32),
            pltpu.VMEM((2, 3, half, tile), F32),
            pltpu.VMEM((3, *sub), BF16),
            pltpu.VMEM((2, CHUNKS, tile // CHUNKS, tile), F32),
            dma((5,)),
            dma((2,)),
            dma((n, SUB)),
            dma((n,)),
            dma((4,)),
            dma((SUB,)),
            dma((SUB,)),
            dma((2,)),
            dma((pairs + 1,)),
            dma((2,)),
            dma((2,)),
            dma((pairs + 1,)),
            dma((5,)),
            dma((5,)),
            dma((2, pairs)),
            dma((3,)),
            dma((3,)),
            dma((2,)),
            dma((CHUNKS,)),
            dma((1,)),
        ],
        compiler_params=pltpu.CompilerParams(
            collective_id=0, has_side_effects=True, vmem_limit_bytes=VMEM
        ),
        name="panel",
    )(
        pltpu.with_memory_space_constraint(factor.reshape(rows_here, *sub), pltpu.HBM),
        pltpu.with_memory_space_constraint(grad.reshape(rows_here, *sub), pltpu.HBM),
    )


def per_device(l_saved, l_grad):
    rows_here, tile = l_saved.shape[0], l_saved.shape[2]
    n_row = lax.axis_size("row")
    n_col = lax.axis_size("col")
    assert n_col % n_row == 0 and n_row % 2 == 0 and tile % (SUB * 16) == 0
    first = n_col // n_row
    factor = l_saved.reshape(rows_here, tile, tile)
    grad = l_grad.reshape(rows_here, tile, tile)
    lin = panel(factor, grad, n_row, n_col, first)
    return lin.reshape(l_grad.shape)


def solution(mesh):
    spec = P(None, "row", None, "col", None)
    return jax.shard_map(
        per_device, mesh=mesh, in_specs=(spec, spec), out_specs=spec, check_vma=False
    )
```

```python
import functools

import jax
import jax.numpy as jnp
from jax import lax
from jax.experimental import pallas as pl
from jax.experimental.pallas import tpu as pltpu
from jax.sharding import PartitionSpec as P

F32 = jnp.float32
BF16 = jnp.bfloat16
HIGH3 = lax.Precision.HIGH
MESH = pl.DeviceIdType.MESH
CHUNKS = 8
SUB = 4
LANE = 128
VMEM = 40 * 1024 * 1024


def dot3(a, b, ca=1, cb=0):
    return lax.dot_general(
        a, b, (((ca,), (cb,)), ((), ())), precision=HIGH3, preferred_element_type=F32
    )


def outer(a, b):
    return lax.dot_general(a, b, (((0,), (0,)), ((), ())), preferred_element_type=F32)


def panel_kernel(
    n_row,
    n_col,
    l_hbm,
    g_hbm,
    lin,
    lv,
    gv,
    gbuf,
    xh,
    xl,
    lk,
    lbuf,
    w,
    h,
    tout,
    tin,
    tslot,
    hin,
    hsum,
    hslot,
    htwin,
    hfull,
    gd,
    sbuf,
    vs,
    gs,
    gm,
    gx,
    ls,
    lm,
    lx,
    lf,
    lp,
    ks,
    kr,
    ts,
    tr,
    hs,
    hr,
    hq,
    ds,
    dr,
    ss,
    sm,
    sx,
):
    held, tile = lv.shape[0], lv.shape[3]
    half = tile // 2
    n = gbuf.shape[1]
    first = held - n
    loc = first - 1
    ring = n_col // 2
    cut = n // 2
    head = min(2, n)
    pairs = n_row // 2
    parts = tile // LANE

    row = lax.axis_index("row")
    col = lax.axis_index("col")
    q, p = col // 2, col % 2
    y, c = row // 2, row % 2
    panel = q == ring - 1
    top = y == pairs - 1
    hub = max(ring - 3, 0)
    other = jnp.logical_not(panel)
    below = (q > 0) & (q <= hub)
    above = (q == hub) & (q < ring - 2)
    lower = jnp.where(panel, 2 * hub + p, jnp.maximum(col - 2, 0))
    upper_col = jnp.minimum(col + 2, n_col - 1)
    feeder = jnp.where(q == hub, n_col - 2 + p, jnp.where(q < hub, upper_col, lower))
    twin = 2 * q + 1 - p
    mate = 2 * y + 1 - c
    part = y % 2
    pal = 2 * (y + 1 - 2 * part) + c
    hs_sub = SUB // 2
    root = n_row - 2 + c

    rows = lax.broadcasted_iota(jnp.int32, (tile, tile), 0)
    cols = lax.broadcasted_iota(jnp.int32, (tile, tile), 1)

    def rdma(src, dst, s_sem, r_sem, dev):
        return pltpu.make_async_remote_copy(
            src_ref=src, dst_ref=dst, send_sem=s_sem, recv_sem=r_sem, device_id=dev, device_id_type=MESH
        )

    def loop(a, b, body):
        def step(i, carry):
            body(i)
            return carry

        if a < b:
            lax.fori_loop(a, b, step, 0)

    def load(src, dst, k, a, b):
        return pltpu.make_async_copy(src.at[pl.ds(a, b - a)], dst.at[pl.ds(a, b - a)], vs.at[k])

    spans = [
        (l_hbm, lv, 0, loc, first),
        (g_hbm, gv, 1, first, first + head),
        (l_hbm, lv, 2, first, held),
        (g_hbm, gv, 3, first + head, held),
        (g_hbm, gv, 4, 0, first),
    ]
    loads = {span[2]: load(*span) for span in spans if span[3] < span[4]}
    for cp in loads.values():
        cp.start()

    def loaded(*ks):
        for k in ks:
            if k in loads:
                loads[k].wait()

    barrier = pltpu.get_barrier_semaphore()

    def greet(dev):
        pl.semaphore_signal(barrier, inc=1, device_id=dev, device_id_type=MESH)

    greet({"col": twin})
    greet({"row": mate})
    greet({"row": pal})

    @pl.when(below | panel)
    def _():
        greet({"col": lower})

    @pl.when(above)
    def _():
        greet({"col": upper_col})

    @pl.when(other)
    def _():
        greet({"col": feeder})

    @pl.when(jnp.logical_not(top))
    def _():
        greet({"row": root})

    @pl.when(top)
    def _():
        for k in range(pairs - 1):
            greet({"row": 2 * k + c})

    @pl.when(top & panel)
    def _():
        greet({"row": mate, "col": twin})

    heard = (
        3
        + (below | panel).astype(jnp.int32)
        + above.astype(jnp.int32)
        + other.astype(jnp.int32)
        + jnp.where(top, pairs - 1, 1)
        + (top & panel).astype(jnp.int32)
    )
    with jax.named_scope("barrier"):
        pl.semaphore_wait(barrier, heard)

    loaded(0)

    def mat(ref, *at):
        return ref[at].reshape(tile, tile)

    def g_down(t, k, src):
        return rdma(src.at[k], gbuf.at[p, t, k], gs.at[0], gm.at[t, k], {"col": lower})

    def g_up(t, k, src):
        return rdma(src.at[k], gbuf.at[p, t, k], gs.at[2], gm.at[t, k], {"col": upper_col})

    def g_cross(t, k, src):
        return rdma(src.at[k], gbuf.at[p, t, k], gs.at[1], gx.at[t], {"col": twin})

    def f_cross(t, k):
        return rdma(lv.at[first + t, k], gbuf.at[0, t, k], gs.at[1], gx.at[t], {"col": twin})

    def g_main(t, k):
        ref = gbuf.at[p, t, k]
        rdma(ref, ref, gs.at[0], gm.at[t, k], {"col": twin}).wait_recv()

    def g_twin(t):
        ref = gbuf.at[1 - p, t]
        rdma(ref, ref, gs.at[1], gx.at[t], {"col": twin}).wait_recv()

    def g_sent(k, ref):
        rdma(ref, ref, gs.at[k], gx.at[0], {"col": twin}).wait_send()

    def l_down(j, src):
        k = part * hs_sub + j
        return rdma(src.at[k], lbuf.at[p, c, k], ls.at[0], lm.at[j], {"col": lower})

    def l_up(j, src):
        k = part * hs_sub + j
        return rdma(src.at[k], lbuf.at[p, c, k], ls.at[6], lm.at[j], {"col": upper_col})

    def l_cross(j, src):
        k = part * hs_sub + j
        return rdma(src.at[k], lbuf.at[p, c, k], ls.at[1], lx.at[j], {"col": twin})

    def l_share(s, j):
        ref = lbuf.at[s, c, part * hs_sub + j]
        rdma(ref, ref, ls.at[2 + s], lf.at[s], {"row": mate}).start()
        rdma(ref, ref, ls.at[4 + s], lp.at[s], {"row": pal}).start()

    def l_main(j):
        ref = lbuf.at[p, c, part * hs_sub + j]
        rdma(ref, ref, ls.at[0], lm.at[j], {"col": twin}).wait_recv()

    def l_twin(j):
        ref = lbuf.at[1 - p, c, part * hs_sub + j]
        rdma(ref, ref, ls.at[1], lx.at[j], {"col": twin}).wait_recv()

    def l_rest(s):
        ref = lbuf.at[s, c, pl.ds((1 - part) * hs_sub, hs_sub)]
        rdma(ref, ref, ls.at[4], lp.at[s], {"row": pal}).wait_recv()
        rdma(ref, ref, ls.at[2 + s], lf.at[s], {"row": mate}).start()

    def l_full(s):
        ref = lbuf.at[s, 1 - c]
        rdma(ref, ref, ls.at[2], lf.at[s], {"row": mate}).wait_recv()

    def l_sent(k, whole=False):
        ref = lbuf.at[0, 0] if whole else lbuf.at[0, 0, pl.ds(0, hs_sub)]
        rdma(ref, ref, ls.at[k], lf.at[0], {"row": mate}).wait_send()

    def k_star(k):
        return rdma(lv.at[loc], lk.at[c], ks.at[k], kr.at[c], {"row": 2 * k + c})

    def k_mate(src):
        return rdma(src, lk.at[c], ks.at[pairs], kr.at[c], {"row": mate})

    def k_wait(i):
        rdma(lk.at[i], lk.at[i], ks.at[pairs], kr.at[i], {"row": mate}).wait_recv()

    def t_mate():
        return rdma(tout.at[1 - c], tin, ts.at[0], tr.at[pairs], {"row": mate})

    def t_root():
        return rdma(tout.at[c], tslot.at[y], ts.at[1], tr.at[y], {"row": root})

    def h_mate(k):
        return rdma(h.at[k, 1 - c], hin.at[k], hs.at[k], hr.at[k], {"row": mate})

    def h_root(k):
        return rdma(hsum.at[k], hslot.at[k, y], hs.at[2 + k], hq.at[k, y], {"row": root})

    def h_twin(k):
        return rdma(hsum.at[k], htwin.at[k], hs.at[2 + k], hr.at[2 + k], {"col": twin})

    def h_full():
        return rdma(hfull.at[c], hfull.at[c], hs.at[4], hr.at[4], {"row": mate})

    def d_copy(k, src, i, dev):
        return rdma(src, gd.at[k], ds.at[i], dr.at[k], dev)

    def d_wait(k):
        d_copy(k, gd.at[k], 0, {"row": mate}).wait_recv()

    def s_down(k):
        return rdma(sbuf.at[p, k], sbuf.at[p, k], ss.at[0], sm.at[k], {"col": lower})

    def s_up(k):
        return rdma(sbuf.at[p, k], sbuf.at[p, k], ss.at[2], sm.at[k], {"col": upper_col})

    def s_cross(k):
        return rdma(sbuf.at[p, k], sbuf.at[p, k], ss.at[1], sx.at[0], {"col": twin})

    def s_main(k):
        s_down(k).wait_recv()

    def s_twin():
        ref = sbuf.at[1 - p]
        rdma(ref, ref, ss.at[1], sx.at[0], {"col": twin}).wait_recv()

    def s_sent(k):
        ref = sbuf.at[p]
        rdma(ref, ref, ss.at[k], sx.at[0], {"col": twin}).wait_send()

    @pl.when(top)
    def _():
        for k in range(pairs - 1):
            k_star(k).start()
        k_mate(lv.at[loc]).start()
        lk[c] = lv[loc]

    def gather_rows():
        @pl.when(jnp.logical_not(top))
        def _():
            k_wait(c)
            k_mate(lk.at[c]).start()

        k_wait(1 - c)

    def start_inverse(k):
        d = mat(lbuf, k, k).astype(F32)
        e = (rows == cols).astype(F32)
        on = d * e
        rc = 1.0 / jnp.sum(on, axis=1, keepdims=True)
        rr = 1.0 / jnp.sum(on, axis=0, keepdims=True)
        off = ((rows & 1) == 1) & (cols == rows - 1)
        w[k] = e * rr - rc * jnp.where(off, d, 0.0) * rr

    n_lev = tile.bit_length() - 2

    def inverse_level(sh, k):
        off = ((jnp.right_shift(rows, sh) & 1) == 1) & (
            jnp.right_shift(cols, sh) == jnp.right_shift(rows, sh) - 1
        )
        part = jnp.where(off, mat(lbuf, k, k).astype(F32), 0.0)
        cur = w[k]
        w[k] = cur - dot3(cur, dot3(part, cur))

    def finish_inverse():
        w[2] = -dot3(w[1], dot3(mat(lbuf, 0, 1).astype(F32), w[0]))

    def put_x(i, x):
        hi = x.astype(BF16)
        xh[i] = hi
        xl[i] = (x - hi.astype(F32)).astype(BF16)

    def store(a, value):
        for b in range(parts):
            lin[a, pl.ds(b, tile, stride=parts), :] = value[:, b * LANE : (b + 1) * LANE]

    h[...] = jnp.zeros_like(h)

    def add_h(k, left, right):
        h[k] += outer(left, right).reshape(2, half, tile)

    def times_x(total, i, g):
        for part in (xl, xh):
            total = total - jnp.dot(g, part[i], preferred_element_type=F32)
        return total

    @pl.when(jnp.logical_not(panel))
    def _():
        loaded(1, 2, 3, 4)

        def relay(t, work=()):
            for k in range(SUB):
                with jax.named_scope("w_main"):
                    g_main(t, k)

                @pl.when(below)
                def _():
                    g_down(t, k, gbuf.at[p, t]).start()

                @pl.when(above)
                def _():
                    g_up(t, k, gbuf.at[p, t]).start()

                g_cross(t, k, gbuf.at[p, t]).start()
                if k < len(work):
                    work[k]()

        def use(t):
            with jax.named_scope("w_cross"):
                g_twin(t)
            right = mat(lv, first + t)
            add_h(0, mat(gbuf, 0, t), right)
            add_h(1, mat(gbuf, 1, t), right)

        def low(t):
            total = mat(gv, first + t).astype(F32)
            for s in range(2):
                total = times_x(total, s, mat(gbuf, s, t))
            store(first + t, total)

        main_l = (p == 0) | (c == 1)
        other_l = (p == 1) | (c == 1)

        for t in range(head):
            relay(t)
        with jax.named_scope("gather"):
            gather_rows()

        with jax.named_scope("l_relay"):

            @pl.when(main_l)
            def _():
                def step(k):
                    l_main(k)

                    @pl.when(below)
                    def _():
                        l_down(k, lbuf.at[p, c]).start()

                    @pl.when(above)
                    def _():
                        l_up(k, lbuf.at[p, c]).start()

                    l_cross(k, lbuf.at[p, c]).start()
                    l_share(p, k)

                loop(0, hs_sub, step)

        def share_first():
            @pl.when(main_l)
            def _():
                l_rest(p)

            @pl.when(other_l)
            def _():
                def step(k):
                    l_twin(k)
                    l_share(1 - p, k)

                loop(0, hs_sub, step)

        def share_rest():
            @pl.when(other_l)
            def _():
                l_rest(1 - p)

        def share_done():
            l_full(0)

            @pl.when(c == 0)
            def _():
                l_full(1)

        steps = (lambda: None, share_first, share_rest, share_done)
        for j, share in enumerate(steps):
            if head + j < n:
                relay(head + j, (lambda: None, functools.partial(use, j - 1)) if j > 0 else ())
            with jax.named_scope("l_wait"):
                share()
        warm = min(head + len(steps), n)
        used = max(warm - head - 1, 0)

        start_inverse(0)
        start_inverse(1)

        base = warm
        lag = base - used
        double = min(n_lev // 2, n - base)

        def level_step(i):
            lev = 2 * (i - base) + 1

            def third():
                inverse_level(lev + 1, 0)
                use(i - lag)

            relay(
                i,
                (
                    lambda: inverse_level(lev, 0),
                    lambda: inverse_level(lev, 1),
                    third,
                    lambda: inverse_level(lev + 1, 1),
                ),
            )

        loop(base, base + double, level_step)
        used += double

        def level_rest(k):
            loop(2 * double + 1, n_lev + 1, lambda lev: inverse_level(lev, k))

        def x_first():
            put_x(0, dot3(w[0], mat(lk, 0).astype(F32)))

        def x_second():
            put_x(1, dot3(w[2], mat(lk, 0).astype(F32)) + dot3(w[1], mat(lk, 1).astype(F32)))

        def solve_x():
            x_first()
            x_second()
            loop(used, at - 1, use)

        at = base + double
        if at < n:
            relay(at, (lambda: level_rest(0), lambda: level_rest(1), finish_inverse, solve_x))
            used = at - 1
            at += 1
        else:
            level_rest(0)
            level_rest(1)
            finish_inverse()
            x_first()
            x_second()
        begun = at

        per = max(d for d in (1, 2, 3) if d == 1 or d * max(n - begun, 1) <= n - 2)

        def low_step(i):
            j = (i - begun) * per
            relay(i, [lambda: use(i - 2)] + [functools.partial(lambda d: low(j + d), d) for d in range(per)])

        loop(begun, n, low_step)
        lows = per * max(n - begun, 0)
        used += max(n - begun, 0)

        def send_t():
            loop(used, n, use)
            h0, h1 = mat(h, 0), mat(h, 1)

            def first_t():
                tout[1] = dot3(w[1], h1, 0, 0)

            def second_t():
                tout[0] = dot3(w[0], h0, 0, 0) + dot3(w[2], h1, 0, 0)

            for mine, one, two in ((0, first_t, second_t), (1, second_t, first_t)):

                @pl.when(c == mine)
                def _(one=one, two=two):
                    one()
                    t_mate().start()
                    two()

        def upper(a):
            store(a, mat(gv, a).astype(F32))

        @pl.when(jnp.logical_not(top))
        def _():
            send_t()
            with jax.named_scope("w_tmate"):
                t_mate().wait_recv()
            tout[c] += tin[...]
            t_root().start()
            loop(lows, n, low)
            loop(0, loc + 1, upper)

        @pl.when(top)
        def _():
            def s_relay(k):
                with jax.named_scope("w_s"):
                    s_main(k)

                @pl.when(below)
                def _():
                    s_down(k).start()

                @pl.when(above)
                def _():
                    s_up(k).start()

                s_cross(k).start()

            loop(0, CHUNKS, s_relay)
            send_t()
            loop(lows, n, low)
            loop(0, loc, upper)
            with jax.named_scope("w_s2"):
                s_twin()
            k0, k1 = mat(lk, 0).astype(F32), mat(lk, 1).astype(F32)
            total = mat(gv, loc).astype(F32) - dot3(mat(sbuf, 0), k0) - dot3(mat(sbuf, 1), k1)
            with jax.named_scope("w_tmate2"):
                t_mate().wait_recv()
            total = total - (tout[c] + tin[...])
            with jax.named_scope("w_tslot"):
                for k in range(pairs - 1):
                    rdma(tslot.at[k], tslot.at[k], ts.at[1], tr.at[k], {"row": mate}).wait_recv()
            for k in range(pairs - 1):
                total = total - tslot[k]
            store(loc, total)

        drain = jax.named_scope("drain")
        drain.__enter__()

        g_sent(1, gbuf.at[p])

        @pl.when(below)
        def _():
            g_sent(0, gbuf.at[p])

        @pl.when(above)
        def _():
            g_sent(2, gbuf.at[p])

        @pl.when(main_l)
        def _():
            l_sent(1)
            l_sent(2 + p, True)
            l_sent(4 + p)

            @pl.when(below)
            def _():
                l_sent(0)

            @pl.when(above)
            def _():
                l_sent(6)

        @pl.when(other_l)
        def _():
            l_sent(3 - p, True)
            l_sent(5 - p)

        t_mate().wait_send()

        @pl.when(jnp.logical_not(top))
        def _():
            t_root().wait_send()

        @pl.when(top)
        def _():
            s_sent(1)

            @pl.when(below)
            def _():
                s_sent(0)

            @pl.when(above)
            def _():
                s_sent(2)

        drain.__exit__(None, None, None)

    @pl.when(panel)
    def _():
        def each(body):
            def run(t):
                for k in range(SUB):
                    body(t, k)

            return run

        send = each(lambda t, k: g_down(t, k, gv.at[first + t]).start() if ring > 1 else None)
        cross_lo = each(lambda t, k: f_cross(t, k).start())
        cross_hi = each(lambda t, k: g_cross(t, k, gv.at[first + t]).start())
        lead = min(2, cut)
        mid = min(cut + 2, n)
        loaded(1)
        loop(0, head, send)

        @pl.when(p == 0)
        def _():
            loaded(2)
            loop(cut, mid, cross_lo)

        @pl.when(p == 1)
        def _():
            loop(0, lead, cross_hi)
            loaded(2)

        loaded(3, 4)
        with jax.named_scope("gather"):
            gather_rows()

        def send_l():
            def step(k):
                if ring > 1:
                    l_down(k, lk.at[c]).start()
                l_cross(k, lk.at[c]).start()

            loop(0, hs_sub, step)

        @pl.when(p == 0)
        def _():
            send_l()
            lbuf[0] = lk[...]
            loop(mid, n, cross_lo)

            @pl.when(top & (c == 1))
            def _():
                d_copy(1, gv.at[loc], 0, {"row": mate}).start()
                d_copy(1, gv.at[loc], 1, {"row": mate, "col": twin}).start()
                gd[1] = gv[loc]

        @pl.when(p == 1)
        def _():
            @pl.when(c == 1)
            def _():
                send_l()

            lbuf[1, 1] = lk[1]
            loop(lead, cut, cross_hi)

            @pl.when(top & (c == 1))
            def _():
                d_copy(2, gv.at[loc], 0, {"row": mate}).start()
                d_copy(2, gv.at[loc], 1, {"col": twin}).start()
                gd[2] = gv[loc]

        loop(head, n, send)

        with jax.named_scope("hd"):
            loop(0, n, lambda t: add_h(0, mat(gv, first + t), mat(lv, first + t)))
        h_mate(0).start()

        with jax.named_scope("l_wait"):
            @pl.when((p == 1) | (c == 1))
            def _():
                def step(k):
                    l_twin(k)
                    l_share(1 - p, k)

                loop(0, hs_sub, step)
                l_rest(1 - p)

            @pl.when(p == 1)
            def _():
                l_full(0)

            @pl.when((p == 0) & (c == 0))
            def _():
                l_full(1)

        def reduce_mate(k):
            with jax.named_scope("w_hmate"):
                h_mate(k).wait_recv()
            hsum[k] = h[k, c] + hin[k]

            @pl.when(jnp.logical_not(top))
            def _():
                h_root(k).start()

        def reduce_root(k):
            total = hsum[k]
            for i in range(pairs - 1):
                with jax.named_scope("w_hroot"):
                    ref = hslot.at[k, i]
                    rdma(ref, ref, hs.at[2 + k], hq.at[k, i], {"row": mate}).wait_recv()
                total = total + hslot[k, i]
            hsum[k] = total
            h_twin(k).start()

        start_inverse(0)
        start_inverse(1)
        reduce_mate(0)

        def level(lev):
            inverse_level(lev, 0)
            inverse_level(lev, 1)

        early = (n_lev + 1) // 2
        loop(1, early + 1, level)

        @pl.when(top)
        def _():
            reduce_root(0)

        loop(early + 1, n_lev + 1, level)
        finish_inverse()

        @pl.when(p == 0)
        def _():
            def use(t):
                with jax.named_scope("w_x"):
                    g_twin(t)
                add_h(1, mat(gbuf, 1, t), mat(lv, first + t))

            loop(0, cut, use)

        @pl.when(p == 1)
        def _():
            def use(t):
                with jax.named_scope("w_x"):
                    g_twin(t)
                add_h(1, mat(gv, first + t), mat(gbuf, 0, t))

            loop(cut, n, use)

        h_mate(1).start()

        @pl.when(top & (c == 1) & (p == 0))
        def _():
            d_wait(2)
            d_copy(2, gd.at[2], 2, {"row": mate}).start()

        reduce_mate(1)

        @pl.when(top)
        def _():
            reduce_root(1)

        @pl.when(p == 1)
        def _():
            loop(cut, n, cross_hi)

        @pl.when(top)
        def _():
            with jax.named_scope("w_htwin"):
                for k in range(2):
                    h_twin(k).wait_recv()
            mine, theirs = hsum[0], htwin[0]
            hfull[c, 0] = jnp.where(p == 0, mine, theirs)
            hfull[c, 2] = jnp.where(p == 0, theirs, mine)
            hfull[c, 1] = hsum[1] + htwin[1]
            h_full().start()
            with jax.named_scope("w_hfull"):
                ref = hfull.at[1 - c]
                rdma(ref, ref, hs.at[4], hr.at[4], {"row": mate}).wait_recv()

                @pl.when(c == 0)
                def _():
                    d_wait(1)
                    d_wait(2)

            eye = (rows == cols).astype(F32)

            def keep(x):
                return jnp.where(rows >= cols, x, 0.0)

            w66, w77, w76 = w[0], w[1], w[2]
            l77 = mat(lbuf, 1, 1).astype(F32)
            g_here = mat(gv, loc).astype(F32)

            def full(k):
                return jnp.concatenate([hfull[0, k], hfull[1, k]], 0)

            q77 = keep(mat(gd, 2).astype(F32) - dot3(w77, full(2), 0, 0))
            m77 = dot3(l77, q77, 0, 0)
            phi77 = keep(m77) - 0.5 * m77 * eye

            def put_s(s, o):
                sbuf[p] = s.reshape(CHUNKS, tile // CHUNKS, tile)
                if ring > 1:
                    loop(0, CHUNKS, lambda k: s_down(k).start())
                store(loc, o)

            def tri(s):
                return keep(s) - 0.5 * s * eye

            @pl.when((c == 1) & (p == 1))
            def _():
                half77 = dot3(dot3(w77, phi77, 0, 0), w77)
                s = half77 + half77.T
                put_s(s, tri(s))

            @pl.when(jnp.logical_not((c == 1) & (p == 1)))
            def _():
                g76 = jnp.where(c == 1, g_here, mat(gd, 1).astype(F32))
                q76 = g76 - dot3(w77, full(1), 0, 0)
                phi76 = dot3(l77, q76, 0, 0)

                @pl.when((c == 0) & (p == 0))
                def _():
                    t66 = dot3(w66, full(0), 0, 0) + dot3(w76, full(1), 0, 0)
                    q66 = keep(g_here - t66)
                    l66, l76 = mat(lbuf, 0, 0).astype(F32), mat(lbuf, 0, 1).astype(F32)
                    m66 = dot3(l66, q66, 0, 0) + dot3(l76, q76, 0, 0)
                    phi66 = keep(m66) - 0.5 * m66 * eye
                    inner = dot3(phi76, w66) + dot3(phi77, w76)
                    half66 = dot3(w66, dot3(phi66, w66), 0, 0) + dot3(w76, inner, 0, 0)
                    s = half66 + half66.T
                    put_s(s, tri(s))

                @pl.when(jnp.logical_not((c == 0) & (p == 0)))
                def _():
                    inner = dot3(phi76, w66) + dot3(phi77 + phi77.T, w76)

                    @pl.when(c == 1)
                    def _():
                        s = dot3(w77, inner, 0, 0)
                        put_s(s, s)

                    @pl.when(c == 0)
                    def _():
                        put_s(dot3(inner, w77, 0, 0), jnp.zeros((tile, tile), F32))

        zero = jnp.zeros((tile, tile), F32)
        loop(0, loc, lambda a: store(a, zero))

        @pl.when(jnp.logical_not(top))
        def _():
            store(loc, zero)

        put_x(1, jnp.where(p == 0, -w[2], -w[1]))

        with jax.named_scope("low"):

            @pl.when(p == 0)
            def _():
                put_x(0, -w[0])

                def low(t):
                    total = times_x(zero, 0, mat(gv, first + t))
                    store(first + t, times_x(total, 1, mat(gbuf, 1, t)))

                def late(t):
                    g_twin(t)
                    low(t)

                loop(0, cut, low)
                loop(cut, n, late)

            @pl.when(p == 1)
            def _():
                loop(0, n, lambda t: store(first + t, times_x(zero, 1, mat(gv, first + t))))

        drain = jax.named_scope("drain")
        drain.__enter__()

        @pl.when(p == 0)
        def _():
            g_sent(1, gbuf.at[0, pl.ds(cut, n - cut)])

            @pl.when(top & (c == 1))
            def _():
                d_copy(1, gv.at[loc], 0, {"row": mate}).wait_send()
                d_copy(1, gv.at[loc], 1, {"row": mate, "col": twin}).wait_send()
                d_copy(2, gd.at[2], 2, {"row": mate}).wait_send()

        @pl.when(p == 1)
        def _():
            g_sent(1, gbuf.at[1])

            @pl.when(top & (c == 1))
            def _():
                d_copy(2, gv.at[loc], 0, {"row": mate}).wait_send()
                d_copy(2, gv.at[loc], 1, {"col": twin}).wait_send()

        @pl.when((p == 0) | (c == 1))
        def _():
            l_sent(1)
            if ring > 1:
                l_sent(0)

        @pl.when((p == 1) | (c == 1))
        def _():
            l_sent(3 - p, True)
            l_sent(5 - p)

        if ring > 1:
            g_sent(0, gbuf.at[p])
        for k in range(2):
            h_mate(k).wait_send()

            @pl.when(jnp.logical_not(top))
            def _():
                h_root(k).wait_send()

            @pl.when(top)
            def _():
                h_twin(k).wait_send()

        @pl.when(top)
        def _():
            h_full().wait_send()
            if ring > 1:
                s_sent(0)

        drain.__exit__(None, None, None)

    @pl.when(top)
    def _():
        for k in range(pairs - 1):
            k_star(k).wait_send()
        k_mate(lv.at[loc]).wait_send()

    @pl.when(jnp.logical_not(top))
    def _():
        k_mate(lk.at[c]).wait_send()


def panel(factor, grad, n_row, n_col, first):
    rows_here, tile = factor.shape[0], factor.shape[1]
    n = rows_here - first
    half = tile // 2
    pairs = n_row // 2
    sub = (SUB, tile // SUB, tile)
    hbm = pl.BlockSpec(memory_space=pltpu.HBM)
    dma = pltpu.SemaphoreType.DMA
    return pl.pallas_call(
        functools.partial(panel_kernel, n_row, n_col),
        out_shape=jax.ShapeDtypeStruct((rows_here, tile * tile // LANE, LANE), F32),
        in_specs=[hbm, hbm],
        out_specs=pl.BlockSpec(memory_space=pltpu.VMEM),
        scratch_shapes=[
            pltpu.VMEM((rows_here, *sub), BF16),
            pltpu.VMEM((rows_here, *sub), BF16),
            pltpu.VMEM((2, n, *sub), BF16),
            pltpu.VMEM((2, tile, tile), BF16),
            pltpu.VMEM((2, tile, tile), BF16),
            pltpu.VMEM((2, *sub), BF16),
            pltpu.VMEM((2, 2, *sub), BF16),
            pltpu.VMEM((3, tile, tile), F32),
            pltpu.VMEM((2, 2, half, tile), F32),
            pltpu.VMEM((2, tile, tile), F32),
            pltpu.VMEM((tile, tile), F32),
            pltpu.VMEM((pairs, tile, tile), F32),
            pltpu.VMEM((2, half, tile), F32),
            pltpu.VMEM((2, half, tile), F32),
            pltpu.VMEM((2, pairs, half, tile), F32),
            pltpu.VMEM((2, half, tile), F32),
            pltpu.VMEM((2, 3, half, tile), F32),
            pltpu.VMEM((3, *sub), BF16),
            pltpu.VMEM((2, CHUNKS, tile // CHUNKS, tile), F32),
            dma((5,)),
            dma((3,)),
            dma((n, SUB)),
            dma((n,)),
            dma((7,)),
            dma((SUB // 2,)),
            dma((SUB // 2,)),
            dma((2,)),
            dma((2,)),
            dma((pairs + 1,)),
            dma((2,)),
            dma((2,)),
            dma((pairs + 1,)),
            dma((5,)),
            dma((5,)),
            dma((2, pairs)),
            dma((3,)),
            dma((3,)),
            dma((3,)),
            dma((CHUNKS,)),
            dma((1,)),
        ],
        compiler_params=pltpu.CompilerParams(
            collective_id=0, has_side_effects=True, vmem_limit_bytes=VMEM
        ),
        name="panel",
    )(
        pltpu.with_memory_space_constraint(factor.reshape(rows_here, *sub), pltpu.HBM),
        pltpu.with_memory_space_constraint(grad.reshape(rows_here, *sub), pltpu.HBM),
    )


def per_device(l_saved, l_grad):
    rows_here, tile = l_saved.shape[0], l_saved.shape[2]
    n_row = lax.axis_size("row")
    n_col = lax.axis_size("col")
    assert n_col % n_row == 0 and n_row % 4 == 0 and tile % (SUB * 16) == 0
    first = n_col // n_row
    factor = l_saved.reshape(rows_here, tile, tile)
    grad = l_grad.reshape(rows_here, tile, tile)
    lin = panel(factor, grad, n_row, n_col, first)
    return lin.reshape(l_grad.shape)


def solution(mesh):
    spec = P(None, "row", None, "col", None)
    return jax.shard_map(
        per_device, mesh=mesh, in_specs=(spec, spec), out_specs=spec, check_vma=False
    )
```

```python
import functools

import jax
import jax.numpy as jnp
from jax import lax
from jax.experimental import pallas as pl
from jax.experimental.pallas import tpu as pltpu
from jax.sharding import PartitionSpec as P

F32 = jnp.float32
BF16 = jnp.bfloat16
HIGH3 = lax.Precision.HIGH
MESH = pl.DeviceIdType.MESH
CHUNKS = 8
SUB = 4
LANE = 128
VMEM = 40 * 1024 * 1024


def dot3(a, b, ca=1, cb=0):
    return lax.dot_general(
        a, b, (((ca,), (cb,)), ((), ())), precision=HIGH3, preferred_element_type=F32
    )


def outer(a, b):
    return lax.dot_general(a, b, (((0,), (0,)), ((), ())), preferred_element_type=F32)


def panel_kernel(
    n_row,
    n_col,
    l_hbm,
    g_hbm,
    lin,
    lv,
    gv,
    gbuf,
    xh,
    xl,
    lk,
    lbuf,
    w,
    h,
    tout,
    tin,
    tslot,
    hin,
    hsum,
    hslot,
    htwin,
    hfull,
    gd,
    sbuf,
    vs,
    gs,
    gm,
    gx,
    ls,
    lm,
    lx,
    lf,
    lp,
    ks,
    kr,
    ts,
    tr,
    hs,
    hr,
    hq,
    ds,
    dr,
    ss,
    sm,
    sx,
):
    held, tile = lv.shape[0], lv.shape[3]
    half = tile // 2
    n = gbuf.shape[1]
    first = held - n
    loc = first - 1
    ring = n_col // 2
    cut = n // 2
    head = min(2, n)
    pairs = n_row // 2
    parts = tile // LANE

    row = lax.axis_index("row")
    col = lax.axis_index("col")
    q, p = col // 2, col % 2
    y, c = row // 2, row % 2
    panel = q == ring - 1
    top = y == pairs - 1
    hub = max(ring - 3, 0)
    other = jnp.logical_not(panel)
    below = (q > 0) & (q <= hub)
    above = (q == hub) & (q < ring - 2)
    lower = jnp.where(panel, 2 * hub + p, jnp.maximum(col - 2, 0))
    upper_col = jnp.minimum(col + 2, n_col - 1)
    feeder = jnp.where(q == hub, n_col - 2 + p, jnp.where(q < hub, upper_col, lower))
    twin = 2 * q + 1 - p
    mate = 2 * y + 1 - c
    odd = y % 2 == 1
    pal = 2 * (y + 1 - 2 * (y % 2)) + c
    root = n_row - 2 + c

    rows = lax.broadcasted_iota(jnp.int32, (tile, tile), 0)
    cols = lax.broadcasted_iota(jnp.int32, (tile, tile), 1)

    def rdma(src, dst, s_sem, r_sem, dev):
        return pltpu.make_async_remote_copy(
            src_ref=src, dst_ref=dst, send_sem=s_sem, recv_sem=r_sem, device_id=dev, device_id_type=MESH
        )

    def loop(a, b, body):
        def step(i, carry):
            body(i)
            return carry

        if a < b:
            lax.fori_loop(a, b, step, 0)

    def load(src, dst, k, a, b):
        return pltpu.make_async_copy(src.at[pl.ds(a, b - a)], dst.at[pl.ds(a, b - a)], vs.at[k])

    spans = [
        (l_hbm, lv, 0, loc, first),
        (g_hbm, gv, 1, first, first + head),
        (l_hbm, lv, 2, first, held),
        (g_hbm, gv, 3, first + head, held),
        (g_hbm, gv, 4, 0, first),
    ]
    loads = {span[2]: load(*span) for span in spans if span[3] < span[4]}
    for cp in loads.values():
        cp.start()

    def loaded(*ks):
        for k in ks:
            if k in loads:
                loads[k].wait()

    barrier = pltpu.get_barrier_semaphore()

    def greet(dev):
        pl.semaphore_signal(barrier, inc=1, device_id=dev, device_id_type=MESH)

    greet({"col": twin})
    greet({"row": mate})
    greet({"row": pal})

    @pl.when(below | panel)
    def _():
        greet({"col": lower})

    @pl.when(above)
    def _():
        greet({"col": upper_col})

    @pl.when(other)
    def _():
        greet({"col": feeder})

    @pl.when(jnp.logical_not(top))
    def _():
        greet({"row": root})

    @pl.when(top)
    def _():
        for k in range(pairs - 1):
            greet({"row": 2 * k + c})

    @pl.when(top & panel)
    def _():
        greet({"row": mate, "col": twin})

    heard = (
        3
        + (below | panel).astype(jnp.int32)
        + above.astype(jnp.int32)
        + other.astype(jnp.int32)
        + jnp.where(top, pairs - 1, 1)
        + (top & panel).astype(jnp.int32)
    )
    with jax.named_scope("barrier"):
        pl.semaphore_wait(barrier, heard)

    loaded(0)

    def mat(ref, *at):
        return ref[at].reshape(tile, tile)

    def g_down(t, k, src):
        return rdma(src.at[k], gbuf.at[p, t, k], gs.at[0], gm.at[t, k], {"col": lower})

    def g_up(t, k, src):
        return rdma(src.at[k], gbuf.at[p, t, k], gs.at[2], gm.at[t, k], {"col": upper_col})

    def g_cross(t, k, src):
        return rdma(src.at[k], gbuf.at[p, t, k], gs.at[1], gx.at[t], {"col": twin})

    def f_cross(t, k):
        return rdma(lv.at[first + t, k], gbuf.at[0, t, k], gs.at[1], gx.at[t], {"col": twin})

    def g_main(t, k):
        ref = gbuf.at[p, t, k]
        rdma(ref, ref, gs.at[0], gm.at[t, k], {"col": twin}).wait_recv()

    def g_twin(t):
        ref = gbuf.at[1 - p, t]
        rdma(ref, ref, gs.at[1], gx.at[t], {"col": twin}).wait_recv()

    def g_sent(k, ref):
        rdma(ref, ref, gs.at[k], gx.at[0], {"col": twin}).wait_send()

    def l_down(k, src):
        return rdma(src.at[k], lbuf.at[p, c, k], ls.at[0], lm.at[k], {"col": lower})

    def l_up(k, src):
        return rdma(src.at[k], lbuf.at[p, c, k], ls.at[6], lm.at[k], {"col": upper_col})

    def l_cross(k, src):
        return rdma(src.at[k], lbuf.at[p, c, k], ls.at[1], lx.at[k], {"col": twin})

    def l_share(s, k):
        ref = lbuf.at[s, c, k]
        rdma(ref, ref, ls.at[4 + s], lp.at[s], {"row": pal}).start()
        rdma(ref, ref, ls.at[2 + s], lf.at[s], {"row": mate}).start()

    def l_main(k):
        ref = lbuf.at[p, c, k]
        rdma(ref, ref, ls.at[0], lm.at[k], {"col": twin}).wait_recv()

    def l_twin(k):
        ref = lbuf.at[1 - p, c, k]
        rdma(ref, ref, ls.at[1], lx.at[k], {"col": twin}).wait_recv()

    def l_rest(s):
        ref = lbuf.at[s, c]
        rdma(ref, ref, ls.at[4], lp.at[s], {"row": pal}).wait_recv()
        rdma(ref, ref, ls.at[2 + s], lf.at[s], {"row": mate}).start()

    def l_full(s):
        ref = lbuf.at[s, 1 - c]
        rdma(ref, ref, ls.at[2], lf.at[s], {"row": mate}).wait_recv()

    def l_sent(k):
        ref = lbuf.at[0, 0]
        rdma(ref, ref, ls.at[k], lf.at[0], {"row": mate}).wait_send()

    def k_star(k):
        return rdma(lv.at[loc], lk.at[c], ks.at[k], kr.at[c], {"row": 2 * k + c})

    def k_mate(src):
        return rdma(src, lk.at[c], ks.at[pairs], kr.at[c], {"row": mate})

    def k_wait(i):
        rdma(lk.at[i], lk.at[i], ks.at[pairs], kr.at[i], {"row": mate}).wait_recv()

    def t_mate():
        return rdma(tout.at[1 - c], tin, ts.at[0], tr.at[pairs], {"row": mate})

    def t_root():
        return rdma(tout.at[c], tslot.at[y], ts.at[1], tr.at[y], {"row": root})

    def h_mate(k):
        return rdma(h.at[k, 1 - c], hin.at[k], hs.at[k], hr.at[k], {"row": mate})

    def h_root(k):
        return rdma(hsum.at[k], hslot.at[k, y], hs.at[2 + k], hq.at[k, y], {"row": root})

    def h_twin(k):
        return rdma(hsum.at[k], htwin.at[k], hs.at[2 + k], hr.at[2 + k], {"col": twin})

    def h_full():
        return rdma(hfull.at[c], hfull.at[c], hs.at[4], hr.at[4], {"row": mate})

    def d_copy(k, src, i, dev):
        return rdma(src, gd.at[k], ds.at[i], dr.at[k], dev)

    def d_wait(k):
        d_copy(k, gd.at[k], 0, {"row": mate}).wait_recv()

    def s_down(k):
        return rdma(sbuf.at[p, k], sbuf.at[p, k], ss.at[0], sm.at[k], {"col": lower})

    def s_up(k):
        return rdma(sbuf.at[p, k], sbuf.at[p, k], ss.at[2], sm.at[k], {"col": upper_col})

    def s_cross(k):
        return rdma(sbuf.at[p, k], sbuf.at[p, k], ss.at[1], sx.at[0], {"col": twin})

    def s_main(k):
        s_down(k).wait_recv()

    def s_twin():
        ref = sbuf.at[1 - p]
        rdma(ref, ref, ss.at[1], sx.at[0], {"col": twin}).wait_recv()

    def s_sent(k):
        ref = sbuf.at[p]
        rdma(ref, ref, ss.at[k], sx.at[0], {"col": twin}).wait_send()

    @pl.when(top)
    def _():
        for k in range(pairs - 1):
            k_star(k).start()
        k_mate(lv.at[loc]).start()
        lk[c] = lv[loc]

    def gather_rows():
        @pl.when(jnp.logical_not(top))
        def _():
            k_wait(c)
            k_mate(lk.at[c]).start()

    def start_inverse(k):
        d = mat(lbuf, k, k).astype(F32)
        e = (rows == cols).astype(F32)
        on = d * e
        rc = 1.0 / jnp.sum(on, axis=1, keepdims=True)
        rr = 1.0 / jnp.sum(on, axis=0, keepdims=True)
        off = ((rows & 1) == 1) & (cols == rows - 1)
        w[k] = e * rr - rc * jnp.where(off, d, 0.0) * rr

    n_lev = tile.bit_length() - 2

    def inverse_level(sh, k):
        off = ((jnp.right_shift(rows, sh) & 1) == 1) & (
            jnp.right_shift(cols, sh) == jnp.right_shift(rows, sh) - 1
        )
        part = jnp.where(off, mat(lbuf, k, k).astype(F32), 0.0)
        cur = w[k]
        w[k] = cur - dot3(cur, dot3(part, cur))

    def finish_inverse():
        w[2] = -dot3(w[1], dot3(mat(lbuf, 0, 1).astype(F32), w[0]))

    def put_x(i, x):
        hi = x.astype(BF16)
        xh[i] = hi
        xl[i] = (x - hi.astype(F32)).astype(BF16)

    def store(a, value):
        for b in range(parts):
            lin[a, pl.ds(b, tile, stride=parts), :] = value[:, b * LANE : (b + 1) * LANE]

    h[...] = jnp.zeros_like(h)

    def add_h(k, left, right):
        h[k] += outer(left, right).reshape(2, half, tile)

    def times_x(total, i, g):
        for part in (xl, xh):
            total = total - jnp.dot(g, part[i], preferred_element_type=F32)
        return total

    @pl.when(jnp.logical_not(panel))
    def _():
        loaded(1, 2, 3, 4)

        def relay(t, work=()):
            for k in range(SUB):
                with jax.named_scope("w_main"):
                    g_main(t, k)

                @pl.when(below)
                def _():
                    g_down(t, k, gbuf.at[p, t]).start()

                @pl.when(above)
                def _():
                    g_up(t, k, gbuf.at[p, t]).start()

                g_cross(t, k, gbuf.at[p, t]).start()
                if k < len(work):
                    work[k]()

        def use(t):
            with jax.named_scope("w_cross"):
                g_twin(t)
            right = mat(lv, first + t)
            add_h(0, mat(gbuf, 0, t), right)
            add_h(1, mat(gbuf, 1, t), right)

        def low(t):
            total = mat(gv, first + t).astype(F32)
            for s in range(2):
                total = times_x(total, s, mat(gbuf, s, t))
            store(first + t, total)

        main_l = (p == 0) | (c == 1)
        other_l = (p == 1) | (c == 1)

        for t in range(head):
            relay(t)
            if t == 0:
                with jax.named_scope("gather"):
                    gather_rows()

        with jax.named_scope("l_relay"):

            @pl.when(main_l & odd)
            def _():
                def step(k):
                    l_main(k)

                    @pl.when(below)
                    def _():
                        l_down(k, lbuf.at[p, c]).start()

                    @pl.when(above)
                    def _():
                        l_up(k, lbuf.at[p, c]).start()

                    l_cross(k, lbuf.at[p, c]).start()
                    l_share(p, k)

                loop(0, SUB, step)

        def share_first():
            @pl.when(main_l & jnp.logical_not(odd))
            def _():
                l_rest(p)

            @pl.when(other_l & odd)
            def _():
                def step(k):
                    l_twin(k)
                    l_share(1 - p, k)

                loop(0, SUB, step)

        def share_rest():
            @pl.when(other_l & jnp.logical_not(odd))
            def _():
                l_rest(1 - p)

        def share_done():
            k_wait(1 - c)
            l_full(0)

            @pl.when(c == 0)
            def _():
                l_full(1)

        steps = (lambda: None, share_first, lambda: None, share_rest, share_done)
        for j, share in enumerate(steps):
            if head + j < n:
                relay(head + j, (lambda: None, functools.partial(use, j - 1)) if j > 0 else ())
            with jax.named_scope("l_wait"):
                share()
        warm = min(head + len(steps), n)
        used = max(warm - head - 1, 0)

        start_inverse(0)
        start_inverse(1)

        base = warm
        lag = base - used
        double = min(n_lev // 2, n - base)

        def level_step(i):
            lev = 2 * (i - base) + 1

            def third():
                inverse_level(lev + 1, 0)
                use(i - lag)

            relay(
                i,
                (
                    lambda: inverse_level(lev, 0),
                    lambda: inverse_level(lev, 1),
                    third,
                    lambda: inverse_level(lev + 1, 1),
                ),
            )

        loop(base, base + double, level_step)
        used += double

        def level_rest(k):
            loop(2 * double + 1, n_lev + 1, lambda lev: inverse_level(lev, k))

        def x_first():
            put_x(0, dot3(w[0], mat(lk, 0).astype(F32)))

        def x_second():
            put_x(1, dot3(w[2], mat(lk, 0).astype(F32)) + dot3(w[1], mat(lk, 1).astype(F32)))

        def solve_x():
            x_first()
            x_second()
            loop(used, at - 1, use)

        at = base + double
        if at < n:
            relay(at, (lambda: level_rest(0), lambda: level_rest(1), finish_inverse, solve_x))
            used = at - 1
            at += 1
        else:
            level_rest(0)
            level_rest(1)
            finish_inverse()
            x_first()
            x_second()
        begun = at

        per = max(d for d in (1, 2, 3) if d == 1 or d * max(n - begun, 1) <= n - 2)

        def low_step(i):
            j = (i - begun) * per
            relay(i, [lambda: use(i - 2)] + [functools.partial(lambda d: low(j + d), d) for d in range(per)])

        loop(begun, n, low_step)
        lows = per * max(n - begun, 0)
        used += max(n - begun, 0)

        def send_t():
            loop(used, n, use)
            h0, h1 = mat(h, 0), mat(h, 1)

            def first_t():
                tout[1] = dot3(w[1], h1, 0, 0)

            def second_t():
                tout[0] = dot3(w[0], h0, 0, 0) + dot3(w[2], h1, 0, 0)

            for mine, one, two in ((0, first_t, second_t), (1, second_t, first_t)):

                @pl.when(c == mine)
                def _(one=one, two=two):
                    one()
                    t_mate().start()
                    two()

        def upper(a):
            store(a, mat(gv, a).astype(F32))

        @pl.when(jnp.logical_not(top))
        def _():
            send_t()
            with jax.named_scope("w_tmate"):
                t_mate().wait_recv()
            tout[c] += tin[...]
            t_root().start()
            loop(lows, n, low)
            loop(0, loc + 1, upper)

        @pl.when(top)
        def _():
            def s_relay(k):
                with jax.named_scope("w_s"):
                    s_main(k)

                @pl.when(below)
                def _():
                    s_down(k).start()

                @pl.when(above)
                def _():
                    s_up(k).start()

                s_cross(k).start()

            loop(0, CHUNKS, s_relay)
            send_t()
            loop(lows, n, low)
            loop(0, loc, upper)
            with jax.named_scope("w_s2"):
                s_twin()
            k0, k1 = mat(lk, 0).astype(F32), mat(lk, 1).astype(F32)
            total = mat(gv, loc).astype(F32) - dot3(mat(sbuf, 0), k0) - dot3(mat(sbuf, 1), k1)
            with jax.named_scope("w_tmate2"):
                t_mate().wait_recv()
            total = total - (tout[c] + tin[...])
            with jax.named_scope("w_tslot"):
                for k in range(pairs - 1):
                    rdma(tslot.at[k], tslot.at[k], ts.at[1], tr.at[k], {"row": mate}).wait_recv()
            for k in range(pairs - 1):
                total = total - tslot[k]
            store(loc, total)

        drain = jax.named_scope("drain")
        drain.__enter__()

        g_sent(1, gbuf.at[p])

        @pl.when(below)
        def _():
            g_sent(0, gbuf.at[p])

        @pl.when(above)
        def _():
            g_sent(2, gbuf.at[p])

        @pl.when(main_l)
        def _():
            l_sent(2 + p)

            @pl.when(odd)
            def _():
                l_sent(1)
                l_sent(4 + p)

            @pl.when(odd & below)
            def _():
                l_sent(0)

            @pl.when(odd & above)
            def _():
                l_sent(6)

        @pl.when(other_l)
        def _():
            l_sent(3 - p)

            @pl.when(odd)
            def _():
                l_sent(5 - p)

        t_mate().wait_send()

        @pl.when(jnp.logical_not(top))
        def _():
            t_root().wait_send()

        @pl.when(top)
        def _():
            s_sent(1)

            @pl.when(below)
            def _():
                s_sent(0)

            @pl.when(above)
            def _():
                s_sent(2)

        drain.__exit__(None, None, None)

    @pl.when(panel)
    def _():
        def each(body):
            def run(t):
                for k in range(SUB):
                    body(t, k)

            return run

        send = each(lambda t, k: g_down(t, k, gv.at[first + t]).start() if ring > 1 else None)
        cross_lo = each(lambda t, k: f_cross(t, k).start())
        cross_hi = each(lambda t, k: g_cross(t, k, gv.at[first + t]).start())
        lead = min(2, cut)
        mid = min(cut + 2, n)
        loaded(1)
        loop(0, head, send)

        @pl.when(p == 0)
        def _():
            loaded(2)
            loop(cut, mid, cross_lo)

        @pl.when(p == 1)
        def _():
            loop(0, lead, cross_hi)
            loaded(2)

        loaded(3, 4)
        @pl.when(jnp.logical_not(odd))
        def _():
            loop(head, n, send)

        with jax.named_scope("gather"):
            gather_rows()
            k_wait(1 - c)

        def send_l():
            @pl.when(odd)
            def _():
                def step(k):
                    if ring > 1:
                        l_down(k, lk.at[c]).start()
                    l_cross(k, lk.at[c]).start()

                loop(0, SUB, step)

        @pl.when(p == 0)
        def _():
            send_l()
            lbuf[0] = lk[...]
            loop(mid, n, cross_lo)

            @pl.when(top & (c == 1))
            def _():
                d_copy(1, gv.at[loc], 0, {"row": mate}).start()
                d_copy(1, gv.at[loc], 1, {"row": mate, "col": twin}).start()
                gd[1] = gv[loc]

        @pl.when(p == 1)
        def _():
            @pl.when(c == 1)
            def _():
                send_l()

            lbuf[1, 1] = lk[1]
            loop(lead, cut, cross_hi)

            @pl.when(top & (c == 1))
            def _():
                d_copy(2, gv.at[loc], 0, {"row": mate}).start()
                d_copy(2, gv.at[loc], 1, {"col": twin}).start()
                gd[2] = gv[loc]

        @pl.when(odd)
        def _():
            loop(head, n, send)

        with jax.named_scope("hd"):
            loop(0, n, lambda t: add_h(0, mat(gv, first + t), mat(lv, first + t)))
        h_mate(0).start()

        with jax.named_scope("l_wait"):
            @pl.when(((p == 1) | (c == 1)) & odd)
            def _():
                def step(k):
                    l_twin(k)
                    l_share(1 - p, k)

                loop(0, SUB, step)

            @pl.when(((p == 1) | (c == 1)) & jnp.logical_not(odd))
            def _():
                l_rest(1 - p)

            @pl.when(p == 1)
            def _():
                l_full(0)

            @pl.when((p == 0) & (c == 0))
            def _():
                l_full(1)

        def reduce_mate(k):
            with jax.named_scope("w_hmate"):
                h_mate(k).wait_recv()
            hsum[k] = h[k, c] + hin[k]

            @pl.when(jnp.logical_not(top))
            def _():
                h_root(k).start()

        def reduce_root(k):
            total = hsum[k]
            for i in range(pairs - 1):
                with jax.named_scope("w_hroot"):
                    ref = hslot.at[k, i]
                    rdma(ref, ref, hs.at[2 + k], hq.at[k, i], {"row": mate}).wait_recv()
                total = total + hslot[k, i]
            hsum[k] = total
            h_twin(k).start()

        start_inverse(0)
        start_inverse(1)
        reduce_mate(0)

        def level(lev):
            inverse_level(lev, 0)
            inverse_level(lev, 1)

        early = (n_lev + 1) // 2
        loop(1, early + 1, level)

        @pl.when(top)
        def _():
            reduce_root(0)

        loop(early + 1, n_lev + 1, level)
        finish_inverse()

        @pl.when(p == 0)
        def _():
            def use(t):
                with jax.named_scope("w_x"):
                    g_twin(t)
                add_h(1, mat(gbuf, 1, t), mat(lv, first + t))

            loop(0, cut, use)

        @pl.when(p == 1)
        def _():
            def use(t):
                with jax.named_scope("w_x"):
                    g_twin(t)
                add_h(1, mat(gv, first + t), mat(gbuf, 0, t))

            loop(cut, n, use)

        h_mate(1).start()

        @pl.when(top & (c == 1) & (p == 0))
        def _():
            d_wait(2)
            d_copy(2, gd.at[2], 2, {"row": mate}).start()

        reduce_mate(1)

        @pl.when(top)
        def _():
            reduce_root(1)

        @pl.when(p == 1)
        def _():
            loop(cut, n, cross_hi)

        @pl.when(top)
        def _():
            with jax.named_scope("w_htwin"):
                for k in range(2):
                    h_twin(k).wait_recv()
            mine, theirs = hsum[0], htwin[0]
            hfull[c, 0] = jnp.where(p == 0, mine, theirs)
            hfull[c, 2] = jnp.where(p == 0, theirs, mine)
            hfull[c, 1] = hsum[1] + htwin[1]
            h_full().start()
            with jax.named_scope("w_hfull"):
                ref = hfull.at[1 - c]
                rdma(ref, ref, hs.at[4], hr.at[4], {"row": mate}).wait_recv()

                @pl.when(c == 0)
                def _():
                    d_wait(1)
                    d_wait(2)

            eye = (rows == cols).astype(F32)

            def keep(x):
                return jnp.where(rows >= cols, x, 0.0)

            w66, w77, w76 = w[0], w[1], w[2]
            l77 = mat(lbuf, 1, 1).astype(F32)
            g_here = mat(gv, loc).astype(F32)

            def full(k):
                return jnp.concatenate([hfull[0, k], hfull[1, k]], 0)

            q77 = keep(mat(gd, 2).astype(F32) - dot3(w77, full(2), 0, 0))
            m77 = dot3(l77, q77, 0, 0)
            phi77 = keep(m77) - 0.5 * m77 * eye

            def put_s(s, o):
                sbuf[p] = s.reshape(CHUNKS, tile // CHUNKS, tile)
                if ring > 1:
                    loop(0, CHUNKS, lambda k: s_down(k).start())
                store(loc, o)

            def tri(s):
                return keep(s) - 0.5 * s * eye

            @pl.when((c == 1) & (p == 1))
            def _():
                half77 = dot3(dot3(w77, phi77, 0, 0), w77)
                s = half77 + half77.T
                put_s(s, tri(s))

            @pl.when(jnp.logical_not((c == 1) & (p == 1)))
            def _():
                g76 = jnp.where(c == 1, g_here, mat(gd, 1).astype(F32))
                q76 = g76 - dot3(w77, full(1), 0, 0)
                phi76 = dot3(l77, q76, 0, 0)

                @pl.when((c == 0) & (p == 0))
                def _():
                    t66 = dot3(w66, full(0), 0, 0) + dot3(w76, full(1), 0, 0)
                    q66 = keep(g_here - t66)
                    l66, l76 = mat(lbuf, 0, 0).astype(F32), mat(lbuf, 0, 1).astype(F32)
                    m66 = dot3(l66, q66, 0, 0) + dot3(l76, q76, 0, 0)
                    phi66 = keep(m66) - 0.5 * m66 * eye
                    inner = dot3(phi76, w66) + dot3(phi77, w76)
                    half66 = dot3(w66, dot3(phi66, w66), 0, 0) + dot3(w76, inner, 0, 0)
                    s = half66 + half66.T
                    put_s(s, tri(s))

                @pl.when(jnp.logical_not((c == 0) & (p == 0)))
                def _():
                    inner = dot3(phi76, w66) + dot3(phi77 + phi77.T, w76)

                    @pl.when(c == 1)
                    def _():
                        s = dot3(w77, inner, 0, 0)
                        put_s(s, s)

                    @pl.when(c == 0)
                    def _():
                        put_s(dot3(inner, w77, 0, 0), jnp.zeros((tile, tile), F32))

        zero = jnp.zeros((tile, tile), F32)
        loop(0, loc, lambda a: store(a, zero))

        @pl.when(jnp.logical_not(top))
        def _():
            store(loc, zero)

        put_x(1, jnp.where(p == 0, -w[2], -w[1]))

        with jax.named_scope("low"):

            @pl.when(p == 0)
            def _():
                put_x(0, -w[0])

                def low(t):
                    total = times_x(zero, 0, mat(gv, first + t))
                    store(first + t, times_x(total, 1, mat(gbuf, 1, t)))

                def late(t):
                    g_twin(t)
                    low(t)

                loop(0, cut, low)
                loop(cut, n, late)

            @pl.when(p == 1)
            def _():
                loop(0, n, lambda t: store(first + t, times_x(zero, 1, mat(gv, first + t))))

        drain = jax.named_scope("drain")
        drain.__enter__()

        @pl.when(p == 0)
        def _():
            g_sent(1, gbuf.at[0, pl.ds(cut, n - cut)])

            @pl.when(top & (c == 1))
            def _():
                d_copy(1, gv.at[loc], 0, {"row": mate}).wait_send()
                d_copy(1, gv.at[loc], 1, {"row": mate, "col": twin}).wait_send()
                d_copy(2, gd.at[2], 2, {"row": mate}).wait_send()

        @pl.when(p == 1)
        def _():
            g_sent(1, gbuf.at[1])

            @pl.when(top & (c == 1))
            def _():
                d_copy(2, gv.at[loc], 0, {"row": mate}).wait_send()
                d_copy(2, gv.at[loc], 1, {"col": twin}).wait_send()

        @pl.when(((p == 0) | (c == 1)) & odd)
        def _():
            l_sent(1)
            if ring > 1:
                l_sent(0)

        @pl.when((p == 1) | (c == 1))
        def _():
            l_sent(3 - p)

            @pl.when(odd)
            def _():
                l_sent(5 - p)

        if ring > 1:
            g_sent(0, gbuf.at[p])
        for k in range(2):
            h_mate(k).wait_send()

            @pl.when(jnp.logical_not(top))
            def _():
                h_root(k).wait_send()

            @pl.when(top)
            def _():
                h_twin(k).wait_send()

        @pl.when(top)
        def _():
            h_full().wait_send()
            if ring > 1:
                s_sent(0)

        drain.__exit__(None, None, None)

    @pl.when(top)
    def _():
        for k in range(pairs - 1):
            k_star(k).wait_send()
        k_mate(lv.at[loc]).wait_send()

    @pl.when(jnp.logical_not(top))
    def _():
        k_mate(lk.at[c]).wait_send()


def panel(factor, grad, n_row, n_col, first):
    rows_here, tile = factor.shape[0], factor.shape[1]
    n = rows_here - first
    half = tile // 2
    pairs = n_row // 2
    sub = (SUB, tile // SUB, tile)
    hbm = pl.BlockSpec(memory_space=pltpu.HBM)
    dma = pltpu.SemaphoreType.DMA
    return pl.pallas_call(
        functools.partial(panel_kernel, n_row, n_col),
        out_shape=jax.ShapeDtypeStruct((rows_here, tile * tile // LANE, LANE), F32),
        in_specs=[hbm, hbm],
        out_specs=pl.BlockSpec(memory_space=pltpu.VMEM),
        scratch_shapes=[
            pltpu.VMEM((rows_here, *sub), BF16),
            pltpu.VMEM((rows_here, *sub), BF16),
            pltpu.VMEM((2, n, *sub), BF16),
            pltpu.VMEM((2, tile, tile), BF16),
            pltpu.VMEM((2, tile, tile), BF16),
            pltpu.VMEM((2, *sub), BF16),
            pltpu.VMEM((2, 2, *sub), BF16),
            pltpu.VMEM((3, tile, tile), F32),
            pltpu.VMEM((2, 2, half, tile), F32),
            pltpu.VMEM((2, tile, tile), F32),
            pltpu.VMEM((tile, tile), F32),
            pltpu.VMEM((pairs, tile, tile), F32),
            pltpu.VMEM((2, half, tile), F32),
            pltpu.VMEM((2, half, tile), F32),
            pltpu.VMEM((2, pairs, half, tile), F32),
            pltpu.VMEM((2, half, tile), F32),
            pltpu.VMEM((2, 3, half, tile), F32),
            pltpu.VMEM((3, *sub), BF16),
            pltpu.VMEM((2, CHUNKS, tile // CHUNKS, tile), F32),
            dma((5,)),
            dma((3,)),
            dma((n, SUB)),
            dma((n,)),
            dma((7,)),
            dma((SUB,)),
            dma((SUB,)),
            dma((2,)),
            dma((2,)),
            dma((pairs + 1,)),
            dma((2,)),
            dma((2,)),
            dma((pairs + 1,)),
            dma((5,)),
            dma((5,)),
            dma((2, pairs)),
            dma((3,)),
            dma((3,)),
            dma((3,)),
            dma((CHUNKS,)),
            dma((1,)),
        ],
        compiler_params=pltpu.CompilerParams(
            collective_id=0, has_side_effects=True, vmem_limit_bytes=VMEM
        ),
        name="panel",
    )(
        pltpu.with_memory_space_constraint(factor.reshape(rows_here, *sub), pltpu.HBM),
        pltpu.with_memory_space_constraint(grad.reshape(rows_here, *sub), pltpu.HBM),
    )


def per_device(l_saved, l_grad):
    rows_here, tile = l_saved.shape[0], l_saved.shape[2]
    n_row = lax.axis_size("row")
    n_col = lax.axis_size("col")
    assert n_col % n_row == 0 and n_row % 4 == 0 and tile % (SUB * 16) == 0
    first = n_col // n_row
    factor = l_saved.reshape(rows_here, tile, tile)
    grad = l_grad.reshape(rows_here, tile, tile)
    lin = panel(factor, grad, n_row, n_col, first)
    return lin.reshape(l_grad.shape)


def solution(mesh):
    spec = P(None, "row", None, "col", None)
    return jax.shard_map(
        per_device, mesh=mesh, in_specs=(spec, spec), out_specs=spec, check_vma=False
    )
```

```python
import functools

import jax
import jax.numpy as jnp
from jax import lax
from jax.experimental import pallas as pl
from jax.experimental.pallas import tpu as pltpu
from jax.sharding import PartitionSpec as P

F32 = jnp.float32
BF16 = jnp.bfloat16
HIGH3 = lax.Precision.HIGH
MESH = pl.DeviceIdType.MESH
CHUNKS = 8
SUB = 4
LANE = 128
VMEM = 40 * 1024 * 1024


def dot3(a, b, ca=1, cb=0):
    return lax.dot_general(
        a, b, (((ca,), (cb,)), ((), ())), precision=HIGH3, preferred_element_type=F32
    )


def outer(a, b):
    return lax.dot_general(a, b, (((0,), (0,)), ((), ())), preferred_element_type=F32)


def panel_kernel(
    n_row,
    n_col,
    l_hbm,
    g_hbm,
    lin,
    lv,
    gv,
    gbuf,
    xh,
    xl,
    lk,
    lbuf,
    w,
    h,
    own,
    tout,
    tin,
    tslot,
    hin,
    hsum,
    hslot,
    htwin,
    hfull,
    gd,
    sbuf,
    vs,
    gs,
    gm,
    gx,
    ls,
    lm,
    lx,
    lf,
    lp,
    ks,
    kr,
    ts,
    tr,
    hs,
    hr,
    hq,
    ds,
    dr,
    ss,
    sm,
    sx,
):
    held, tile = lv.shape[0], lv.shape[3]
    half = tile // 2
    n = gbuf.shape[1]
    first = held - n
    loc = first - 1
    ring = n_col // 2
    cut = n // 2
    head = min(2, n)
    pairs = n_row // 2
    parts = tile // LANE

    row = lax.axis_index("row")
    col = lax.axis_index("col")
    q, p = col // 2, col % 2
    y, c = row // 2, row % 2
    panel = q == ring - 1
    top = y == pairs - 1
    hub = max(ring - 3, 0)
    other = jnp.logical_not(panel)
    below = (q > 0) & (q <= hub)
    above = (q == hub) & (q < ring - 2)
    lower = jnp.where(panel, 2 * hub + p, jnp.maximum(col - 2, 0))
    upper_col = jnp.minimum(col + 2, n_col - 1)
    feeder = jnp.where(q == hub, n_col - 2 + p, jnp.where(q < hub, upper_col, lower))
    twin = 2 * q + 1 - p
    mate = 2 * y + 1 - c
    odd = y % 2 == 1
    pal = 2 * (y + 1 - 2 * (y % 2)) + c
    root = n_row - 2 + c

    rows = lax.broadcasted_iota(jnp.int32, (tile, tile), 0)
    cols = lax.broadcasted_iota(jnp.int32, (tile, tile), 1)

    def rdma(src, dst, s_sem, r_sem, dev):
        return pltpu.make_async_remote_copy(
            src_ref=src, dst_ref=dst, send_sem=s_sem, recv_sem=r_sem, device_id=dev, device_id_type=MESH
        )

    def loop(a, b, body):
        def step(i, carry):
            body(i)
            return carry

        if a < b:
            lax.fori_loop(a, b, step, 0)

    def load(src, dst, k, a, b):
        return pltpu.make_async_copy(src.at[pl.ds(a, b - a)], dst.at[pl.ds(a, b - a)], vs.at[k])

    spans = [
        (l_hbm, lv, 0, loc, first),
        (g_hbm, gv, 1, first, first + head),
        (l_hbm, lv, 2, first, held),
        (g_hbm, gv, 3, first + head, held),
        (g_hbm, gv, 4, 0, first),
    ]
    loads = {span[2]: load(*span) for span in spans if span[3] < span[4]}
    for cp in loads.values():
        cp.start()

    def loaded(*ks):
        for k in ks:
            if k in loads:
                loads[k].wait()

    barrier = pltpu.get_barrier_semaphore()

    def greet(dev):
        pl.semaphore_signal(barrier, inc=1, device_id=dev, device_id_type=MESH)

    greet({"col": twin})
    greet({"row": mate})
    greet({"row": pal})

    @pl.when(below | panel)
    def _():
        greet({"col": lower})

    @pl.when(above)
    def _():
        greet({"col": upper_col})

    @pl.when(other)
    def _():
        greet({"col": feeder})

    @pl.when(jnp.logical_not(top))
    def _():
        greet({"row": root})

    @pl.when(top)
    def _():
        for k in range(pairs - 1):
            greet({"row": 2 * k + c})

    @pl.when(top & panel)
    def _():
        greet({"row": mate, "col": twin})

    heard = (
        3
        + (below | panel).astype(jnp.int32)
        + above.astype(jnp.int32)
        + other.astype(jnp.int32)
        + jnp.where(top, pairs - 1, 1)
        + (top & panel).astype(jnp.int32)
    )
    with jax.named_scope("barrier"):
        pl.semaphore_wait(barrier, heard)

    loaded(0)

    def mat(ref, *at):
        return ref[at].reshape(tile, tile)

    def g_down(t, k, src):
        return rdma(src.at[k], gbuf.at[p, t, k], gs.at[0], gm.at[t, k], {"col": lower})

    def g_up(t, k, src):
        return rdma(src.at[k], gbuf.at[p, t, k], gs.at[2], gm.at[t, k], {"col": upper_col})

    def g_cross(t, k, src):
        return rdma(src.at[k], gbuf.at[p, t, k], gs.at[1], gx.at[t], {"col": twin})

    def f_cross(t, k):
        return rdma(lv.at[first + t, k], gbuf.at[0, t, k], gs.at[1], gx.at[t], {"col": twin})

    def g_main(t, k):
        ref = gbuf.at[p, t, k]
        rdma(ref, ref, gs.at[0], gm.at[t, k], {"col": twin}).wait_recv()

    def g_twin(t):
        ref = gbuf.at[1 - p, t]
        rdma(ref, ref, gs.at[1], gx.at[t], {"col": twin}).wait_recv()

    def g_sent(k, ref):
        rdma(ref, ref, gs.at[k], gx.at[0], {"col": twin}).wait_send()

    def l_down(k, src):
        return rdma(src.at[k], lbuf.at[p, c, k], ls.at[0], lm.at[k], {"col": lower})

    def l_up(k, src):
        return rdma(src.at[k], lbuf.at[p, c, k], ls.at[6], lm.at[k], {"col": upper_col})

    def l_cross(k, src):
        return rdma(src.at[k], lbuf.at[p, c, k], ls.at[1], lx.at[k], {"col": twin})

    def l_share(s, k):
        ref = lbuf.at[s, c, k]
        rdma(ref, ref, ls.at[4 + s], lp.at[s], {"row": pal}).start()
        rdma(ref, ref, ls.at[2 + s], lf.at[s], {"row": mate}).start()

    def l_main(k):
        ref = lbuf.at[p, c, k]
        rdma(ref, ref, ls.at[0], lm.at[k], {"col": twin}).wait_recv()

    def l_twin(k):
        ref = lbuf.at[1 - p, c, k]
        rdma(ref, ref, ls.at[1], lx.at[k], {"col": twin}).wait_recv()

    def l_rest(s):
        ref = lbuf.at[s, c]
        rdma(ref, ref, ls.at[4], lp.at[s], {"row": pal}).wait_recv()
        rdma(ref, ref, ls.at[2 + s], lf.at[s], {"row": mate}).start()

    def l_full(s):
        ref = lbuf.at[s, 1 - c]
        rdma(ref, ref, ls.at[2], lf.at[s], {"row": mate}).wait_recv()

    def l_sent(k):
        ref = lbuf.at[0, 0]
        rdma(ref, ref, ls.at[k], lf.at[0], {"row": mate}).wait_send()

    def k_star(k):
        return rdma(lv.at[loc], lk.at[c], ks.at[k], kr.at[c], {"row": 2 * k + c})

    def k_mate(src):
        return rdma(src, lk.at[c], ks.at[pairs], kr.at[c], {"row": mate})

    def k_wait(i):
        rdma(lk.at[i], lk.at[i], ks.at[pairs], kr.at[i], {"row": mate}).wait_recv()

    def t_mate():
        return rdma(h.at[1 - c], tin, ts.at[0], tr.at[pairs], {"row": mate})

    def t_root():
        return rdma(tout.at[0], tslot.at[y], ts.at[1], tr.at[y], {"row": root})

    def t_all():
        return rdma(tout.at[0], tout.at[1], ts.at[2], tr.at[pairs + 1], {"row": mate})

    def h_mate(k):
        return rdma(h.at[k, 1 - c], hin.at[k], hs.at[k], hr.at[k], {"row": mate})

    def h_root(k):
        return rdma(hsum.at[k], hslot.at[k, y], hs.at[2 + k], hq.at[k, y], {"row": root})

    def h_twin(k):
        return rdma(hsum.at[k], htwin.at[k], hs.at[2 + k], hr.at[2 + k], {"col": twin})

    def h_full():
        return rdma(hfull.at[c], hfull.at[c], hs.at[4], hr.at[4], {"row": mate})

    def d_copy(k, src, i, dev):
        return rdma(src, gd.at[k], ds.at[i], dr.at[k], dev)

    def d_wait(k):
        d_copy(k, gd.at[k], 0, {"row": mate}).wait_recv()

    def s_down(k):
        return rdma(sbuf.at[p, k], sbuf.at[p, k], ss.at[0], sm.at[k], {"col": lower})

    def s_up(k):
        return rdma(sbuf.at[p, k], sbuf.at[p, k], ss.at[2], sm.at[k], {"col": upper_col})

    def s_cross(k):
        return rdma(sbuf.at[p, k], sbuf.at[p, k], ss.at[1], sx.at[0], {"col": twin})

    def s_main(k):
        s_down(k).wait_recv()

    def s_twin():
        ref = sbuf.at[1 - p]
        rdma(ref, ref, ss.at[1], sx.at[0], {"col": twin}).wait_recv()

    def s_sent(k):
        ref = sbuf.at[p]
        rdma(ref, ref, ss.at[k], sx.at[0], {"col": twin}).wait_send()

    @pl.when(top)
    def _():
        for k in range(pairs - 1):
            k_star(k).start()
        k_mate(lv.at[loc]).start()
        lk[c] = lv[loc]

    def gather_rows():
        @pl.when(jnp.logical_not(top))
        def _():
            k_wait(c)
            k_mate(lk.at[c]).start()

    def start_inverse(k):
        d = mat(lbuf, k, k).astype(F32)
        e = (rows == cols).astype(F32)
        on = d * e
        rc = 1.0 / jnp.sum(on, axis=1, keepdims=True)
        rr = 1.0 / jnp.sum(on, axis=0, keepdims=True)
        off = ((rows & 1) == 1) & (cols == rows - 1)
        w[k] = e * rr - rc * jnp.where(off, d, 0.0) * rr

    n_lev = tile.bit_length() - 2

    def inverse_level(sh, k):
        off = ((jnp.right_shift(rows, sh) & 1) == 1) & (
            jnp.right_shift(cols, sh) == jnp.right_shift(rows, sh) - 1
        )
        part = jnp.where(off, mat(lbuf, k, k).astype(F32), 0.0)
        cur = w[k]
        w[k] = cur - dot3(cur, dot3(part, cur))

    def finish_inverse():
        w[2] = -dot3(w[1], dot3(mat(lbuf, 0, 1).astype(F32), w[0]))

    def put_x(i, x):
        hi = x.astype(BF16)
        xh[i] = hi
        xl[i] = (x - hi.astype(F32)).astype(BF16)

    def store(a, value):
        for b in range(parts):
            lin[a, pl.ds(b, tile, stride=parts), :] = value[:, b * LANE : (b + 1) * LANE]

    h[...] = jnp.zeros_like(h)

    def add_h(k, left, right):
        h[k] += outer(left, right).reshape(2, half, tile)

    def times_x(total, i, g):
        for part in (xl, xh):
            total = total - jnp.dot(g, part[i], preferred_element_type=F32)
        return total

    @pl.when(jnp.logical_not(panel))
    def _():
        loaded(1, 2, 3, 4)

        def relay(t, work=()):
            for k in range(SUB):
                with jax.named_scope("w_main"):
                    g_main(t, k)

                @pl.when(below)
                def _():
                    g_down(t, k, gbuf.at[p, t]).start()

                @pl.when(above)
                def _():
                    g_up(t, k, gbuf.at[p, t]).start()

                g_cross(t, k, gbuf.at[p, t]).start()
                if k < len(work):
                    work[k]()

        def use(t):
            with jax.named_scope("w_cross"):
                g_twin(t)
            right = mat(lv, first + t)
            add_h(0, mat(gbuf, 0, t), right)
            add_h(1, mat(gbuf, 1, t), right)

        def low(t):
            total = mat(gv, first + t).astype(F32)
            for s in range(2):
                total = times_x(total, s, mat(gbuf, s, t))
            store(first + t, total)

        main_l = (p == 0) | (c == 1)
        other_l = (p == 1) | (c == 1)

        for t in range(head):
            relay(t)
            if t == 0:
                with jax.named_scope("gather"):
                    gather_rows()

        with jax.named_scope("l_relay"):

            @pl.when(main_l & odd)
            def _():
                def step(k):
                    l_main(k)

                    @pl.when(below)
                    def _():
                        l_down(k, lbuf.at[p, c]).start()

                    @pl.when(above)
                    def _():
                        l_up(k, lbuf.at[p, c]).start()

                    l_cross(k, lbuf.at[p, c]).start()
                    l_share(p, k)

                loop(0, SUB, step)

        def share_first():
            @pl.when(main_l & jnp.logical_not(odd))
            def _():
                l_rest(p)

            @pl.when(other_l & odd)
            def _():
                def step(k):
                    l_twin(k)
                    l_share(1 - p, k)

                loop(0, SUB, step)

        def share_rest():
            @pl.when(other_l & jnp.logical_not(odd))
            def _():
                l_rest(1 - p)

        def share_done():
            k_wait(1 - c)
            l_full(0)

            @pl.when(c == 0)
            def _():
                l_full(1)

        steps = (lambda: None, share_first, lambda: None, share_rest, share_done)
        for j, share in enumerate(steps):
            if head + j < n:
                relay(head + j, (lambda: None, functools.partial(use, j - 1)) if j > 0 else ())
            with jax.named_scope("l_wait"):
                share()
        warm = min(head + len(steps), n)
        used = max(warm - head - 1, 0)

        start_inverse(0)
        start_inverse(1)

        base = warm
        lag = base - used
        double = min(n_lev // 2, n - base)

        def level_step(i):
            lev = 2 * (i - base) + 1

            def third():
                inverse_level(lev + 1, 0)
                use(i - lag)

            relay(
                i,
                (
                    lambda: inverse_level(lev, 0),
                    lambda: inverse_level(lev, 1),
                    third,
                    lambda: inverse_level(lev + 1, 1),
                ),
            )

        loop(base, base + double, level_step)
        used += double

        def level_rest(k):
            loop(2 * double + 1, n_lev + 1, lambda lev: inverse_level(lev, k))

        def x_first():
            put_x(0, dot3(w[0], mat(lk, 0).astype(F32)))

        def x_second():
            put_x(1, dot3(w[2], mat(lk, 0).astype(F32)) + dot3(w[1], mat(lk, 1).astype(F32)))

        def solve_x():
            x_first()
            x_second()
            loop(used, at - 1, use)

        at = base + double
        if at < n:
            relay(at, (lambda: level_rest(0), lambda: level_rest(1), finish_inverse, solve_x))
            used = at - 1
            at += 1
        else:
            level_rest(0)
            level_rest(1)
            finish_inverse()
            x_first()
            x_second()
        begun = at

        per = max(d for d in (1, 2, 3) if d == 1 or d * max(n - begun, 1) <= n - 2)

        def low_step(i):
            j = (i - begun) * per
            relay(i, [lambda: use(i - 2)] + [functools.partial(lambda d: low(j + d), d) for d in range(per)])

        loop(begun, n, low_step)
        lows = per * max(n - begun, 0)
        used += max(n - begun, 0)

        def use_main(t):
            add_h(p, mat(gbuf, p, t), mat(lv, first + t))

        def use_twin(t):
            with jax.named_scope("w_cross"):
                g_twin(t)
            add_h(1 - p, mat(gbuf, 1 - p, t), mat(lv, first + t))

        def give():
            t_mate().start()

        def take():
            with jax.named_scope("w_tmate"):
                t_mate().wait_recv()
            tout[0] = h[c] + tin[...]

        def upper(a):
            store(a, mat(gv, a).astype(F32))

        @pl.when(jnp.logical_not(top))
        def _():
            loop(used, n, use_main)

            @pl.when(c != p)
            def _():
                give()

            @pl.when(c == p)
            def _():
                take()
                t_root().start()

            loop(used, n, use_twin)

            @pl.when(c == p)
            def _():
                give()

            @pl.when(c != p)
            def _():
                take()
                t_root().start()

            loop(lows, n, low)
            loop(0, loc + 1, upper)

        @pl.when(top)
        def _():
            def s_relay(k):
                with jax.named_scope("w_s"):
                    s_main(k)

                @pl.when(below)
                def _():
                    s_down(k).start()

                @pl.when(above)
                def _():
                    s_up(k).start()

                s_cross(k).start()

            early = max(min(CHUNKS, used - lows), 0)

            def give_twin():
                @pl.when(c == p)
                def _():
                    give()

            loop(used, n, use_main)

            @pl.when(c != p)
            def _():
                give()

            rest = list(range(used, n))
            for k in range(CHUNKS):
                s_relay(k)
                if k < early:
                    low(lows + k)
                if rest and k % 2 == 1 and k >= CHUNKS // 2 - 1:
                    use_twin(rest.pop(0))
                    if not rest:
                        give_twin()
            if rest:
                loop(rest[0], n, use_twin)
                give_twin()

            loop(lows + early, n, low)
            loop(0, loc, upper)
            total = mat(gv, loc).astype(F32) - dot3(mat(sbuf, p), mat(lk, p).astype(F32))
            take()
            with jax.named_scope("w_tslot"):
                for k in range(pairs - 1):
                    rdma(tslot.at[k], tslot.at[k], ts.at[1], tr.at[k], {"row": mate}).wait_recv()
            for k in range(pairs - 1):
                tout[0] += tslot[k]
            own[...] = total

            @pl.when(c == 1)
            def _():
                t_all().start()
                own[...] -= dot3(w[1], mat(tout, 0), 0, 0)

            @pl.when(c == 0)
            def _():
                own[...] -= dot3(w[0], mat(tout, 0), 0, 0)
                with jax.named_scope("w_tall"):
                    t_all().wait_recv()
                own[...] -= dot3(w[2], mat(tout, 1), 0, 0)

            with jax.named_scope("w_s2"):
                s_twin()
            store(loc, own[...] - dot3(mat(sbuf, 1 - p), mat(lk, 1 - p).astype(F32)))

        drain = jax.named_scope("drain")
        drain.__enter__()

        g_sent(1, gbuf.at[p])

        @pl.when(below)
        def _():
            g_sent(0, gbuf.at[p])

        @pl.when(above)
        def _():
            g_sent(2, gbuf.at[p])

        @pl.when(main_l)
        def _():
            l_sent(2 + p)

            @pl.when(odd)
            def _():
                l_sent(1)
                l_sent(4 + p)

            @pl.when(odd & below)
            def _():
                l_sent(0)

            @pl.when(odd & above)
            def _():
                l_sent(6)

        @pl.when(other_l)
        def _():
            l_sent(3 - p)

            @pl.when(odd)
            def _():
                l_sent(5 - p)

        t_mate().wait_send()

        @pl.when(jnp.logical_not(top))
        def _():
            t_root().wait_send()

        @pl.when(top & (c == 1))
        def _():
            t_all().wait_send()

        @pl.when(top)
        def _():
            s_sent(1)

            @pl.when(below)
            def _():
                s_sent(0)

            @pl.when(above)
            def _():
                s_sent(2)

        drain.__exit__(None, None, None)

    @pl.when(panel)
    def _():
        def each(body):
            def run(t):
                for k in range(SUB):
                    body(t, k)

            return run

        send = each(lambda t, k: g_down(t, k, gv.at[first + t]).start() if ring > 1 else None)
        cross_lo = each(lambda t, k: f_cross(t, k).start())
        cross_hi = each(lambda t, k: g_cross(t, k, gv.at[first + t]).start())
        lead = min(2, cut)
        mid = min(cut + 2, n)
        loaded(1)
        loop(0, head, send)

        @pl.when(p == 0)
        def _():
            loaded(2)
            loop(cut, mid, cross_lo)

        @pl.when(p == 1)
        def _():
            loop(0, lead, cross_hi)
            loaded(2)

        loaded(3, 4)
        @pl.when(jnp.logical_not(odd))
        def _():
            loop(head, n, send)

        with jax.named_scope("gather"):
            gather_rows()
            k_wait(1 - c)

        def send_l():
            @pl.when(odd)
            def _():
                def step(k):
                    if ring > 1:
                        l_down(k, lk.at[c]).start()
                    l_cross(k, lk.at[c]).start()

                loop(0, SUB, step)

        @pl.when(p == 0)
        def _():
            send_l()
            lbuf[0] = lk[...]
            loop(mid, n, cross_lo)

            @pl.when(top & (c == 1))
            def _():
                d_copy(1, gv.at[loc], 0, {"row": mate}).start()
                d_copy(1, gv.at[loc], 1, {"row": mate, "col": twin}).start()
                gd[1] = gv[loc]

        @pl.when(p == 1)
        def _():
            @pl.when(c == 1)
            def _():
                send_l()

            lbuf[1, 1] = lk[1]
            loop(lead, cut, cross_hi)

            @pl.when(top & (c == 1))
            def _():
                d_copy(2, gv.at[loc], 0, {"row": mate}).start()
                d_copy(2, gv.at[loc], 1, {"col": twin}).start()
                gd[2] = gv[loc]

        @pl.when(odd)
        def _():
            loop(head, n, send)

        with jax.named_scope("hd"):
            loop(0, n, lambda t: add_h(0, mat(gv, first + t), mat(lv, first + t)))
        h_mate(0).start()

        with jax.named_scope("l_wait"):
            @pl.when(((p == 1) | (c == 1)) & odd)
            def _():
                def step(k):
                    l_twin(k)
                    l_share(1 - p, k)

                loop(0, SUB, step)

            @pl.when(((p == 1) | (c == 1)) & jnp.logical_not(odd))
            def _():
                l_rest(1 - p)

            @pl.when(p == 1)
            def _():
                l_full(0)

            @pl.when((p == 0) & (c == 0))
            def _():
                l_full(1)

        def reduce_mate(k):
            with jax.named_scope("w_hmate"):
                h_mate(k).wait_recv()
            hsum[k] = h[k, c] + hin[k]

            @pl.when(jnp.logical_not(top))
            def _():
                h_root(k).start()

        def reduce_root(k):
            total = hsum[k]
            for i in range(pairs - 1):
                with jax.named_scope("w_hroot"):
                    ref = hslot.at[k, i]
                    rdma(ref, ref, hs.at[2 + k], hq.at[k, i], {"row": mate}).wait_recv()
                total = total + hslot[k, i]
            hsum[k] = total
            h_twin(k).start()

        start_inverse(0)
        start_inverse(1)
        reduce_mate(0)

        def level(lev):
            inverse_level(lev, 0)
            inverse_level(lev, 1)

        early = (n_lev + 1) // 2
        loop(1, early + 1, level)

        @pl.when(top)
        def _():
            reduce_root(0)

        loop(early + 1, n_lev + 1, level)
        finish_inverse()

        @pl.when(p == 0)
        def _():
            def use(t):
                with jax.named_scope("w_x"):
                    g_twin(t)
                add_h(1, mat(gbuf, 1, t), mat(lv, first + t))

            loop(0, cut, use)

        @pl.when(p == 1)
        def _():
            def use(t):
                with jax.named_scope("w_x"):
                    g_twin(t)
                add_h(1, mat(gv, first + t), mat(gbuf, 0, t))

            loop(cut, n, use)

        h_mate(1).start()

        @pl.when(top & (c == 1) & (p == 0))
        def _():
            d_wait(2)
            d_copy(2, gd.at[2], 2, {"row": mate}).start()

        reduce_mate(1)

        @pl.when(top)
        def _():
            reduce_root(1)

        @pl.when(p == 1)
        def _():
            loop(cut, n, cross_hi)

        @pl.when(top)
        def _():
            with jax.named_scope("w_htwin"):
                for k in range(2):
                    h_twin(k).wait_recv()
            mine, theirs = hsum[0], htwin[0]
            hfull[c, 0] = jnp.where(p == 0, mine, theirs)
            hfull[c, 2] = jnp.where(p == 0, theirs, mine)
            hfull[c, 1] = hsum[1] + htwin[1]
            h_full().start()
            with jax.named_scope("w_hfull"):
                ref = hfull.at[1 - c]
                rdma(ref, ref, hs.at[4], hr.at[4], {"row": mate}).wait_recv()

                @pl.when(c == 0)
                def _():
                    d_wait(1)
                    d_wait(2)

            eye = (rows == cols).astype(F32)

            def keep(x):
                return jnp.where(rows >= cols, x, 0.0)

            w66, w77, w76 = w[0], w[1], w[2]
            l77 = mat(lbuf, 1, 1).astype(F32)
            g_here = mat(gv, loc).astype(F32)

            def full(k):
                return jnp.concatenate([hfull[0, k], hfull[1, k]], 0)

            q77 = keep(mat(gd, 2).astype(F32) - dot3(w77, full(2), 0, 0))
            m77 = dot3(l77, q77, 0, 0)
            phi77 = keep(m77) - 0.5 * m77 * eye

            def put_s(s, o):
                sbuf[p] = s.reshape(CHUNKS, tile // CHUNKS, tile)
                if ring > 1:
                    loop(0, CHUNKS, lambda k: s_down(k).start())
                store(loc, o)

            def tri(s):
                return keep(s) - 0.5 * s * eye

            @pl.when((c == 1) & (p == 1))
            def _():
                half77 = dot3(dot3(w77, phi77, 0, 0), w77)
                s = half77 + half77.T
                put_s(s, tri(s))

            @pl.when(jnp.logical_not((c == 1) & (p == 1)))
            def _():
                g76 = jnp.where(c == 1, g_here, mat(gd, 1).astype(F32))
                q76 = g76 - dot3(w77, full(1), 0, 0)
                phi76 = dot3(l77, q76, 0, 0)

                @pl.when((c == 0) & (p == 0))
                def _():
                    t66 = dot3(w66, full(0), 0, 0) + dot3(w76, full(1), 0, 0)
                    q66 = keep(g_here - t66)
                    l66, l76 = mat(lbuf, 0, 0).astype(F32), mat(lbuf, 0, 1).astype(F32)
                    m66 = dot3(l66, q66, 0, 0) + dot3(l76, q76, 0, 0)
                    phi66 = keep(m66) - 0.5 * m66 * eye
                    inner = dot3(phi76, w66) + dot3(phi77, w76)
                    half66 = dot3(w66, dot3(phi66, w66), 0, 0) + dot3(w76, inner, 0, 0)
                    s = half66 + half66.T
                    put_s(s, tri(s))

                @pl.when(jnp.logical_not((c == 0) & (p == 0)))
                def _():
                    inner = dot3(phi76, w66) + dot3(phi77 + phi77.T, w76)

                    @pl.when(c == 1)
                    def _():
                        s = dot3(w77, inner, 0, 0)
                        put_s(s, s)

                    @pl.when(c == 0)
                    def _():
                        put_s(dot3(inner, w77, 0, 0), jnp.zeros((tile, tile), F32))

        zero = jnp.zeros((tile, tile), F32)
        loop(0, loc, lambda a: store(a, zero))

        @pl.when(jnp.logical_not(top))
        def _():
            store(loc, zero)

        put_x(1, jnp.where(p == 0, -w[2], -w[1]))

        with jax.named_scope("low"):

            @pl.when(p == 0)
            def _():
                put_x(0, -w[0])

                def low(t):
                    total = times_x(zero, 0, mat(gv, first + t))
                    store(first + t, times_x(total, 1, mat(gbuf, 1, t)))

                def late(t):
                    g_twin(t)
                    low(t)

                loop(0, cut, low)
                loop(cut, n, late)

            @pl.when(p == 1)
            def _():
                loop(0, n, lambda t: store(first + t, times_x(zero, 1, mat(gv, first + t))))

        drain = jax.named_scope("drain")
        drain.__enter__()

        @pl.when(p == 0)
        def _():
            g_sent(1, gbuf.at[0, pl.ds(cut, n - cut)])

            @pl.when(top & (c == 1))
            def _():
                d_copy(1, gv.at[loc], 0, {"row": mate}).wait_send()
                d_copy(1, gv.at[loc], 1, {"row": mate, "col": twin}).wait_send()
                d_copy(2, gd.at[2], 2, {"row": mate}).wait_send()

        @pl.when(p == 1)
        def _():
            g_sent(1, gbuf.at[1])

            @pl.when(top & (c == 1))
            def _():
                d_copy(2, gv.at[loc], 0, {"row": mate}).wait_send()
                d_copy(2, gv.at[loc], 1, {"col": twin}).wait_send()

        @pl.when(((p == 0) | (c == 1)) & odd)
        def _():
            l_sent(1)
            if ring > 1:
                l_sent(0)

        @pl.when((p == 1) | (c == 1))
        def _():
            l_sent(3 - p)

            @pl.when(odd)
            def _():
                l_sent(5 - p)

        if ring > 1:
            g_sent(0, gbuf.at[p])
        for k in range(2):
            h_mate(k).wait_send()

            @pl.when(jnp.logical_not(top))
            def _():
                h_root(k).wait_send()

            @pl.when(top)
            def _():
                h_twin(k).wait_send()

        @pl.when(top)
        def _():
            h_full().wait_send()
            if ring > 1:
                s_sent(0)

        drain.__exit__(None, None, None)

    @pl.when(top)
    def _():
        for k in range(pairs - 1):
            k_star(k).wait_send()
        k_mate(lv.at[loc]).wait_send()

    @pl.when(jnp.logical_not(top))
    def _():
        k_mate(lk.at[c]).wait_send()


def panel(factor, grad, n_row, n_col, first):
    rows_here, tile = factor.shape[0], factor.shape[1]
    n = rows_here - first
    half = tile // 2
    pairs = n_row // 2
    sub = (SUB, tile // SUB, tile)
    hbm = pl.BlockSpec(memory_space=pltpu.HBM)
    dma = pltpu.SemaphoreType.DMA
    return pl.pallas_call(
        functools.partial(panel_kernel, n_row, n_col),
        out_shape=jax.ShapeDtypeStruct((rows_here, tile * tile // LANE, LANE), F32),
        in_specs=[hbm, hbm],
        out_specs=pl.BlockSpec(memory_space=pltpu.VMEM),
        scratch_shapes=[
            pltpu.VMEM((rows_here, *sub), BF16),
            pltpu.VMEM((rows_here, *sub), BF16),
            pltpu.VMEM((2, n, *sub), BF16),
            pltpu.VMEM((2, tile, tile), BF16),
            pltpu.VMEM((2, tile, tile), BF16),
            pltpu.VMEM((2, *sub), BF16),
            pltpu.VMEM((2, 2, *sub), BF16),
            pltpu.VMEM((3, tile, tile), F32),
            pltpu.VMEM((2, 2, half, tile), F32),
            pltpu.VMEM((tile, tile), F32),
            pltpu.VMEM((2, 2, half, tile), F32),
            pltpu.VMEM((2, half, tile), F32),
            pltpu.VMEM((pairs, 2, half, tile), F32),
            pltpu.VMEM((2, half, tile), F32),
            pltpu.VMEM((2, half, tile), F32),
            pltpu.VMEM((2, pairs, half, tile), F32),
            pltpu.VMEM((2, half, tile), F32),
            pltpu.VMEM((2, 3, half, tile), F32),
            pltpu.VMEM((3, *sub), BF16),
            pltpu.VMEM((2, CHUNKS, tile // CHUNKS, tile), F32),
            dma((5,)),
            dma((3,)),
            dma((n, SUB)),
            dma((n,)),
            dma((7,)),
            dma((SUB,)),
            dma((SUB,)),
            dma((2,)),
            dma((2,)),
            dma((pairs + 1,)),
            dma((2,)),
            dma((3,)),
            dma((pairs + 2,)),
            dma((5,)),
            dma((5,)),
            dma((2, pairs)),
            dma((3,)),
            dma((3,)),
            dma((3,)),
            dma((CHUNKS,)),
            dma((1,)),
        ],
        compiler_params=pltpu.CompilerParams(
            collective_id=0, has_side_effects=True, vmem_limit_bytes=VMEM
        ),
        name="panel",
    )(
        pltpu.with_memory_space_constraint(factor.reshape(rows_here, *sub), pltpu.HBM),
        pltpu.with_memory_space_constraint(grad.reshape(rows_here, *sub), pltpu.HBM),
    )


def per_device(l_saved, l_grad):
    rows_here, tile = l_saved.shape[0], l_saved.shape[2]
    n_row = lax.axis_size("row")
    n_col = lax.axis_size("col")
    assert n_col % n_row == 0 and n_row % 4 == 0 and tile % (SUB * 16) == 0
    first = n_col // n_row
    factor = l_saved.reshape(rows_here, tile, tile)
    grad = l_grad.reshape(rows_here, tile, tile)
    lin = panel(factor, grad, n_row, n_col, first)
    return lin.reshape(l_grad.shape)


def solution(mesh):
    spec = P(None, "row", None, "col", None)
    return jax.shard_map(
        per_device, mesh=mesh, in_specs=(spec, spec), out_specs=spec, check_vma=False
    )
```

```python
import functools

import jax
import jax.numpy as jnp
from jax import lax
from jax.experimental import pallas as pl
from jax.experimental.pallas import tpu as pltpu
from jax.sharding import PartitionSpec as P

F32 = jnp.float32
BF16 = jnp.bfloat16
HIGH3 = lax.Precision.HIGH
MESH = pl.DeviceIdType.MESH
CHUNKS = 8
SUB = 4
LANE = 128
VMEM = 40 * 1024 * 1024


def dot3(a, b, ca=1, cb=0):
    return lax.dot_general(
        a, b, (((ca,), (cb,)), ((), ())), precision=HIGH3, preferred_element_type=F32
    )


def outer(a, b):
    return lax.dot_general(a, b, (((0,), (0,)), ((), ())), preferred_element_type=F32)


def panel_kernel(
    n_row,
    n_col,
    l_hbm,
    g_hbm,
    lin,
    lv,
    gv,
    gbuf,
    xh,
    xl,
    lk,
    lbuf,
    w,
    h,
    own,
    tout,
    tin,
    tslot,
    hin,
    hsum,
    hslot,
    htwin,
    hfull,
    gd,
    sbuf,
    vs,
    gs,
    gm,
    gx,
    ls,
    lm,
    lx,
    lf,
    lp,
    ks,
    kr,
    ts,
    tr,
    hs,
    hr,
    hq,
    ds,
    dr,
    ss,
    sm,
    sx,
):
    held, tile = lv.shape[0], lv.shape[3]
    half = tile // 2
    n = gbuf.shape[1]
    first = held - n
    loc = first - 1
    ring = n_col // 2
    cut = n // 2
    head = min(1, n)
    pairs = n_row // 2
    parts = tile // LANE

    row = lax.axis_index("row")
    col = lax.axis_index("col")
    q, p = col // 2, col % 2
    y, c = row // 2, row % 2
    panel = q == ring - 1
    top = y == pairs - 1
    hub = max(ring - 3, 0)
    other = jnp.logical_not(panel)
    below = (q > 0) & (q <= hub)
    above = (q == hub) & (q < ring - 2)
    lower = jnp.where(panel, 2 * hub + p, jnp.maximum(col - 2, 0))
    upper_col = jnp.minimum(col + 2, n_col - 1)
    feeder = jnp.where(q == hub, n_col - 2 + p, jnp.where(q < hub, upper_col, lower))
    twin = 2 * q + 1 - p
    mate = 2 * y + 1 - c
    odd = y % 2 == 1
    pal = 2 * (y + 1 - 2 * (y % 2)) + c
    root = n_row - 2 + c

    rows = lax.broadcasted_iota(jnp.int32, (tile, tile), 0)
    cols = lax.broadcasted_iota(jnp.int32, (tile, tile), 1)

    def rdma(src, dst, s_sem, r_sem, dev):
        return pltpu.make_async_remote_copy(
            src_ref=src, dst_ref=dst, send_sem=s_sem, recv_sem=r_sem, device_id=dev, device_id_type=MESH
        )

    def loop(a, b, body):
        def step(i, carry):
            body(i)
            return carry

        if a < b:
            lax.fori_loop(a, b, step, 0)

    def load(src, dst, k, a, b):
        return pltpu.make_async_copy(src.at[pl.ds(a, b - a)], dst.at[pl.ds(a, b - a)], vs.at[k])

    spans = [
        (l_hbm, lv, 0, loc, first),
        (g_hbm, gv, 1, first, first + head),
        (l_hbm, lv, 2, first, held),
        (g_hbm, gv, 3, first + head, held),
        (g_hbm, gv, 4, 0, first),
    ]
    loads = {span[2]: load(*span) for span in spans if span[3] < span[4]}
    for cp in loads.values():
        cp.start()

    def loaded(*ks):
        for k in ks:
            if k in loads:
                loads[k].wait()

    barrier = pltpu.get_barrier_semaphore()

    def greet(dev):
        pl.semaphore_signal(barrier, inc=1, device_id=dev, device_id_type=MESH)

    greet({"col": twin})
    greet({"row": mate})
    greet({"row": pal})

    @pl.when(below | panel)
    def _():
        greet({"col": lower})

    @pl.when(above)
    def _():
        greet({"col": upper_col})

    @pl.when(other)
    def _():
        greet({"col": feeder})

    @pl.when(jnp.logical_not(top))
    def _():
        greet({"row": root})

    @pl.when(top)
    def _():
        for k in range(pairs - 1):
            greet({"row": 2 * k + c})

    @pl.when(top & panel)
    def _():
        greet({"row": mate, "col": twin})

    heard = (
        3
        + (below | panel).astype(jnp.int32)
        + above.astype(jnp.int32)
        + other.astype(jnp.int32)
        + jnp.where(top, pairs - 1, 1)
        + (top & panel).astype(jnp.int32)
    )
    with jax.named_scope("barrier"):
        pl.semaphore_wait(barrier, heard)

    loaded(0)

    def mat(ref, *at):
        return ref[at].reshape(tile, tile)

    def g_down(t, k, src):
        return rdma(src.at[k], gbuf.at[p, t, k], gs.at[0], gm.at[t, k], {"col": lower})

    def g_up(t, k, src):
        return rdma(src.at[k], gbuf.at[p, t, k], gs.at[2], gm.at[t, k], {"col": upper_col})

    def g_cross(t, k, src):
        return rdma(src.at[k], gbuf.at[p, t, k], gs.at[1], gx.at[t], {"col": twin})

    def f_cross(t, k):
        return rdma(lv.at[first + t, k], gbuf.at[0, t, k], gs.at[1], gx.at[t], {"col": twin})

    def g_main(t, k):
        ref = gbuf.at[p, t, k]
        rdma(ref, ref, gs.at[0], gm.at[t, k], {"col": twin}).wait_recv()

    def g_twin(t):
        ref = gbuf.at[1 - p, t]
        rdma(ref, ref, gs.at[1], gx.at[t], {"col": twin}).wait_recv()

    def g_sent(k, ref):
        rdma(ref, ref, gs.at[k], gx.at[0], {"col": twin}).wait_send()

    def l_down(k, src):
        return rdma(src.at[k], lbuf.at[p, c, k], ls.at[0], lm.at[k], {"col": lower})

    def l_up(k, src):
        return rdma(src.at[k], lbuf.at[p, c, k], ls.at[6], lm.at[k], {"col": upper_col})

    def l_cross(k, src):
        return rdma(src.at[k], lbuf.at[p, c, k], ls.at[1], lx.at[k], {"col": twin})

    def l_share(s, k):
        ref = lbuf.at[s, c, k]
        rdma(ref, ref, ls.at[4 + s], lp.at[s], {"row": pal}).start()
        rdma(ref, ref, ls.at[2 + s], lf.at[s], {"row": mate}).start()

    def l_main(k):
        ref = lbuf.at[p, c, k]
        rdma(ref, ref, ls.at[0], lm.at[k], {"col": twin}).wait_recv()

    def l_twin(k):
        ref = lbuf.at[1 - p, c, k]
        rdma(ref, ref, ls.at[1], lx.at[k], {"col": twin}).wait_recv()

    def l_rest(s):
        ref = lbuf.at[s, c]
        rdma(ref, ref, ls.at[4], lp.at[s], {"row": pal}).wait_recv()
        rdma(ref, ref, ls.at[2 + s], lf.at[s], {"row": mate}).start()

    def l_full(s):
        ref = lbuf.at[s, 1 - c]
        rdma(ref, ref, ls.at[2], lf.at[s], {"row": mate}).wait_recv()

    def l_sent(k):
        ref = lbuf.at[0, 0]
        rdma(ref, ref, ls.at[k], lf.at[0], {"row": mate}).wait_send()

    def k_star(k):
        return rdma(lv.at[loc], lk.at[c], ks.at[k], kr.at[c], {"row": 2 * k + c})

    def k_mate(src):
        return rdma(src, lk.at[c], ks.at[pairs], kr.at[c], {"row": mate})

    def k_wait(i):
        rdma(lk.at[i], lk.at[i], ks.at[pairs], kr.at[i], {"row": mate}).wait_recv()

    def t_mate():
        return rdma(h.at[1 - c], tin, ts.at[0], tr.at[pairs], {"row": mate})

    def t_root():
        return rdma(tout.at[0], tslot.at[y], ts.at[1], tr.at[y], {"row": root})

    def t_all():
        return rdma(tout.at[0], tout.at[1], ts.at[2], tr.at[pairs + 1], {"row": mate})

    def h_mate(k):
        return rdma(h.at[k, 1 - c], hin.at[k], hs.at[k], hr.at[k], {"row": mate})

    def h_root(k):
        return rdma(hsum.at[k], hslot.at[k, y], hs.at[2 + k], hq.at[k, y], {"row": root})

    def h_twin(k):
        return rdma(hsum.at[k], htwin.at[k], hs.at[2 + k], hr.at[2 + k], {"col": twin})

    def h_full():
        return rdma(hfull.at[c], hfull.at[c], hs.at[4], hr.at[4], {"row": mate})

    def d_copy(k, src, i, dev):
        return rdma(src, gd.at[k], ds.at[i], dr.at[k], dev)

    def d_wait(k):
        d_copy(k, gd.at[k], 0, {"row": mate}).wait_recv()

    def s_down(k):
        return rdma(sbuf.at[p, k], sbuf.at[p, k], ss.at[0], sm.at[k], {"col": lower})

    def s_up(k):
        return rdma(sbuf.at[p, k], sbuf.at[p, k], ss.at[2], sm.at[k], {"col": upper_col})

    def s_cross(k):
        return rdma(sbuf.at[p, k], sbuf.at[p, k], ss.at[1], sx.at[0], {"col": twin})

    def s_main(k):
        s_down(k).wait_recv()

    def s_twin():
        ref = sbuf.at[1 - p]
        rdma(ref, ref, ss.at[1], sx.at[0], {"col": twin}).wait_recv()

    def s_sent(k):
        ref = sbuf.at[p]
        rdma(ref, ref, ss.at[k], sx.at[0], {"col": twin}).wait_send()

    @pl.when(top)
    def _():
        for k in range(pairs - 1):
            k_star(k).start()
        k_mate(lv.at[loc]).start()
        lk[c] = lv[loc]

    def gather_rows():
        @pl.when(jnp.logical_not(top))
        def _():
            k_wait(c)
            k_mate(lk.at[c]).start()

    def start_inverse(k):
        d = mat(lbuf, k, k).astype(F32)
        e = (rows == cols).astype(F32)
        on = d * e
        rc = 1.0 / jnp.sum(on, axis=1, keepdims=True)
        rr = 1.0 / jnp.sum(on, axis=0, keepdims=True)
        off = ((rows & 1) == 1) & (cols == rows - 1)
        w[k] = e * rr - rc * jnp.where(off, d, 0.0) * rr

    n_lev = tile.bit_length() - 2

    def inverse_level(sh, k):
        off = ((jnp.right_shift(rows, sh) & 1) == 1) & (
            jnp.right_shift(cols, sh) == jnp.right_shift(rows, sh) - 1
        )
        part = jnp.where(off, mat(lbuf, k, k).astype(F32), 0.0)
        cur = w[k]
        w[k] = cur - dot3(cur, dot3(part, cur))

    def finish_inverse():
        w[2] = -dot3(w[1], dot3(mat(lbuf, 0, 1).astype(F32), w[0]))

    def put_x(i, x):
        hi = x.astype(BF16)
        xh[i] = hi
        xl[i] = (x - hi.astype(F32)).astype(BF16)

    def store(a, value):
        for b in range(parts):
            lin[a, pl.ds(b, tile, stride=parts), :] = value[:, b * LANE : (b + 1) * LANE]

    h[...] = jnp.zeros_like(h)

    def add_h(k, left, right):
        h[k] += outer(left, right).reshape(2, half, tile)

    def times_x(total, i, g):
        for part in (xl, xh):
            total = total - jnp.dot(g, part[i], preferred_element_type=F32)
        return total

    @pl.when(jnp.logical_not(panel))
    def _():
        loaded(1, 2, 3, 4)

        def relay(t, work=()):
            for k in range(SUB):
                with jax.named_scope("w_main"):
                    g_main(t, k)

                @pl.when(below)
                def _():
                    g_down(t, k, gbuf.at[p, t]).start()

                @pl.when(above)
                def _():
                    g_up(t, k, gbuf.at[p, t]).start()

                g_cross(t, k, gbuf.at[p, t]).start()
                if k < len(work):
                    work[k]()

        def use(t):
            with jax.named_scope("w_cross"):
                g_twin(t)
            right = mat(lv, first + t)
            add_h(0, mat(gbuf, 0, t), right)
            add_h(1, mat(gbuf, 1, t), right)

        def low(t):
            total = mat(gv, first + t).astype(F32)
            for s in range(2):
                total = times_x(total, s, mat(gbuf, s, t))
            store(first + t, total)

        main_l = (p == 0) | (c == 1)
        other_l = (p == 1) | (c == 1)

        for t in range(head):
            relay(t)
            if t == 0:
                with jax.named_scope("gather"):
                    gather_rows()

        with jax.named_scope("l_relay"):

            @pl.when(main_l & odd)
            def _():
                def step(k):
                    l_main(k)

                    @pl.when(below)
                    def _():
                        l_down(k, lbuf.at[p, c]).start()

                    @pl.when(above)
                    def _():
                        l_up(k, lbuf.at[p, c]).start()

                    l_cross(k, lbuf.at[p, c]).start()
                    l_share(p, k)

                loop(0, SUB, step)

        def share_first():
            @pl.when(main_l & jnp.logical_not(odd))
            def _():
                l_rest(p)

            @pl.when(other_l & odd)
            def _():
                def step(k):
                    l_twin(k)
                    l_share(1 - p, k)

                loop(0, SUB, step)

        def share_rest():
            @pl.when(other_l & jnp.logical_not(odd))
            def _():
                l_rest(1 - p)

        def share_done():
            k_wait(1 - c)
            l_full(0)

            @pl.when(c == 0)
            def _():
                l_full(1)

        steps = (lambda: None, lambda: None, share_first, lambda: None, share_rest, share_done)
        for j, share in enumerate(steps):
            if head + j < n:
                relay(head + j, (lambda: None, functools.partial(use, j - 1)) if j > 0 else ())
            with jax.named_scope("l_wait"):
                share()
        warm = min(head + len(steps), n)
        used = max(warm - head - 1, 0)

        start_inverse(0)
        start_inverse(1)

        base = warm
        lag = base - used
        double = min(n_lev // 2, n - base)

        def level_step(i):
            lev = 2 * (i - base) + 1

            def third():
                inverse_level(lev + 1, 0)
                use(i - lag)

            relay(
                i,
                (
                    lambda: inverse_level(lev, 0),
                    lambda: inverse_level(lev, 1),
                    third,
                    lambda: inverse_level(lev + 1, 1),
                ),
            )

        loop(base, base + double, level_step)
        used += double

        def level_rest(k):
            loop(2 * double + 1, n_lev + 1, lambda lev: inverse_level(lev, k))

        def x_first():
            put_x(0, dot3(w[0], mat(lk, 0).astype(F32)))

        def x_second():
            put_x(1, dot3(w[2], mat(lk, 0).astype(F32)) + dot3(w[1], mat(lk, 1).astype(F32)))

        def solve_x():
            x_first()
            x_second()
            loop(used, at - 1, use)

        at = base + double
        if at < n:
            relay(at, (lambda: level_rest(0), lambda: level_rest(1), finish_inverse, solve_x))
            used = at - 1
            at += 1
        else:
            level_rest(0)
            level_rest(1)
            finish_inverse()
            x_first()
            x_second()
        begun = at

        per = max(d for d in (1, 2, 3) if d == 1 or d * max(n - begun, 1) <= n - 2)

        def low_step(i):
            j = (i - begun) * per
            relay(i, [lambda: use(i - 2)] + [functools.partial(lambda d: low(j + d), d) for d in range(per)])

        loop(begun, n, low_step)
        lows = per * max(n - begun, 0)
        used += max(n - begun, 0)

        def use_main(t):
            add_h(p, mat(gbuf, p, t), mat(lv, first + t))

        def use_twin(t):
            with jax.named_scope("w_cross"):
                g_twin(t)
            add_h(1 - p, mat(gbuf, 1 - p, t), mat(lv, first + t))

        def give():
            t_mate().start()

        def take():
            with jax.named_scope("w_tmate"):
                t_mate().wait_recv()
            tout[0] = h[c] + tin[...]

        def upper(a):
            store(a, mat(gv, a).astype(F32))

        @pl.when(jnp.logical_not(top))
        def _():
            loop(used, n, use_main)

            @pl.when(c != p)
            def _():
                give()

            @pl.when(c == p)
            def _():
                take()
                t_root().start()

            loop(used, n, use_twin)

            @pl.when(c == p)
            def _():
                give()

            @pl.when(c != p)
            def _():
                take()
                t_root().start()

            loop(lows, n, low)
            loop(0, loc + 1, upper)

        @pl.when(top)
        def _():
            def s_relay(k):
                with jax.named_scope("w_s"):
                    s_main(k)

                @pl.when(below)
                def _():
                    s_down(k).start()

                @pl.when(above)
                def _():
                    s_up(k).start()

                s_cross(k).start()

            early = max(min(CHUNKS, used - lows), 0)

            def give_twin():
                @pl.when(c == p)
                def _():
                    give()

            loop(used, n, use_main)

            @pl.when(c != p)
            def _():
                give()

            rest = list(range(used, n))
            for k in range(CHUNKS):
                s_relay(k)
                if k < early:
                    low(lows + k)
                if rest and k % 2 == 1 and k >= CHUNKS // 2 - 1:
                    use_twin(rest.pop(0))
                    if not rest:
                        give_twin()
            if rest:
                loop(rest[0], n, use_twin)
                give_twin()

            loop(lows + early, n, low)
            loop(0, loc, upper)
            total = mat(gv, loc).astype(F32) - dot3(mat(sbuf, p), mat(lk, p).astype(F32))
            take()
            with jax.named_scope("w_tslot"):
                for k in range(pairs - 1):
                    rdma(tslot.at[k], tslot.at[k], ts.at[1], tr.at[k], {"row": mate}).wait_recv()
            for k in range(pairs - 1):
                tout[0] += tslot[k]
            own[...] = total

            @pl.when(c == 1)
            def _():
                t_all().start()
                own[...] -= dot3(w[1], mat(tout, 0), 0, 0)

            @pl.when(c == 0)
            def _():
                own[...] -= dot3(w[0], mat(tout, 0), 0, 0)
                with jax.named_scope("w_tall"):
                    t_all().wait_recv()
                own[...] -= dot3(w[2], mat(tout, 1), 0, 0)

            with jax.named_scope("w_s2"):
                s_twin()
            store(loc, own[...] - dot3(mat(sbuf, 1 - p), mat(lk, 1 - p).astype(F32)))

        drain = jax.named_scope("drain")
        drain.__enter__()

        g_sent(1, gbuf.at[p])

        @pl.when(below)
        def _():
            g_sent(0, gbuf.at[p])

        @pl.when(above)
        def _():
            g_sent(2, gbuf.at[p])

        @pl.when(main_l)
        def _():
            l_sent(2 + p)

            @pl.when(odd)
            def _():
                l_sent(1)
                l_sent(4 + p)

            @pl.when(odd & below)
            def _():
                l_sent(0)

            @pl.when(odd & above)
            def _():
                l_sent(6)

        @pl.when(other_l)
        def _():
            l_sent(3 - p)

            @pl.when(odd)
            def _():
                l_sent(5 - p)

        t_mate().wait_send()

        @pl.when(jnp.logical_not(top))
        def _():
            t_root().wait_send()

        @pl.when(top & (c == 1))
        def _():
            t_all().wait_send()

        @pl.when(top)
        def _():
            s_sent(1)

            @pl.when(below)
            def _():
                s_sent(0)

            @pl.when(above)
            def _():
                s_sent(2)

        drain.__exit__(None, None, None)

    @pl.when(panel)
    def _():
        def each(body):
            def run(t):
                for k in range(SUB):
                    body(t, k)

            return run

        send = each(lambda t, k: g_down(t, k, gv.at[first + t]).start() if ring > 1 else None)
        cross_lo = each(lambda t, k: f_cross(t, k).start())
        cross_hi = each(lambda t, k: g_cross(t, k, gv.at[first + t]).start())
        lead = min(head, cut)
        mid = min(cut + 2, n)
        loaded(1)
        loop(0, head, send)

        @pl.when(p == 0)
        def _():
            loaded(2)
            loop(cut, mid, cross_lo)

        @pl.when(p == 1)
        def _():
            loop(0, lead, cross_hi)
            loaded(2)

        loaded(3, 4)
        @pl.when(jnp.logical_not(odd))
        def _():
            loop(head, n, send)

        with jax.named_scope("gather"):
            gather_rows()
            k_wait(1 - c)

        def send_l():
            @pl.when(odd)
            def _():
                def step(k):
                    if ring > 1:
                        l_down(k, lk.at[c]).start()
                    l_cross(k, lk.at[c]).start()

                loop(0, SUB, step)

        @pl.when(p == 0)
        def _():
            send_l()
            lbuf[0] = lk[...]
            loop(mid, n, cross_lo)

            @pl.when(top & (c == 1))
            def _():
                d_copy(1, gv.at[loc], 0, {"row": mate}).start()
                d_copy(1, gv.at[loc], 1, {"row": mate, "col": twin}).start()
                gd[1] = gv[loc]

        @pl.when(p == 1)
        def _():
            @pl.when(c == 1)
            def _():
                send_l()

            lbuf[1, 1] = lk[1]
            loop(lead, cut, cross_hi)

            @pl.when(top & (c == 1))
            def _():
                d_copy(2, gv.at[loc], 0, {"row": mate}).start()
                d_copy(2, gv.at[loc], 1, {"col": twin}).start()
                gd[2] = gv[loc]

        @pl.when(odd)
        def _():
            loop(head, n, send)

        with jax.named_scope("hd"):
            loop(0, n, lambda t: add_h(0, mat(gv, first + t), mat(lv, first + t)))
        h_mate(0).start()

        with jax.named_scope("l_wait"):
            @pl.when(((p == 1) | (c == 1)) & odd)
            def _():
                def step(k):
                    l_twin(k)
                    l_share(1 - p, k)

                loop(0, SUB, step)

            @pl.when(((p == 1) | (c == 1)) & jnp.logical_not(odd))
            def _():
                l_rest(1 - p)

            @pl.when(p == 1)
            def _():
                l_full(0)

            @pl.when((p == 0) & (c == 0))
            def _():
                l_full(1)

        def reduce_mate(k):
            with jax.named_scope("w_hmate"):
                h_mate(k).wait_recv()
            hsum[k] = h[k, c] + hin[k]

            @pl.when(jnp.logical_not(top))
            def _():
                h_root(k).start()

        def reduce_root(k):
            total = hsum[k]
            for i in range(pairs - 1):
                with jax.named_scope("w_hroot"):
                    ref = hslot.at[k, i]
                    rdma(ref, ref, hs.at[2 + k], hq.at[k, i], {"row": mate}).wait_recv()
                total = total + hslot[k, i]
            hsum[k] = total
            h_twin(k).start()

        start_inverse(0)
        start_inverse(1)
        reduce_mate(0)

        def level(lev):
            inverse_level(lev, 0)
            inverse_level(lev, 1)

        early = (n_lev + 1) // 2
        loop(1, early + 1, level)

        @pl.when(top)
        def _():
            reduce_root(0)

        loop(early + 1, n_lev + 1, level)
        finish_inverse()

        @pl.when(p == 0)
        def _():
            def use(t):
                with jax.named_scope("w_x"):
                    g_twin(t)
                add_h(1, mat(gbuf, 1, t), mat(lv, first + t))

            loop(0, cut, use)

        @pl.when(p == 1)
        def _():
            def use(t):
                with jax.named_scope("w_x"):
                    g_twin(t)
                add_h(1, mat(gv, first + t), mat(gbuf, 0, t))

            loop(cut, n, use)

        h_mate(1).start()

        @pl.when(top & (c == 1) & (p == 0))
        def _():
            d_wait(2)
            d_copy(2, gd.at[2], 2, {"row": mate}).start()

        reduce_mate(1)

        @pl.when(top)
        def _():
            reduce_root(1)

        @pl.when(p == 1)
        def _():
            loop(cut, n, cross_hi)

        @pl.when(top)
        def _():
            with jax.named_scope("w_htwin"):
                for k in range(2):
                    h_twin(k).wait_recv()
            mine, theirs = hsum[0], htwin[0]
            hfull[c, 0] = jnp.where(p == 0, mine, theirs)
            hfull[c, 2] = jnp.where(p == 0, theirs, mine)
            hfull[c, 1] = hsum[1] + htwin[1]
            h_full().start()
            with jax.named_scope("w_hfull"):
                ref = hfull.at[1 - c]
                rdma(ref, ref, hs.at[4], hr.at[4], {"row": mate}).wait_recv()

                @pl.when(c == 0)
                def _():
                    d_wait(1)
                    d_wait(2)

            eye = (rows == cols).astype(F32)

            def keep(x):
                return jnp.where(rows >= cols, x, 0.0)

            w66, w77, w76 = w[0], w[1], w[2]
            l77 = mat(lbuf, 1, 1).astype(F32)
            g_here = mat(gv, loc).astype(F32)

            def full(k):
                return jnp.concatenate([hfull[0, k], hfull[1, k]], 0)

            q77 = keep(mat(gd, 2).astype(F32) - dot3(w77, full(2), 0, 0))
            m77 = dot3(l77, q77, 0, 0)
            phi77 = keep(m77) - 0.5 * m77 * eye

            def put_s(s, o):
                sbuf[p] = s.reshape(CHUNKS, tile // CHUNKS, tile)
                if ring > 1:
                    loop(0, CHUNKS, lambda k: s_down(k).start())
                store(loc, o)

            def tri(s):
                return keep(s) - 0.5 * s * eye

            @pl.when((c == 1) & (p == 1))
            def _():
                half77 = dot3(dot3(w77, phi77, 0, 0), w77)
                s = half77 + half77.T
                put_s(s, tri(s))

            @pl.when(jnp.logical_not((c == 1) & (p == 1)))
            def _():
                g76 = jnp.where(c == 1, g_here, mat(gd, 1).astype(F32))
                q76 = g76 - dot3(w77, full(1), 0, 0)
                phi76 = dot3(l77, q76, 0, 0)

                @pl.when((c == 0) & (p == 0))
                def _():
                    t66 = dot3(w66, full(0), 0, 0) + dot3(w76, full(1), 0, 0)
                    q66 = keep(g_here - t66)
                    l66, l76 = mat(lbuf, 0, 0).astype(F32), mat(lbuf, 0, 1).astype(F32)
                    m66 = dot3(l66, q66, 0, 0) + dot3(l76, q76, 0, 0)
                    phi66 = keep(m66) - 0.5 * m66 * eye
                    inner = dot3(phi76, w66) + dot3(phi77, w76)
                    half66 = dot3(w66, dot3(phi66, w66), 0, 0) + dot3(w76, inner, 0, 0)
                    s = half66 + half66.T
                    put_s(s, tri(s))

                @pl.when(jnp.logical_not((c == 0) & (p == 0)))
                def _():
                    inner = dot3(phi76, w66) + dot3(phi77 + phi77.T, w76)

                    @pl.when(c == 1)
                    def _():
                        s = dot3(w77, inner, 0, 0)
                        put_s(s, s)

                    @pl.when(c == 0)
                    def _():
                        put_s(dot3(inner, w77, 0, 0), jnp.zeros((tile, tile), F32))

        zero = jnp.zeros((tile, tile), F32)
        loop(0, loc, lambda a: store(a, zero))

        @pl.when(jnp.logical_not(top))
        def _():
            store(loc, zero)

        put_x(1, jnp.where(p == 0, -w[2], -w[1]))

        with jax.named_scope("low"):

            @pl.when(p == 0)
            def _():
                put_x(0, -w[0])

                def low(t):
                    total = times_x(zero, 0, mat(gv, first + t))
                    store(first + t, times_x(total, 1, mat(gbuf, 1, t)))

                def late(t):
                    g_twin(t)
                    low(t)

                loop(0, cut, low)
                loop(cut, n, late)

            @pl.when(p == 1)
            def _():
                loop(0, n, lambda t: store(first + t, times_x(zero, 1, mat(gv, first + t))))

        drain = jax.named_scope("drain")
        drain.__enter__()

        @pl.when(p == 0)
        def _():
            g_sent(1, gbuf.at[0, pl.ds(cut, n - cut)])

            @pl.when(top & (c == 1))
            def _():
                d_copy(1, gv.at[loc], 0, {"row": mate}).wait_send()
                d_copy(1, gv.at[loc], 1, {"row": mate, "col": twin}).wait_send()
                d_copy(2, gd.at[2], 2, {"row": mate}).wait_send()

        @pl.when(p == 1)
        def _():
            g_sent(1, gbuf.at[1])

            @pl.when(top & (c == 1))
            def _():
                d_copy(2, gv.at[loc], 0, {"row": mate}).wait_send()
                d_copy(2, gv.at[loc], 1, {"col": twin}).wait_send()

        @pl.when(((p == 0) | (c == 1)) & odd)
        def _():
            l_sent(1)
            if ring > 1:
                l_sent(0)

        @pl.when((p == 1) | (c == 1))
        def _():
            l_sent(3 - p)

            @pl.when(odd)
            def _():
                l_sent(5 - p)

        if ring > 1:
            g_sent(0, gbuf.at[p])
        for k in range(2):
            h_mate(k).wait_send()

            @pl.when(jnp.logical_not(top))
            def _():
                h_root(k).wait_send()

            @pl.when(top)
            def _():
                h_twin(k).wait_send()

        @pl.when(top)
        def _():
            h_full().wait_send()
            if ring > 1:
                s_sent(0)

        drain.__exit__(None, None, None)

    @pl.when(top)
    def _():
        for k in range(pairs - 1):
            k_star(k).wait_send()
        k_mate(lv.at[loc]).wait_send()

    @pl.when(jnp.logical_not(top))
    def _():
        k_mate(lk.at[c]).wait_send()


def panel(factor, grad, n_row, n_col, first):
    rows_here, tile = factor.shape[0], factor.shape[1]
    n = rows_here - first
    half = tile // 2
    pairs = n_row // 2
    sub = (SUB, tile // SUB, tile)
    hbm = pl.BlockSpec(memory_space=pltpu.HBM)
    dma = pltpu.SemaphoreType.DMA
    return pl.pallas_call(
        functools.partial(panel_kernel, n_row, n_col),
        out_shape=jax.ShapeDtypeStruct((rows_here, tile * tile // LANE, LANE), F32),
        in_specs=[hbm, hbm],
        out_specs=pl.BlockSpec(memory_space=pltpu.VMEM),
        scratch_shapes=[
            pltpu.VMEM((rows_here, *sub), BF16),
            pltpu.VMEM((rows_here, *sub), BF16),
            pltpu.VMEM((2, n, *sub), BF16),
            pltpu.VMEM((2, tile, tile), BF16),
            pltpu.VMEM((2, tile, tile), BF16),
            pltpu.VMEM((2, *sub), BF16),
            pltpu.VMEM((2, 2, *sub), BF16),
            pltpu.VMEM((3, tile, tile), F32),
            pltpu.VMEM((2, 2, half, tile), F32),
            pltpu.VMEM((tile, tile), F32),
            pltpu.VMEM((2, 2, half, tile), F32),
            pltpu.VMEM((2, half, tile), F32),
            pltpu.VMEM((pairs, 2, half, tile), F32),
            pltpu.VMEM((2, half, tile), F32),
            pltpu.VMEM((2, half, tile), F32),
            pltpu.VMEM((2, pairs, half, tile), F32),
            pltpu.VMEM((2, half, tile), F32),
            pltpu.VMEM((2, 3, half, tile), F32),
            pltpu.VMEM((3, *sub), BF16),
            pltpu.VMEM((2, CHUNKS, tile // CHUNKS, tile), F32),
            dma((5,)),
            dma((3,)),
            dma((n, SUB)),
            dma((n,)),
            dma((7,)),
            dma((SUB,)),
            dma((SUB,)),
            dma((2,)),
            dma((2,)),
            dma((pairs + 1,)),
            dma((2,)),
            dma((3,)),
            dma((pairs + 2,)),
            dma((5,)),
            dma((5,)),
            dma((2, pairs)),
            dma((3,)),
            dma((3,)),
            dma((3,)),
            dma((CHUNKS,)),
            dma((1,)),
        ],
        compiler_params=pltpu.CompilerParams(
            collective_id=0, has_side_effects=True, vmem_limit_bytes=VMEM
        ),
        name="panel",
    )(
        pltpu.with_memory_space_constraint(factor.reshape(rows_here, *sub), pltpu.HBM),
        pltpu.with_memory_space_constraint(grad.reshape(rows_here, *sub), pltpu.HBM),
    )


def per_device(l_saved, l_grad):
    rows_here, tile = l_saved.shape[0], l_saved.shape[2]
    n_row = lax.axis_size("row")
    n_col = lax.axis_size("col")
    assert n_col % n_row == 0 and n_row % 4 == 0 and tile % (SUB * 16) == 0
    first = n_col // n_row
    factor = l_saved.reshape(rows_here, tile, tile)
    grad = l_grad.reshape(rows_here, tile, tile)
    lin = panel(factor, grad, n_row, n_col, first)
    return lin.reshape(l_grad.shape)


def solution(mesh):
    spec = P(None, "row", None, "col", None)
    return jax.shard_map(
        per_device, mesh=mesh, in_specs=(spec, spec), out_specs=spec, check_vma=False
    )
```
